64 devices in a mesh: data: 4 (over x, y), dap: 16 (over z, core).
Axes of the slice: x: 2, y: 2, z: 8, core: 2. Of those that a mesh axis runs over, the one named last changes fastest.
The devices are a block of a 4x4x8 slice.
Arguments:
- msa_act: bfloat16 [8192, 128, 64], P(('data', 'dap')), parts along dimension 0
- pair_act: bfloat16 [512, 128, 128], P(('data', 'dap')), parts along dimension 0
- msa_mask: int32 [8192, 128], P('data'), parts along dimension 0
- res_mask: int32 [512], P('data'), parts along dimension 0
- row_bias_w: bfloat16 [128, 8], replicated
- row_qkvg_w: bfloat16 [64, 4, 8, 8], replicated
- row_out_w: bfloat16 [8, 8, 64], replicated
- col_query_w: bfloat16 [64, 8, 8], replicated
- col_kv_w: bfloat16 [64, 2, 8], replicated
- col_gate_w: bfloat16 [64, 8, 8], replicated
- col_out_w: bfloat16 [8, 8, 64], replicated
- opm_proj_w: bfloat16 [64, 2, 32], replicated
- opm_out_w: bfloat16 [32, 32, 128], replicated
- start_bias_w: bfloat16 [128, 4], replicated
- start_qkvg_w: bfloat16 [128, 4, 4, 32], replicated
- start_out_w: bfloat16 [4, 32, 128], replicated
- end_bias_w: bfloat16 [128, 4], replicated
- end_qkvg_w: bfloat16 [128, 4, 4, 32], replicated
- end_out_w: bfloat16 [4, 32, 128], replicated
Outputs:
- output 1: bfloat16 [8192, 128, 64], P(('data', 'dap')), parts along dimension 0
- output 2: bfloat16 [512, 128, 128], P(('data', 'dap')), parts along dimension 0
There are 4 independent parts. The reference program is written for one: setup_inputs(seed, part) draws one part's arguments, and reference() takes and returns one part's arrays. A program takes and returns all parts, laid end to end along the dimension named above; an argument that names none is the same for every part.
All inputs are finite; a program needn't handle non-finite values.
Results may differ from the reference program's by a relative error of at most 0.0148932.
Values are sent between devices in bfloat16 or wider.
A program may use at most 768 MiB of HBM per device.

```python
import jax
import jax.numpy as jnp
from jax import lax

NUM_SEQ = 2048
NUM_RES = 128
MSA_DIM = 64
PAIR_DIM = 128
MSA_HEADS = 8
MSA_HEAD_DIM = 8
TRI_HEADS = 4
TRI_HEAD_DIM = 32
OPM_DIM = 32


def draw_weight(rng_key, arr_shape, fan_in, gain_val):
    return (jax.random.normal(rng_key, arr_shape, jnp.float32) * (gain_val * fan_in ** -0.5)).astype(jnp.bfloat16)


def setup_inputs(seed: int = 0, part: int = 0) -> dict:
    part_key = jax.random.fold_in(jax.random.key(seed), part)
    part_keys = jax.random.split(part_key, 6)
    common = jax.random.normal(part_keys[0], (NUM_RES, MSA_DIM), jnp.float32)
    seq_noise = jax.random.normal(part_keys[1], (NUM_SEQ, NUM_RES, MSA_DIM), jnp.float32)
    msa_act = (0.8 * common[None] + 0.6 * seq_noise).astype(jnp.bfloat16)
    pair_act = jax.random.normal(part_keys[2], (NUM_RES, NUM_RES, PAIR_DIM), jnp.float32).astype(jnp.bfloat16)
    msa_mask = (jax.random.randint(part_keys[3], (NUM_SEQ, NUM_RES), 0, 5) != 0).astype(jnp.int32)
    res_mask = (jax.random.randint(part_keys[4], (NUM_RES,), 0, 4) != 0).astype(jnp.int32)
    weight_keys = jax.random.split(jax.random.key(seed + 1), 15)
    msa_width = MSA_HEADS * MSA_HEAD_DIM
    tri_width = TRI_HEADS * TRI_HEAD_DIM
    return {
        'msa_act': msa_act,
        'pair_act': pair_act,
        'msa_mask': msa_mask,
        'res_mask': res_mask,
        'row_bias_w': draw_weight(weight_keys[0], (PAIR_DIM, MSA_HEADS), PAIR_DIM, 1.5),
        'row_qkvg_w': draw_weight(weight_keys[1], (MSA_DIM, 4, MSA_HEADS, MSA_HEAD_DIM), MSA_DIM, 1.25),
        'row_out_w': draw_weight(weight_keys[2], (MSA_HEADS, MSA_HEAD_DIM, MSA_DIM), msa_width, 1.0),
        'col_query_w': draw_weight(weight_keys[3], (MSA_DIM, MSA_HEADS, MSA_HEAD_DIM), MSA_DIM, 2.0),
        'col_kv_w': draw_weight(weight_keys[4], (MSA_DIM, 2, MSA_HEAD_DIM), MSA_DIM, 1.25),
        'col_gate_w': draw_weight(weight_keys[5], (MSA_DIM, MSA_HEADS, MSA_HEAD_DIM), MSA_DIM, 1.0),
        'col_out_w': draw_weight(weight_keys[6], (MSA_HEADS, MSA_HEAD_DIM, MSA_DIM), msa_width, 1.0),
        'opm_proj_w': draw_weight(weight_keys[7], (MSA_DIM, 2, OPM_DIM), MSA_DIM, 1.0),
        'opm_out_w': draw_weight(weight_keys[8], (OPM_DIM, OPM_DIM, PAIR_DIM), OPM_DIM * OPM_DIM, 0.5),
        'start_bias_w': draw_weight(weight_keys[9], (PAIR_DIM, TRI_HEADS), PAIR_DIM, 1.5),
        'start_qkvg_w': draw_weight(weight_keys[10], (PAIR_DIM, 4, TRI_HEADS, TRI_HEAD_DIM), PAIR_DIM, 1.25),
        'start_out_w': draw_weight(weight_keys[11], (TRI_HEADS, TRI_HEAD_DIM, PAIR_DIM), tri_width, 1.0),
        'end_bias_w': draw_weight(weight_keys[12], (PAIR_DIM, TRI_HEADS), PAIR_DIM, 1.5),
        'end_qkvg_w': draw_weight(weight_keys[13], (PAIR_DIM, 4, TRI_HEADS, TRI_HEAD_DIM), PAIR_DIM, 1.25),
        'end_out_w': draw_weight(weight_keys[14], (TRI_HEADS, TRI_HEAD_DIM, PAIR_DIM), tri_width, 1.0),
    }


def layer_norm(values):
    widened = values.astype(jnp.float32)
    mean_val = jnp.mean(widened, axis=-1, keepdims=True)
    centered = widened - mean_val
    variance = jnp.mean(centered * centered, axis=-1, keepdims=True)
    return (centered * lax.rsqrt(variance + 1e-5)).astype(jnp.bfloat16)


def project(einsum_form, activations, weight):
    return jnp.einsum(einsum_form, activations.astype(jnp.float32), weight.astype(jnp.float32)).astype(jnp.bfloat16)


def mask_bias(mask_vals):
    return (mask_vals.astype(jnp.float32) - 1.0) * 1e4


def gated_out(einsum_form, gate_proj, attended, out_w):
    gated_vals = (jax.nn.sigmoid(gate_proj.astype(jnp.float32)) * attended).astype(jnp.bfloat16)
    return jnp.einsum(einsum_form, gated_vals.astype(jnp.float32), out_w.astype(jnp.float32))


def row_attention(msa_act, pair_act, msa_mask, row_bias_w, row_qkvg_w, row_out_w):
    pair_bias = project('ijc,ch->hij', layer_norm(pair_act), row_bias_w).astype(jnp.float32)
    logit_scale = MSA_HEAD_DIM ** -0.5

    def one_seq(seq_inputs):
        seq_ln, seq_mask = seq_inputs
        projected = project('ic,cahd->aihd', seq_ln, row_qkvg_w)
        logits = jnp.einsum('ihd,jhd->hij', projected[0].astype(jnp.float32), projected[1].astype(jnp.float32)) * logit_scale + pair_bias + mask_bias(seq_mask)[None, None, :]
        attn_probs = jax.nn.softmax(logits, axis=-1).astype(jnp.bfloat16)
        attended = jnp.einsum('hij,jhd->ihd', attn_probs.astype(jnp.float32), projected[2].astype(jnp.float32))
        return gated_out('ihd,hdc->ic', projected[3], attended, row_out_w)

    updates = lax.map(one_seq, (layer_norm(msa_act), msa_mask))
    return (msa_act.astype(jnp.float32) + updates).astype(jnp.bfloat16)


def column_attention(msa_act, msa_mask, col_query_w, col_kv_w, col_gate_w, col_out_w):
    msa_ln = layer_norm(msa_act)
    mask_f = msa_mask.astype(jnp.float32)
    mask_count = jnp.sum(mask_f, axis=0) + 1e-10
    mean_query = (jnp.einsum('sr,src->rc', mask_f, msa_ln.astype(jnp.float32)) / mask_count[:, None]).astype(jnp.bfloat16)
    query_proj = project('rc,chd->rhd', mean_query, col_query_w)
    key_val = project('src,cad->asrd', msa_ln, col_kv_w)
    gate_proj = project('src,chd->srhd', msa_ln, col_gate_w)
    logits = jnp.einsum('rhd,srd->rhs', query_proj.astype(jnp.float32), key_val[0].astype(jnp.float32)) * (MSA_HEAD_DIM ** -0.5) + mask_bias(msa_mask).T[:, None, :]
    attn_probs = jax.nn.softmax(logits, axis=-1).astype(jnp.bfloat16)
    attended = jnp.einsum('rhs,srd->rhd', attn_probs.astype(jnp.float32), key_val[1].astype(jnp.float32))
    update = gated_out('srhd,hdc->src', gate_proj, attended[None], col_out_w)
    return (msa_act.astype(jnp.float32) + update).astype(jnp.bfloat16)


def outer_product_mean(msa_act, pair_act, msa_mask, opm_proj_w, opm_out_w):
    mask_f = msa_mask.astype(jnp.float32)
    projected = project('src,cae->asre', layer_norm(msa_act), opm_proj_w) * msa_mask.astype(jnp.bfloat16)[None, :, :, None]
    counts = jnp.einsum('si,sj->ij', mask_f, mask_f)
    right_proj = projected[1].astype(jnp.float32)
    out_f = opm_out_w.astype(jnp.float32)

    def one_row(row_inputs):
        left_row, count_row = row_inputs
        outer_sum = jnp.einsum('se,sjf->jef', left_row.astype(jnp.float32), right_proj).astype(jnp.bfloat16)
        return jnp.einsum('jef,efc->jc', outer_sum.astype(jnp.float32), out_f) / (1e-3 + count_row)[:, None]

    updates = lax.map(one_row, (jnp.swapaxes(projected[0], 0, 1), counts))
    return (pair_act.astype(jnp.float32) + updates).astype(jnp.bfloat16)


def triangle_start(pair_act, res_mask, bias_w, qkvg_w, out_w):
    pair_ln = layer_norm(pair_act)
    tri_bias = project('jkc,ch->hjk', pair_ln, bias_w).astype(jnp.float32)
    key_bias = mask_bias(res_mask)[None, None, :]
    logit_scale = TRI_HEAD_DIM ** -0.5

    def one_row(row_ln):
        projected = project('jc,cahd->ajhd', row_ln, qkvg_w)
        logits = jnp.einsum('jhd,khd->hjk', projected[0].astype(jnp.float32), projected[1].astype(jnp.float32)) * logit_scale + tri_bias + key_bias
        attn_probs = jax.nn.softmax(logits, axis=-1).astype(jnp.bfloat16)
        attended = jnp.einsum('hjk,khd->jhd', attn_probs.astype(jnp.float32), projected[2].astype(jnp.float32))
        return gated_out('jhd,hdc->jc', projected[3], attended, out_w)

    updates = lax.map(one_row, pair_ln)
    return (pair_act.astype(jnp.float32) + updates).astype(jnp.bfloat16)


def reference(msa_act, pair_act, msa_mask, res_mask, row_bias_w, row_qkvg_w, row_out_w, col_query_w, col_kv_w, col_gate_w, col_out_w, opm_proj_w, opm_out_w, start_bias_w, start_qkvg_w, start_out_w, end_bias_w, end_qkvg_w, end_out_w):
    msa_act = row_attention(msa_act, pair_act, msa_mask, row_bias_w, row_qkvg_w, row_out_w)
    msa_act = column_attention(msa_act, msa_mask, col_query_w, col_kv_w, col_gate_w, col_out_w)
    pair_act = outer_product_mean(msa_act, pair_act, msa_mask, opm_proj_w, opm_out_w)
    pair_act = triangle_start(pair_act, res_mask, start_bias_w, start_qkvg_w, start_out_w)
    pair_act = jnp.swapaxes(triangle_start(jnp.swapaxes(pair_act, 0, 1), res_mask, end_bias_w, end_qkvg_w, end_out_w), 0, 1)
    return (msa_act, pair_act)
```

```python
import functools
import math

import jax
import jax.numpy as jnp
from jax import lax
from jax.experimental import pallas as pl
from jax.experimental.pallas import tpu as pltpu
from jax.sharding import PartitionSpec as P

F32 = jnp.float32
BF16 = jnp.bfloat16
MESH = pl.DeviceIdType.MESH
LOG2E = math.log2(math.e)
VMEM = pltpu.VMEM


def layer_norm(values):
    widened = values.astype(jnp.float32)
    mean_val = jnp.mean(widened, axis=-1, keepdims=True)
    centered = widened - mean_val
    variance = jnp.mean(centered * centered, axis=-1, keepdims=True)
    return (centered * lax.rsqrt(variance + 1e-5)).astype(jnp.bfloat16)


def mask_bias(mask_vals):
    return (mask_vals.astype(jnp.float32) - 1.0) * 1e4


def matmul_bf(einsum_form, left_arr, right_arr):
    return jnp.einsum(einsum_form, left_arr, right_arr, preferred_element_type=jnp.float32).astype(jnp.bfloat16)


def gated_out(einsum_form, gate_proj, attended, out_w):
    gated_vals = (jax.nn.sigmoid(gate_proj.astype(jnp.float32)) * attended).astype(jnp.bfloat16)
    return jnp.einsum(einsum_form, gated_vals, out_w, preferred_element_type=jnp.float32)


def triangle_rows(pair_act, pair_ln, bias_full, res_mask, qkvg_w, out_w):
    projected = matmul_bf('ijc,cahd->aijhd', pair_ln, qkvg_w)
    logits = jnp.einsum('ijhd,ikhd->ihjk', projected[0], projected[1], preferred_element_type=jnp.float32) * (qkvg_w.shape[-1] ** -0.5) + bias_full[None] + mask_bias(res_mask)[None, None, None, :]
    attn_probs = jax.nn.softmax(logits, axis=-1).astype(jnp.bfloat16)
    attended = jnp.einsum('ihjk,ikhd->ijhd', attn_probs, projected[2], preferred_element_type=jnp.float32)
    return (pair_act + gated_out('ijhd,hdc->ijc', projected[3], attended, out_w)).astype(jnp.bfloat16)


def triangle_cols(pair_cols, pair_ln, bias_full, res_mask, qkvg_w, out_w):
    projected = matmul_bf('ijc,cahd->aijhd', pair_ln, qkvg_w)
    logits = jnp.einsum('ijhd,kjhd->jhik', projected[0], projected[1], preferred_element_type=jnp.float32) * (qkvg_w.shape[-1] ** -0.5) + bias_full[None] + mask_bias(res_mask)[None, None, None, :]
    attn_probs = jax.nn.softmax(logits, axis=-1).astype(jnp.bfloat16)
    attended = jnp.einsum('jhik,kjhd->ijhd', attn_probs, projected[2], preferred_element_type=jnp.float32)
    return (pair_cols + gated_out('ijhd,hdc->ijc', projected[3], attended, out_w)).astype(jnp.bfloat16)


def mm(left, right):
    return jnp.dot(left, right, preferred_element_type=F32)


def mm_nt(left, right):
    return lax.dot_general(left, right, (((1,), (1,)), ((), ())), preferred_element_type=F32)


def ln_rows(x):
    n = x.shape[0]
    xc = x - jnp.sum(x, axis=0, keepdims=True) * (1.0 / n)
    var = jnp.sum(xc * xc, axis=0, keepdims=True) * (1.0 / n)
    return (xc * lax.rsqrt(var + 1e-5)).astype(BF16)


def ln_lanes(x):
    n = x.shape[1]
    xc = x - jnp.sum(x, axis=1, keepdims=True) * (1.0 / n)
    var = jnp.sum(xc * xc, axis=1, keepdims=True) * (1.0 / n)
    return (xc * lax.rsqrt(var + 1e-5)).astype(BF16)


def bf16_split(value, terms):
    import numpy as np
    out = []
    for _ in range(terms):
        t = float(np.asarray(value, dtype=jnp.bfloat16))
        out.append(t)
        value = value - t
    return out


def bias_kernel(z_ref, w_ref, out_ref):
    heads = w_ref.shape[0]
    for r in range(z_ref.shape[0]):
        ln = ln_lanes(z_ref[r].astype(F32))
        out_ref[r * heads:(r + 1) * heads, :] = mm_nt(w_ref[...], ln).astype(BF16).astype(F32)


def row_kernel(m_ref, braw_ref, mask_ref, wqkvg_ref, wout_ref, wkvg_ref, m1_ref, kv_ref, g_ref, qsum_ref, bias_ref, wo_ref, *, heads, hd):
    seqs, chans, res = m_ref.shape
    width = heads * hd
    scale2 = hd ** -0.5 * LOG2E
    wo_ref[...] = wout_ref[...].astype(F32).T.astype(BF16)
    for h in range(heads):
        plane = braw_ref[pl.ds(h, res, stride=heads), :]
        bias_ref[:, h * res:(h + 1) * res] = plane.T * LOG2E
    qsum_ref[...] = jnp.zeros_like(qsum_ref)
    terms = bf16_split(1e4 / hd ** -0.5, 3)
    rows16 = lax.broadcasted_iota(jnp.int32, (16, res), 0)
    first = rows16 < hd
    mvec = jnp.where(rows16 == 0, terms[0], jnp.where(rows16 == 1, terms[1], jnp.where(rows16 == 2, terms[2], 0.0)))
    zero16 = jnp.zeros((16, res), BF16)
    one16 = jnp.ones((16, res), BF16)
    npairs = heads // 2

    def attend(qkvg, mrow):
        q = qkvg[0:width]
        kaug = jnp.concatenate([qkvg[width:2 * width], (mrow - 1.0) * mvec], axis=0)
        kt = kaug.T.astype(BF16)
        vT = qkvg[2 * width:3 * width].astype(BF16)
        outs = []
        for t in range(npairs):
            q16 = q[t * 16:(t + 1) * 16]
            qa = jnp.where(first, q16, 0.0).astype(BF16)
            qb = jnp.where(first, 0.0, q16).astype(BF16)
            left = jnp.concatenate([zero16] * t + [qa] + [zero16] * (npairs - 1 - t) + [one16], axis=0)
            right = jnp.concatenate([zero16] * t + [qb] + [zero16] * (npairs - 1 - t) + [one16], axis=0)
            s = mm(kt, jnp.concatenate([left, right], axis=1))
            s = s * scale2 + bias_ref[:, t * 2 * res:(t + 1) * 2 * res]
            p = jnp.exp2(s - jnp.max(s, axis=0, keepdims=True))
            inv = 1.0 / jnp.sum(p, axis=0, keepdims=True)
            o = mm(vT[t * 16:(t + 1) * 16], p.astype(BF16)) * inv
            outs += [o[0:hd, 0:res], o[hd:2 * hd, res:2 * res]]
        att = jnp.concatenate(outs, axis=0)
        return (jax.nn.sigmoid(qkvg[3 * width:4 * width]) * att).astype(BF16)

    def body(it, _):
        s0 = it * 2
        xs = [m_ref[s0 + u].astype(F32) for u in range(2)]
        lns = [ln_rows(x) for x in xs]
        proj = mm(wqkvg_ref[...], jnp.concatenate(lns, axis=1)).astype(BF16).astype(F32)
        mrows = [mask_ref[pl.ds(s0 + u, 1), :] for u in range(2)]
        ys = [attend(proj[:, u * res:(u + 1) * res], mrows[u]) for u in range(2)]
        upd = mm(wo_ref[...], jnp.concatenate(ys, axis=1))
        ln1 = []
        for u in range(2):
            m1 = (xs[u] + upd[:, u * res:(u + 1) * res]).astype(BF16)
            m1_ref[s0 + u] = m1
            l1 = ln_rows(m1.astype(F32))
            qsum_ref[...] += l1.astype(F32) * mrows[u]
            ln1.append(l1)
        kvg = mm(wkvg_ref[...], jnp.concatenate(ln1, axis=1)).astype(BF16)
        for u in range(2):
            kv_ref[pl.ds((s0 + u) * 2 * hd, 2 * hd), :] = kvg[0:2 * hd, u * res:(u + 1) * res].astype(F32)
            g_ref[s0 + u] = kvg[2 * hd:, u * res:(u + 1) * res]
        return 0

    lax.fori_loop(0, seqs // 2, body, 0)


def col_stats(qtot, cnt, kv_ref, mask_ref, wq_ref, planes_ref, stats_ref, heads, hd):
    seqs, res = mask_ref.shape
    qbar = (qtot / (cnt + 1e-10)).astype(BF16)
    q = mm(wq_ref[...], qbar).astype(BF16).astype(F32)
    for d in range(2 * hd):
        planes_ref[d] = kv_ref[pl.ds(d, seqs, stride=2 * hd), :]
    mb = (mask_ref[...] - 1.0) * (1e4 * LOG2E)
    for h in range(heads):
        acc = q[h * hd:h * hd + 1] * planes_ref[0]
        for d in range(1, hd):
            acc = acc + q[h * hd + d:h * hd + d + 1] * planes_ref[d]
        t = acc * (hd ** -0.5 * LOG2E) + mb
        mx = jnp.max(t, axis=0, keepdims=True)
        p = jnp.exp2(t - mx)
        stats_ref[h:h + 1, :] = mx
        stats_ref[heads + h:heads + h + 1, :] = jnp.sum(p, axis=0, keepdims=True)
        pb = p.astype(BF16).astype(F32)
        for d in range(hd):
            r = 2 * heads + h * hd + d
            stats_ref[r:r + 1, :] = jnp.sum(pb * planes_ref[hd + d], axis=0, keepdims=True)


def col1_kernel(qtot_ref, fmask_ref, kv_ref, mask_ref, wq_ref, stats_ref, planes_ref, *, heads, hd):
    cnt = jnp.sum(fmask_ref[...], axis=0, keepdims=True).astype(F32)
    col_stats(qtot_ref[...], cnt, kv_ref, mask_ref, wq_ref, planes_ref, stats_ref, heads, hd)


def combine_stats(stats, heads, hd):
    gm = stats[0][0:heads]
    for st in stats[1:]:
        gm = jnp.maximum(gm, st[0:heads])
    tot = None
    wv = None
    for st in stats:
        f = jnp.exp2(st[0:heads] - gm)
        fx = jnp.concatenate([jnp.broadcast_to(f[h:h + 1], (hd, f.shape[1])) for h in range(heads)], axis=0)
        tot = f * st[heads:2 * heads] if tot is None else tot + f * st[heads:2 * heads]
        wv = fx * st[2 * heads:] if wv is None else wv + fx * st[2 * heads:]
    totx = jnp.concatenate([jnp.broadcast_to(tot[h:h + 1], (hd, tot.shape[1])) for h in range(heads)], axis=0)
    return wv / totx


def col2_kernel(stats_ref, g_ref, m1_ref, mask_ref, wout_ref, wac_ref, m2_ref, a_ref, c_ref, o_ref, wo_ref, as_ref, cs_ref, at_ref, *, heads, hd):
    seqs, chans, res = m1_ref.shape
    wide = wac_ref.shape[0] // 2
    wo_ref[...] = wout_ref[...].astype(F32).T.astype(BF16)
    o_ref[...] = combine_stats([stats_ref[d] for d in range(stats_ref.shape[0])], heads, hd)

    def body(it, _):
        s0 = it * 2
        ys = [(jax.nn.sigmoid(g_ref[s0 + u].astype(F32)) * o_ref[...]).astype(BF16) for u in range(2)]
        upd = mm(wo_ref[...], jnp.concatenate(ys, axis=1))
        lns = []
        for u in range(2):
            m2 = (m1_ref[s0 + u].astype(F32) + upd[:, u * res:(u + 1) * res]).astype(BF16)
            m2_ref[s0 + u] = m2
            lns.append(ln_rows(m2.astype(F32)))
        ac = mm(wac_ref[...], jnp.concatenate(lns, axis=1)).astype(BF16).astype(F32)
        for u in range(2):
            mrow = mask_ref[pl.ds(s0 + u, 1), :]
            as_ref[pl.ds((s0 + u) * wide, wide), :] = ac[0:wide, u * res:(u + 1) * res] * mrow
            cs_ref[pl.ds((s0 + u) * wide, wide), :] = ac[wide:, u * res:(u + 1) * res] * mrow
        return 0

    lax.fori_loop(0, seqs // 2, body, 0)

    def planes(e, _):
        c_ref[e] = cs_ref[pl.ds(e, seqs, stride=wide), :].astype(BF16)
        at_ref[pl.ds(e, res, stride=wide), :] = as_ref[pl.ds(e, seqs, stride=wide), :].T
        return 0

    lax.fori_loop(0, wide, planes, 0)
    a_ref[...] = at_ref[...].astype(BF16)


def dap_index(chip, core, chips):
    return lax.rem(chip + 2 * chips, chips) * 2 + core


def opm_kernel(a_ref, c_ref, z_ref, mask_ref, w_ref, out_ref, ap_ref, cp_ref, part_ref, xhi_ref, xlo_ref, wt_ref, w32_ref, cnt_ref, pos_ref, neg_ref, ex_send, ex_recv, send_sem, recv_sem, *, chips):
    me = lax.axis_index('dap')
    chip, core = me // 2, lax.rem(me, 2)
    wide, seqs, res = c_ref.shape
    rows = z_ref.shape[0]
    brow = rows * wide
    outc = w_ref.shape[1]
    partner = chip * 2 + 1 - core
    peer = {1: dap_index(chip + 1, core, chips), -1: dap_index(chip - 1, core, chips)}
    half_chips = chips // 2

    barrier = pltpu.get_barrier_semaphore()
    for dev in (partner, peer[1], peer[-1]):
        pl.semaphore_signal(barrier, inc=1, device_id={'dap': dev}, device_id_type=MESH)
    pl.semaphore_wait(barrier, 3)

    swaps = []
    for n, (src, dst) in enumerate(((a_ref.at[:, 1 - core], ap_ref), (c_ref, cp_ref))):
        cp = pltpu.make_async_remote_copy(src, dst, ex_send.at[n], ex_recv.at[n], device_id={'dap': partner}, device_id_type=MESH)
        cp.start()
        swaps.append(cp)

    w32_ref[...] = w_ref[...].astype(F32)
    per = 128 // wide
    for b in range(wide // per):
        cols = [w32_ref[pl.ds(b * per + f, wide, stride=wide), :] for f in range(per)]
        wt_ref[:, b * 128:(b + 1) * 128] = jnp.concatenate(cols, axis=0).T.astype(BF16)

    def count_step(n, acc):
        blk = mask_ref[pl.ds(n * 128, 128), :].astype(F32)
        return acc + mm(blk.T.astype(BF16), blk.astype(BF16))

    cnt_ref[...] = lax.fori_loop(0, mask_ref.shape[0] // 128, count_step, jnp.zeros((res, res), F32))

    for cp in swaps:
        cp.wait()

    def block(dest, slot):
        lhs = jnp.concatenate([a_ref[dest, core], ap_ref[dest]], axis=1)

        def outer(fp, _):
            f0 = fp * 2
            rhs = jnp.concatenate([
                jnp.concatenate([c_ref[f0], c_ref[f0 + 1]], axis=1),
                jnp.concatenate([cp_ref[f0], cp_ref[f0 + 1]], axis=1)], axis=0)
            o = mm(lhs, rhs)
            hi = o.astype(BF16)
            lo = (o - hi.astype(F32)).astype(BF16)
            for i in range(rows):
                for u in range(2):
                    r0 = pl.multiple_of((f0 + u) * wide, wide)
                    src = (slice(i * wide, (i + 1) * wide), slice(u * res, (u + 1) * res))
                    xhi_ref[i // 2, pl.ds(r0, wide), (i % 2) * res:(i % 2 + 1) * res] = hi[src]
                    xlo_ref[i // 2, pl.ds(r0, wide), (i % 2) * res:(i % 2 + 1) * res] = lo[src]
            return 0

        lax.fori_loop(0, wide // 2, outer, 0)

        def inner(n, _):
            part_ref[slot, n] = mm(wt_ref[...], xhi_ref[n]) + mm(wt_ref[...], xlo_ref[n])
            return 0

        lax.fori_loop(0, rows // 2, inner, 0)

    sends = []
    arrivals = {}
    bufs = {1: pos_ref, -1: neg_ref}
    hq = rows // 4

    def hops(d, half):
        return half_chips if (half == 1) == (d == 1) else half_chips - 1

    slot_of = {}
    nbuf = 2 * half_chips - 1

    def buf_index(d, half, k):
        return (k - 1) + (0 if (half == 1) == (d == 1) else half_chips)

    def message(d, half, k, slot):
        idx = buf_index(d, half, k)
        src = part_ref.at[slot, pl.ds(half * hq, hq)]
        cp = pltpu.make_async_remote_copy(src, bufs[d].at[idx], send_sem.at[(d + 1) // 2, idx], recv_sem.at[(d + 1) // 2, idx], device_id={'dap': peer[d]}, device_id_type=MESH)
        arrivals[(d, half, k)] = cp
        sends.append(cp)
        cp.start()

    def take(d, half, k, slot):
        arrivals[(d, half, k)].wait_recv()
        part_ref[slot, half * hq:(half + 1) * hq] += bufs[d][buf_index(d, half, k)]

    def relay(d, k, slot):
        for half in ((0, 1) if d == 1 else (1, 0)):
            if k < hops(d, half):
                take(d, half, k + 1, slot)
            if k <= hops(d, half):
                message(d, half, k, slot)

    def dest_of(d, k):
        return lax.rem(chip + d * k + 2 * chips, chips)

    far = half_chips
    block(dest_of(1, far), 0)
    message(1, 1, far, 0)
    message(-1, 0, far, 0)
    slot = 1
    pending = []
    for k in range(far - 1, 0, -1):
        for d in (1, -1):
            block(dest_of(d, k), slot)
            if k == far - 1:
                message(d, 0 if d == 1 else 1, k, slot)
                pending.append((d, slot))
            else:
                relay(d, k, slot)
            slot += 1
        if k == far - 1:
            for d, sl in pending:
                half = 1 if d == 1 else 0
                take(d, half, far, sl)
                message(d, half, k, sl)
    block(chip, slot)
    for half in (0, 1):
        for d in (1, -1):
            take(d, half, 1, slot)
    for n in range(rows // 2):
        pair = part_ref[slot, n]
        for u in range(2):
            i = n * 2 + u
            cnt = cnt_ref[pl.ds(me * rows + i, 1), :] + 1e-3
            upd = (pair[:, u * res:(u + 1) * res] / cnt).T
            out_ref[i] = (z_ref[i].astype(F32) + upd).astype(BF16)
    for cp in sends:
        cp.wait_send()


def vspec():
    return pl.BlockSpec(memory_space=VMEM)


def call(kernel, outs, n_in, scratch, name, cid=None, flops=10 ** 9):
    params = dict(vmem_limit_bytes=60 * 2 ** 20)
    if cid is not None:
        params.update(collective_id=cid, has_side_effects=True)
    return pl.pallas_call(
        kernel,
        out_shape=outs,
        in_specs=[vspec()] * n_in,
        out_specs=jax.tree.map(lambda _: vspec(), outs),
        scratch_shapes=scratch,
        compiler_params=pltpu.CompilerParams(**params),
        cost_estimate=pl.CostEstimate(flops=flops, bytes_accessed=10 ** 6, transcendentals=0),
        name=name,
    )


def sds(shape, dtype):
    return jax.ShapeDtypeStruct(shape, dtype)


def solution(mesh):
    ndap = mesh.shape['dap']
    chips = ndap // 2

    def evoformer_block(msa, pair_act, full_mask, res_mask, row_bias_w, row_qkvg_w, row_out_w, col_query_w, col_kv_w, col_gate_w, col_out_w, opm_proj_w, opm_out_w, start_bias_w, start_qkvg_w, start_out_w, end_bias_w, end_qkvg_w, end_out_w):
        seqs, res, chans = msa.shape
        rows = pair_act.shape[0]
        heads, hd = row_qkvg_w.shape[2], row_qkvg_w.shape[3]
        width = heads * hd
        wide = opm_proj_w.shape[2]
        outc = opm_out_w.shape[2]
        me = lax.axis_index('dap')
        mask = lax.dynamic_slice_in_dim(full_mask, me * seqs, seqs, axis=0).astype(F32)
        m_t = jnp.swapaxes(msa, 1, 2)
        wt = lambda w: w.reshape(w.shape[0], -1).T

        braw = call(bias_kernel, sds((rows * heads, res), F32), 2, [], 'row_bias')(pair_act, row_bias_w.T)
        braw = lax.all_gather(braw, 'dap', axis=0, tiled=True)

        wkvg = jnp.concatenate([wt(col_kv_w), wt(col_gate_w)], axis=0)
        m1, kv, g, qsum = call(
            functools.partial(row_kernel, heads=heads, hd=hd),
            [sds((seqs, chans, res), BF16), sds((seqs * 2 * hd, res), F32), sds((seqs, width, res), BF16), sds((chans, res), F32)], 6,
            [VMEM((res, heads * res), F32), VMEM((chans, width), BF16)], 'row_attention',
        )(m_t, braw, mask, wt(row_qkvg_w), row_out_w.reshape(width, chans), wkvg)

        qtot = lax.psum(qsum, 'dap')
        nstat = 2 * heads + width
        stats = call(
            functools.partial(col1_kernel, heads=heads, hd=hd),
            sds((nstat, res), F32), 5, [VMEM((2 * hd, seqs, res), F32)], 'col_stats',
        )(qtot, full_mask, kv, mask, wt(col_query_w))
        stats = lax.all_gather(stats, 'dap', axis=0)

        m2, a, c = call(
            functools.partial(col2_kernel, heads=heads, hd=hd),
            [sds((seqs, chans, res), BF16), sds((res * wide, seqs), BF16), sds((wide, seqs, res), BF16)], 6,
            [VMEM((width, res), F32), VMEM((chans, width), BF16), VMEM((seqs * wide, res), F32), VMEM((seqs * wide, res), F32), VMEM((res * wide, seqs), F32)], 'col_out',
        )(stats, g, m1, mask, col_out_w.reshape(width, chans), wt(opm_proj_w))
        msa_out = jnp.swapaxes(m2, 1, 2)

        npair = rows // 2
        nbuf = 2 * (chips // 2) - 1
        pair_act = call(
            functools.partial(opm_kernel, chips=chips),
            sds(pair_act.shape, BF16), 5,
            [VMEM((chips, rows * wide, seqs), BF16), VMEM((wide, seqs, res), BF16),
             VMEM((chips, npair, outc, 2 * res), F32),
             VMEM((npair, wide * wide, 2 * res), BF16), VMEM((npair, wide * wide, 2 * res), BF16),
             VMEM((outc, wide * wide), BF16), VMEM((wide * wide, outc), F32), VMEM((res, res), F32),
             VMEM((nbuf, npair // 2, outc, 2 * res), F32), VMEM((nbuf, npair // 2, outc, 2 * res), F32),
             pltpu.SemaphoreType.DMA((2,)), pltpu.SemaphoreType.DMA((2,)),
             pltpu.SemaphoreType.DMA((2, nbuf)), pltpu.SemaphoreType.DMA((2, nbuf))],
            'outer_mean', cid=1,
        )(a.reshape(chips, 2, rows * wide, seqs), c, pair_act, full_mask, opm_out_w.reshape(wide * wide, outc))

        pair_ln = layer_norm(pair_act)
        start_full = lax.all_gather(matmul_bf('ijc,ch->hij', pair_ln, start_bias_w), 'dap', axis=1, tiled=True)
        pair_act = triangle_rows(pair_act, pair_ln, start_full, res_mask, start_qkvg_w, start_out_w)

        pair_cols = lax.all_to_all(pair_act, 'dap', 1, 0, tiled=True)
        cols_ln = layer_norm(pair_cols)
        end_full = lax.all_gather(matmul_bf('ijc,ch->hji', cols_ln, end_bias_w), 'dap', axis=1, tiled=True)
        pair_cols = triangle_cols(pair_cols, cols_ln, end_full, res_mask, end_qkvg_w, end_out_w)
        pair_out = lax.all_to_all(pair_cols, 'dap', 0, 1, tiled=True)
        return msa_out, pair_out

    row_spec = P(('data', 'dap'), None, None)
    in_specs = (row_spec, row_spec, P('data', None), P('data')) + (P(),) * 15
    return jax.shard_map(evoformer_block, mesh=mesh, in_specs=in_specs, out_specs=(row_spec, row_spec), check_vma=False)
```

```python
import functools
import math

import jax
import jax.numpy as jnp
from jax import lax
from jax.experimental import pallas as pl
from jax.experimental.pallas import tpu as pltpu
from jax.sharding import PartitionSpec as P

F32 = jnp.float32
BF16 = jnp.bfloat16
MESH = pl.DeviceIdType.MESH
LOG2E = math.log2(math.e)
VMEM = pltpu.VMEM


def layer_norm(values):
    widened = values.astype(jnp.float32)
    mean_val = jnp.mean(widened, axis=-1, keepdims=True)
    centered = widened - mean_val
    variance = jnp.mean(centered * centered, axis=-1, keepdims=True)
    return (centered * lax.rsqrt(variance + 1e-5)).astype(jnp.bfloat16)


def mask_bias(mask_vals):
    return (mask_vals.astype(jnp.float32) - 1.0) * 1e4


def matmul_bf(einsum_form, left_arr, right_arr):
    return jnp.einsum(einsum_form, left_arr, right_arr, preferred_element_type=jnp.float32).astype(jnp.bfloat16)


def gated_out(einsum_form, gate_proj, attended, out_w):
    gated_vals = (jax.nn.sigmoid(gate_proj.astype(jnp.float32)) * attended).astype(jnp.bfloat16)
    return jnp.einsum(einsum_form, gated_vals, out_w, preferred_element_type=jnp.float32)


def triangle_rows(pair_act, pair_ln, bias_full, res_mask, qkvg_w, out_w):
    projected = matmul_bf('ijc,cahd->aijhd', pair_ln, qkvg_w)
    logits = jnp.einsum('ijhd,ikhd->ihjk', projected[0], projected[1], preferred_element_type=jnp.float32) * (qkvg_w.shape[-1] ** -0.5) + bias_full[None] + mask_bias(res_mask)[None, None, None, :]
    attn_probs = jax.nn.softmax(logits, axis=-1).astype(jnp.bfloat16)
    attended = jnp.einsum('ihjk,ikhd->ijhd', attn_probs, projected[2], preferred_element_type=jnp.float32)
    return (pair_act + gated_out('ijhd,hdc->ijc', projected[3], attended, out_w)).astype(jnp.bfloat16)


def triangle_cols(pair_cols, pair_ln, bias_full, res_mask, qkvg_w, out_w):
    projected = matmul_bf('ijc,cahd->aijhd', pair_ln, qkvg_w)
    logits = jnp.einsum('ijhd,kjhd->jhik', projected[0], projected[1], preferred_element_type=jnp.float32) * (qkvg_w.shape[-1] ** -0.5) + bias_full[None] + mask_bias(res_mask)[None, None, None, :]
    attn_probs = jax.nn.softmax(logits, axis=-1).astype(jnp.bfloat16)
    attended = jnp.einsum('jhik,kjhd->ijhd', attn_probs, projected[2], preferred_element_type=jnp.float32)
    return (pair_cols + gated_out('ijhd,hdc->ijc', projected[3], attended, out_w)).astype(jnp.bfloat16)


def mm(left, right):
    return jnp.dot(left, right, preferred_element_type=F32)


def mm_nt(left, right):
    return lax.dot_general(left, right, (((1,), (1,)), ((), ())), preferred_element_type=F32)


def ln_rows(x):
    n = x.shape[0]
    xc = x - jnp.sum(x, axis=0, keepdims=True) * (1.0 / n)
    var = jnp.sum(xc * xc, axis=0, keepdims=True) * (1.0 / n)
    return (xc * lax.rsqrt(var + 1e-5)).astype(BF16)


def ln_lanes(x):
    n = x.shape[1]
    xc = x - jnp.sum(x, axis=1, keepdims=True) * (1.0 / n)
    var = jnp.sum(xc * xc, axis=1, keepdims=True) * (1.0 / n)
    return (xc * lax.rsqrt(var + 1e-5)).astype(BF16)


def bf16_split(value, terms):
    import numpy as np
    out = []
    for _ in range(terms):
        t = float(np.asarray(value, dtype=jnp.bfloat16))
        out.append(t)
        value = value - t
    return out


def bias_kernel(z_ref, w_ref, out_ref):
    heads = w_ref.shape[0]
    for r in range(z_ref.shape[0]):
        ln = ln_lanes(z_ref[r].astype(F32))
        out_ref[r * heads:(r + 1) * heads, :] = mm_nt(w_ref[...], ln).astype(BF16).astype(F32)


def row_kernel(m_ref, braw_ref, mask_ref, wqkvg_ref, wout_ref, wkvg_ref, m1_ref, kv_ref, g_ref, qsum_ref, bias_ref, wo_ref, q_ref, kt_ref, v_ref, y_ref, s0_ref, s1_ref, p0_ref, p1_ref, l0_ref, l1_ref, *, heads, hd):
    seqs, chans, res = m_ref.shape
    width = heads * hd
    wo_ref[...] = wout_ref[...].astype(F32).T.astype(BF16)
    for h in range(heads):
        plane = braw_ref[pl.ds(h, res, stride=heads), :]
        bias_ref[:, h * res:(h + 1) * res] = plane.T * LOG2E
    qsum_ref[...] = jnp.zeros_like(qsum_ref)
    row_project(m_ref, mask_ref, wqkvg_ref, q_ref, kt_ref, v_ref, g_ref, heads, hd)
    row_attend(bias_ref, q_ref, kt_ref, v_ref, g_ref, y_ref, s0_ref, s1_ref, p0_ref, p1_ref, l0_ref, l1_ref, heads, hd)
    row_finish(m_ref, mask_ref, wo_ref, wkvg_ref, y_ref, m1_ref, kv_ref, g_ref, qsum_ref, hd)


def row_project(m_ref, mask_ref, wqkvg_ref, q_ref, kt_ref, v_ref, g_ref, heads, hd, unroll=8):
    seqs, chans, res = m_ref.shape
    width = heads * hd
    aug = kt_ref.shape[2] - width
    terms = bf16_split(1e4 / hd ** -0.5, 3)
    rowi = lax.broadcasted_iota(jnp.int32, (aug, res), 0)
    mvec = jnp.where(rowi == 0, terms[0], jnp.where(rowi == 1, terms[1], jnp.where(rowi == 2, terms[2], 0.0)))

    def body(it, _):
        for n in range(unroll // 2):
            s0 = it * unroll + n * 2
            lns = [ln_rows(m_ref[s0 + u].astype(F32)) for u in range(2)]
            proj = mm(wqkvg_ref[...], jnp.concatenate(lns, axis=1))
            for u in range(2):
                cols = slice(u * res, (u + 1) * res)
                s = s0 + u
                q_ref[s] = proj[0:width, cols].astype(BF16)
                mrow = mask_ref[pl.ds(s, 1), :] - 1.0
                k = proj[width:2 * width, cols].astype(BF16).astype(F32)
                kt_ref[s] = jnp.concatenate([k, mrow * mvec], axis=0).T.astype(BF16)
                v_ref[s] = proj[2 * width:3 * width, cols].astype(BF16)
                g_ref[s] = proj[3 * width:, cols].astype(BF16)
        return 0

    lax.fori_loop(0, seqs // unroll, body, 0)


def row_attend(bias_ref, q_ref, kt_ref, v_ref, g_ref, y_ref, s0_ref, s1_ref, p0_ref, p1_ref, l0_ref, l1_ref, heads, hd):
    seqs, width, res = q_ref.shape
    scale2 = hd ** -0.5 * LOG2E
    npairs = heads // 2
    aug = kt_ref.shape[2] - width
    rows16 = lax.broadcasted_iota(jnp.int32, (2 * hd, res), 0)
    first = rows16 < hd
    zero16 = jnp.zeros((2 * hd, res), BF16)
    ones = jnp.ones((aug, res), BF16)

    def scores(s, s_ref):
        s = jnp.minimum(s, seqs - 1)
        kt = kt_ref[s]
        for t in range(npairs):
            q16 = q_ref[s, t * 2 * hd:(t + 1) * 2 * hd]
            qa = jnp.where(first, q16, zero16)
            qb = jnp.where(first, zero16, q16)
            left = jnp.concatenate([zero16] * t + [qa] + [zero16] * (npairs - 1 - t) + [ones], axis=0)
            right = jnp.concatenate([zero16] * t + [qb] + [zero16] * (npairs - 1 - t) + [ones], axis=0)
            s_ref[:, t * 2 * res:(t + 1) * 2 * res] = mm(kt, jnp.concatenate([left, right], axis=1))

    def soft(s_ref, p_ref, l_ref):
        for h in range(heads):
            cols = slice(h * res, (h + 1) * res)
            x = s_ref[:, cols] * scale2 + bias_ref[:, cols]
            p = jnp.exp2(x - jnp.max(x, axis=0, keepdims=True))
            l_ref[0:1, cols] = jnp.sum(p, axis=0, keepdims=True)
            p_ref[:, cols] = p.astype(BF16)

    def values(s, p_ref, l_ref):
        s = jnp.maximum(s, 0)
        outs = []
        for t in range(npairs):
            cols = slice(t * 2 * res, (t + 1) * 2 * res)
            o = mm(v_ref[s, t * 2 * hd:(t + 1) * 2 * hd], p_ref[:, cols])
            inv = 1.0 / l_ref[0:1, cols]
            outs += [o[0:hd, 0:res] * inv[:, 0:res], o[hd:2 * hd, res:2 * res] * inv[:, res:2 * res]]
        att = jnp.concatenate(outs, axis=0)
        y_ref[s] = (jax.nn.sigmoid(g_ref[s].astype(F32)) * att).astype(BF16)

    scores(0, s0_ref)

    def body(it, _):
        s = it * 2
        values(s - 1, p1_ref, l1_ref)
        scores(s + 1, s1_ref)
        soft(s0_ref, p0_ref, l0_ref)
        values(s, p0_ref, l0_ref)
        scores(s + 2, s0_ref)
        soft(s1_ref, p1_ref, l1_ref)
        return 0

    lax.fori_loop(0, seqs // 2, body, 0)
    values(seqs - 1, p1_ref, l1_ref)


def row_finish(m_ref, mask_ref, wo_ref, wkvg_ref, y_ref, m1_ref, kv_ref, g_ref, qsum_ref, hd, unroll=8):
    seqs, chans, res = m_ref.shape

    def body(it, _):
        acc = jnp.zeros((chans, res), F32)
        for n in range(unroll // 2):
            s0 = it * unroll + n * 2
            upd = mm(wo_ref[...], jnp.concatenate([y_ref[s0], y_ref[s0 + 1]], axis=1))
            ln1 = []
            for u in range(2):
                m1 = (m_ref[s0 + u].astype(F32) + upd[:, u * res:(u + 1) * res]).astype(BF16)
                m1_ref[s0 + u] = m1
                l1 = ln_rows(m1.astype(F32))
                acc = acc + l1.astype(F32) * mask_ref[pl.ds(s0 + u, 1), :]
                ln1.append(l1)
            kvg = mm(wkvg_ref[...], jnp.concatenate(ln1, axis=1)).astype(BF16)
            for u in range(2):
                kv_ref[pl.ds((s0 + u) * 2 * hd, 2 * hd), :] = kvg[0:2 * hd, u * res:(u + 1) * res].astype(F32)
                g_ref[s0 + u] = kvg[2 * hd:, u * res:(u + 1) * res]
        qsum_ref[...] += acc
        return 0

    lax.fori_loop(0, seqs // unroll, body, 0)


def col_stats(qtot, cnt, kv_ref, mask_ref, wq_ref, planes_ref, stats_ref, heads, hd):
    seqs, res = mask_ref.shape
    qbar = (qtot / (cnt + 1e-10)).astype(BF16)
    q = mm(wq_ref[...], qbar).astype(BF16).astype(F32)
    for d in range(2 * hd):
        planes_ref[d] = kv_ref[pl.ds(d, seqs, stride=2 * hd), :]
    mb = (mask_ref[...] - 1.0) * (1e4 * LOG2E)
    for h in range(heads):
        acc = q[h * hd:h * hd + 1] * planes_ref[0]
        for d in range(1, hd):
            acc = acc + q[h * hd + d:h * hd + d + 1] * planes_ref[d]
        t = acc * (hd ** -0.5 * LOG2E) + mb
        mx = jnp.max(t, axis=0, keepdims=True)
        p = jnp.exp2(t - mx)
        stats_ref[h:h + 1, :] = mx
        stats_ref[heads + h:heads + h + 1, :] = jnp.sum(p, axis=0, keepdims=True)
        pb = p.astype(BF16).astype(F32)
        for d in range(hd):
            r = 2 * heads + h * hd + d
            stats_ref[r:r + 1, :] = jnp.sum(pb * planes_ref[hd + d], axis=0, keepdims=True)


def col1_kernel(qtot_ref, fmask_ref, kv_ref, mask_ref, wq_ref, stats_ref, planes_ref, *, heads, hd):
    cnt = jnp.sum(fmask_ref[...], axis=0, keepdims=True).astype(F32)
    col_stats(qtot_ref[...], cnt, kv_ref, mask_ref, wq_ref, planes_ref, stats_ref, heads, hd)


def combine_stats(stats, heads, hd):
    gm = stats[0][0:heads]
    for st in stats[1:]:
        gm = jnp.maximum(gm, st[0:heads])
    tot = None
    wv = None
    for st in stats:
        f = jnp.exp2(st[0:heads] - gm)
        fx = jnp.concatenate([jnp.broadcast_to(f[h:h + 1], (hd, f.shape[1])) for h in range(heads)], axis=0)
        tot = f * st[heads:2 * heads] if tot is None else tot + f * st[heads:2 * heads]
        wv = fx * st[2 * heads:] if wv is None else wv + fx * st[2 * heads:]
    totx = jnp.concatenate([jnp.broadcast_to(tot[h:h + 1], (hd, tot.shape[1])) for h in range(heads)], axis=0)
    return wv / totx


def col2_kernel(stats_ref, g_ref, m1_ref, mask_ref, wout_ref, wac_ref, m2_ref, a_ref, c_ref, o_ref, wo_ref, as_ref, cs_ref, at_ref, *, heads, hd):
    seqs, chans, res = m1_ref.shape
    wide = wac_ref.shape[0] // 2
    wo_ref[...] = wout_ref[...].astype(F32).T.astype(BF16)
    o_ref[...] = combine_stats([stats_ref[d] for d in range(stats_ref.shape[0])], heads, hd)

    def pair(s0):
        ys = [(jax.nn.sigmoid(g_ref[s0 + u].astype(F32)) * o_ref[...]).astype(BF16) for u in range(2)]
        upd = mm(wo_ref[...], jnp.concatenate(ys, axis=1))
        lns = []
        for u in range(2):
            m2 = (m1_ref[s0 + u].astype(F32) + upd[:, u * res:(u + 1) * res]).astype(BF16)
            m2_ref[s0 + u] = m2
            lns.append(ln_rows(m2.astype(F32)))
        ac = mm(wac_ref[...], jnp.concatenate(lns, axis=1)).astype(BF16).astype(F32)
        for u in range(2):
            mrow = mask_ref[pl.ds(s0 + u, 1), :]
            as_ref[pl.ds((s0 + u) * wide, wide), :] = ac[0:wide, u * res:(u + 1) * res] * mrow
            cs_ref[pl.ds((s0 + u) * wide, wide), :] = ac[wide:, u * res:(u + 1) * res] * mrow

    def body(it, _):
        for n in range(4):
            pair(it * 8 + n * 2)
        return 0

    lax.fori_loop(0, seqs // 8, body, 0)

    def planes(e, _):
        c_ref[e] = cs_ref[pl.ds(e, seqs, stride=wide), :].astype(BF16)
        at_ref[pl.ds(e, res, stride=wide), :] = as_ref[pl.ds(e, seqs, stride=wide), :].T
        return 0

    lax.fori_loop(0, wide, planes, 0)
    a_ref[...] = at_ref[...].astype(BF16)


def dap_index(chip, core, chips):
    return lax.rem(chip + 2 * chips, chips) * 2 + core


def opm_kernel(a_ref, c_ref, z_ref, mask_ref, w_ref, out_ref, ap_ref, cp_ref, part_ref, xhi_ref, xlo_ref, wt_ref, w32_ref, cnt_ref, pos_ref, neg_ref, ex_send, ex_recv, send_sem, recv_sem, *, chips):
    me = lax.axis_index('dap')
    chip, core = me // 2, lax.rem(me, 2)
    wide, seqs, res = c_ref.shape
    rows = z_ref.shape[0]
    brow = rows * wide
    outc = w_ref.shape[1]
    partner = chip * 2 + 1 - core
    peer = {1: dap_index(chip + 1, core, chips), -1: dap_index(chip - 1, core, chips)}
    half_chips = chips // 2

    barrier = pltpu.get_barrier_semaphore()
    for dev in (partner, peer[1], peer[-1]):
        pl.semaphore_signal(barrier, inc=1, device_id={'dap': dev}, device_id_type=MESH)
    pl.semaphore_wait(barrier, 3)

    swaps = []
    for n, (src, dst) in enumerate(((a_ref.at[:, 1 - core], ap_ref), (c_ref, cp_ref))):
        cp = pltpu.make_async_remote_copy(src, dst, ex_send.at[n], ex_recv.at[n], device_id={'dap': partner}, device_id_type=MESH)
        cp.start()
        swaps.append(cp)

    w32_ref[...] = w_ref[...].astype(F32)
    per = 128 // wide
    for b in range(wide // per):
        cols = [w32_ref[pl.ds(b * per + f, wide, stride=wide), :] for f in range(per)]
        wt_ref[:, b * 128:(b + 1) * 128] = jnp.concatenate(cols, axis=0).T.astype(BF16)

    def count_step(n, acc):
        blk = mask_ref[pl.ds(n * 128, 128), :].astype(F32)
        return acc + mm(blk.T.astype(BF16), blk.astype(BF16))

    cnt_ref[...] = lax.fori_loop(0, mask_ref.shape[0] // 128, count_step, jnp.zeros((res, res), F32))

    for cp in swaps:
        cp.wait()

    def block(dest, slot):
        lhs = jnp.concatenate([a_ref[dest, core], ap_ref[dest]], axis=1)

        def outer(fp, _):
            f0 = fp * 2
            rhs = jnp.concatenate([
                jnp.concatenate([c_ref[f0], c_ref[f0 + 1]], axis=1),
                jnp.concatenate([cp_ref[f0], cp_ref[f0 + 1]], axis=1)], axis=0)
            o = mm(lhs, rhs)
            hi = o.astype(BF16)
            lo = (o - hi.astype(F32)).astype(BF16)
            for i in range(rows):
                for u in range(2):
                    r0 = pl.multiple_of((f0 + u) * wide, wide)
                    src = (slice(i * wide, (i + 1) * wide), slice(u * res, (u + 1) * res))
                    xhi_ref[i // 2, pl.ds(r0, wide), (i % 2) * res:(i % 2 + 1) * res] = hi[src]
                    xlo_ref[i // 2, pl.ds(r0, wide), (i % 2) * res:(i % 2 + 1) * res] = lo[src]
            return 0

        lax.fori_loop(0, wide // 2, outer, 0)

        def inner(n, _):
            part_ref[slot, n] = mm(wt_ref[...], xhi_ref[n]) + mm(wt_ref[...], xlo_ref[n])
            return 0

        lax.fori_loop(0, rows // 2, inner, 0)

    sends = []
    arrivals = {}
    bufs = {1: pos_ref, -1: neg_ref}
    hq = rows // 4

    def hops(d, half):
        return half_chips if (half == 1) == (d == 1) else half_chips - 1

    slot_of = {}
    nbuf = 2 * half_chips - 1

    def buf_index(d, half, k):
        return (k - 1) + (0 if (half == 1) == (d == 1) else half_chips)

    def message(d, half, k, slot):
        idx = buf_index(d, half, k)
        src = part_ref.at[slot, pl.ds(half * hq, hq)]
        cp = pltpu.make_async_remote_copy(src, bufs[d].at[idx], send_sem.at[(d + 1) // 2, idx], recv_sem.at[(d + 1) // 2, idx], device_id={'dap': peer[d]}, device_id_type=MESH)
        arrivals[(d, half, k)] = cp
        sends.append(cp)
        cp.start()

    def take(d, half, k, slot):
        arrivals[(d, half, k)].wait_recv()
        part_ref[slot, half * hq:(half + 1) * hq] += bufs[d][buf_index(d, half, k)]

    def relay(d, k, slot):
        for half in ((0, 1) if d == 1 else (1, 0)):
            if k < hops(d, half):
                take(d, half, k + 1, slot)
            if k <= hops(d, half):
                message(d, half, k, slot)

    def dest_of(d, k):
        return lax.rem(chip + d * k + 2 * chips, chips)

    far = half_chips
    block(dest_of(1, far), 0)
    message(1, 1, far, 0)
    message(-1, 0, far, 0)
    slot = 1
    pending = []
    for k in range(far - 1, 0, -1):
        for d in (1, -1):
            block(dest_of(d, k), slot)
            if k == far - 1:
                message(d, 0 if d == 1 else 1, k, slot)
                pending.append((d, slot))
            else:
                relay(d, k, slot)
            slot += 1
        if k == far - 1:
            for d, sl in pending:
                half = 1 if d == 1 else 0
                take(d, half, far, sl)
                message(d, half, k, sl)
    block(chip, slot)
    for half in (0, 1):
        for d in (1, -1):
            take(d, half, 1, slot)
    for n in range(rows // 2):
        pair = part_ref[slot, n]
        for u in range(2):
            i = n * 2 + u
            cnt = cnt_ref[pl.ds(me * rows + i, 1), :] + 1e-3
            upd = (pair[:, u * res:(u + 1) * res] / cnt).T
            out_ref[i] = (z_ref[i].astype(F32) + upd).astype(BF16)
    for cp in sends:
        cp.wait_send()


def vspec():
    return pl.BlockSpec(memory_space=VMEM)


def call(kernel, outs, n_in, scratch, name, cid=None, flops=10 ** 9):
    params = dict(vmem_limit_bytes=60 * 2 ** 20)
    if cid is not None:
        params.update(collective_id=cid, has_side_effects=True)
    return pl.pallas_call(
        kernel,
        out_shape=outs,
        in_specs=[vspec()] * n_in,
        out_specs=jax.tree.map(lambda _: vspec(), outs),
        scratch_shapes=scratch,
        compiler_params=pltpu.CompilerParams(**params),
        cost_estimate=pl.CostEstimate(flops=flops, bytes_accessed=10 ** 6, transcendentals=0),
        name=name,
    )


def sds(shape, dtype):
    return jax.ShapeDtypeStruct(shape, dtype)


def solution(mesh):
    ndap = mesh.shape['dap']
    chips = ndap // 2

    def evoformer_block(msa, pair_act, full_mask, res_mask, row_bias_w, row_qkvg_w, row_out_w, col_query_w, col_kv_w, col_gate_w, col_out_w, opm_proj_w, opm_out_w, start_bias_w, start_qkvg_w, start_out_w, end_bias_w, end_qkvg_w, end_out_w):
        seqs, res, chans = msa.shape
        rows = pair_act.shape[0]
        heads, hd = row_qkvg_w.shape[2], row_qkvg_w.shape[3]
        width = heads * hd
        wide = opm_proj_w.shape[2]
        outc = opm_out_w.shape[2]
        me = lax.axis_index('dap')
        mask = lax.dynamic_slice_in_dim(full_mask, me * seqs, seqs, axis=0).astype(F32)
        m_t = jnp.swapaxes(msa, 1, 2)
        wt = lambda w: w.reshape(w.shape[0], -1).T

        braw = call(bias_kernel, sds((rows * heads, res), F32), 2, [], 'row_bias')(pair_act, row_bias_w.T)
        braw = lax.all_gather(braw, 'dap', axis=0, tiled=True)

        wkvg = jnp.concatenate([wt(col_kv_w), wt(col_gate_w)], axis=0)
        m1, kv, g, qsum = call(
            functools.partial(row_kernel, heads=heads, hd=hd),
            [sds((seqs, chans, res), BF16), sds((seqs * 2 * hd, res), F32), sds((seqs, width, res), BF16), sds((chans, res), F32)], 6,
            [VMEM((res, heads * res), F32), VMEM((chans, width), BF16),
             VMEM((seqs, width, res), BF16), VMEM((seqs, res, width + 16), BF16), VMEM((seqs, width, res), BF16), VMEM((seqs, width, res), BF16),
             VMEM((res, heads * res), F32), VMEM((res, heads * res), F32), VMEM((res, heads * res), BF16), VMEM((res, heads * res), BF16),
             VMEM((8, heads * res), F32), VMEM((8, heads * res), F32)], 'row_attention',
        )(m_t, braw, mask, wt(row_qkvg_w), row_out_w.reshape(width, chans), wkvg)

        qtot = lax.psum(qsum, 'dap')
        nstat = 2 * heads + width
        stats = call(
            functools.partial(col1_kernel, heads=heads, hd=hd),
            sds((nstat, res), F32), 5, [VMEM((2 * hd, seqs, res), F32)], 'col_stats',
        )(qtot, full_mask, kv, mask, wt(col_query_w))
        stats = lax.all_gather(stats, 'dap', axis=0)

        m2, a, c = call(
            functools.partial(col2_kernel, heads=heads, hd=hd),
            [sds((seqs, chans, res), BF16), sds((res * wide, seqs), BF16), sds((wide, seqs, res), BF16)], 6,
            [VMEM((width, res), F32), VMEM((chans, width), BF16), VMEM((seqs * wide, res), F32), VMEM((seqs * wide, res), F32), VMEM((res * wide, seqs), F32)], 'col_out',
        )(stats, g, m1, mask, col_out_w.reshape(width, chans), wt(opm_proj_w))
        msa_out = jnp.swapaxes(m2, 1, 2)

        npair = rows // 2
        nbuf = 2 * (chips // 2) - 1
        pair_act = call(
            functools.partial(opm_kernel, chips=chips),
            sds(pair_act.shape, BF16), 5,
            [VMEM((chips, rows * wide, seqs), BF16), VMEM((wide, seqs, res), BF16),
             VMEM((chips, npair, outc, 2 * res), F32),
             VMEM((npair, wide * wide, 2 * res), BF16), VMEM((npair, wide * wide, 2 * res), BF16),
             VMEM((outc, wide * wide), BF16), VMEM((wide * wide, outc), F32), VMEM((res, res), F32),
             VMEM((nbuf, npair // 2, outc, 2 * res), F32), VMEM((nbuf, npair // 2, outc, 2 * res), F32),
             pltpu.SemaphoreType.DMA((2,)), pltpu.SemaphoreType.DMA((2,)),
             pltpu.SemaphoreType.DMA((2, nbuf)), pltpu.SemaphoreType.DMA((2, nbuf))],
            'outer_mean', cid=1,
        )(a.reshape(chips, 2, rows * wide, seqs), c, pair_act, full_mask, opm_out_w.reshape(wide * wide, outc))

        pair_ln = layer_norm(pair_act)
        start_full = lax.all_gather(matmul_bf('ijc,ch->hij', pair_ln, start_bias_w), 'dap', axis=1, tiled=True)
        pair_act = triangle_rows(pair_act, pair_ln, start_full, res_mask, start_qkvg_w, start_out_w)

        pair_cols = lax.all_to_all(pair_act, 'dap', 1, 0, tiled=True)
        cols_ln = layer_norm(pair_cols)
        end_full = lax.all_gather(matmul_bf('ijc,ch->hji', cols_ln, end_bias_w), 'dap', axis=1, tiled=True)
        pair_cols = triangle_cols(pair_cols, cols_ln, end_full, res_mask, end_qkvg_w, end_out_w)
        pair_out = lax.all_to_all(pair_cols, 'dap', 0, 1, tiled=True)
        return msa_out, pair_out

    row_spec = P(('data', 'dap'), None, None)
    in_specs = (row_spec, row_spec, P('data', None), P('data')) + (P(),) * 15
    return jax.shard_map(evoformer_block, mesh=mesh, in_specs=in_specs, out_specs=(row_spec, row_spec), check_vma=False)
```

```python
import functools
import math

import jax
import jax.numpy as jnp
from jax import lax
from jax.experimental import pallas as pl
from jax.experimental.pallas import tpu as pltpu
from jax.sharding import PartitionSpec as P

F32 = jnp.float32
BF16 = jnp.bfloat16
MESH = pl.DeviceIdType.MESH
LOG2E = math.log2(math.e)
VMEM = pltpu.VMEM


def mm(left, right):
    return jnp.dot(left, right, preferred_element_type=F32)


def mm_nt(left, right):
    return lax.dot_general(left, right, (((1,), (1,)), ((), ())), preferred_element_type=F32)


def ln_rows(x):
    n = x.shape[0]
    xc = x - jnp.sum(x, axis=0, keepdims=True) * (1.0 / n)
    var = jnp.sum(xc * xc, axis=0, keepdims=True) * (1.0 / n)
    return (xc * lax.rsqrt(var + 1e-5)).astype(BF16)


def ln_lanes(x):
    n = x.shape[1]
    xc = x - jnp.sum(x, axis=1, keepdims=True) * (1.0 / n)
    var = jnp.sum(xc * xc, axis=1, keepdims=True) * (1.0 / n)
    return (xc * lax.rsqrt(var + 1e-5)).astype(BF16)


def bf16_split(value, terms):
    import numpy as np
    out = []
    for _ in range(terms):
        t = float(np.asarray(value, dtype=jnp.bfloat16))
        out.append(t)
        value = value - t
    return out


def group_barrier(me, ndap):
    barrier = pltpu.get_barrier_semaphore()
    for k in range(1, ndap):
        pl.semaphore_signal(barrier, inc=1, device_id={'dap': lax.rem(me + k, ndap)}, device_id_type=MESH)
    pl.semaphore_wait(barrier, ndap - 1)


def far_first(ndap):
    return sorted(range(1, ndap), key=lambda k: -min(k, ndap - k))


def start_gather(src_ref, all_ref, me, ndap, send_sem, recv_sem):
    copies = []
    for k in far_first(ndap):
        cp = pltpu.make_async_remote_copy(src_ref, all_ref.at[me], send_sem.at[k], recv_sem.at[k], device_id={'dap': lax.rem(me + k, ndap)}, device_id_type=MESH)
        cp.start()
        copies.append(cp)
    all_ref[me] = src_ref[...]
    return copies


def start_swap(send_ref, recv_ref, me, ndap, send_sem, recv_sem):
    copies = []
    for k in far_first(ndap):
        other = lax.rem(me + k, ndap)
        cp = pltpu.make_async_remote_copy(send_ref.at[other], recv_ref.at[me], send_sem.at[k], recv_sem.at[k], device_id={'dap': other}, device_id_type=MESH)
        cp.start()
        copies.append(cp)
    recv_ref[me] = send_ref[me]
    return copies


def finish(copies):
    for cp in copies:
        cp.wait_recv()


def drain(copies):
    for cp in copies:
        cp.wait_send()


def pair_bias(z_ref, w_ref, out_ref):
    heads = w_ref.shape[0]
    for r in range(z_ref.shape[0]):
        ln = ln_lanes(z_ref[r].astype(F32))
        out_ref[r * heads:(r + 1) * heads, :] = mm_nt(w_ref[...], ln).astype(BF16).astype(F32)


def row_project(m_ref, mask_ref, wqkvg_ref, q_ref, kt_ref, v_ref, g_ref, heads, hd, unroll=8):
    seqs, chans, res = m_ref.shape
    width = heads * hd
    aug = kt_ref.shape[2] - width
    terms = bf16_split(1e4 / hd ** -0.5, 3)
    rowi = lax.broadcasted_iota(jnp.int32, (aug, res), 0)
    mvec = jnp.where(rowi == 0, terms[0], jnp.where(rowi == 1, terms[1], jnp.where(rowi == 2, terms[2], 0.0)))

    def body(it, _):
        for n in range(unroll // 2):
            s0 = it * unroll + n * 2
            lns = [ln_rows(m_ref[s0 + u].astype(F32)) for u in range(2)]
            proj = mm(wqkvg_ref[...], jnp.concatenate(lns, axis=1))
            for u in range(2):
                cols = slice(u * res, (u + 1) * res)
                s = s0 + u
                q_ref[s] = proj[0:width, cols].astype(BF16)
                mrow = mask_ref[pl.ds(s, 1), :] - 1.0
                k = proj[width:2 * width, cols].astype(BF16).astype(F32)
                kt_ref[s] = jnp.concatenate([k, mrow * mvec], axis=0).T.astype(BF16)
                v_ref[s] = proj[2 * width:3 * width, cols].astype(BF16)
                g_ref[s] = proj[3 * width:, cols].astype(BF16)
        return 0

    lax.fori_loop(0, seqs // unroll, body, 0)


def row_attend(bias_ref, q_ref, kt_ref, v_ref, g_ref, y_ref, s0_ref, s1_ref, p0_ref, p1_ref, l0_ref, l1_ref, heads, hd):
    seqs, width, res = q_ref.shape
    scale2 = hd ** -0.5 * LOG2E
    npairs = heads // 2
    aug = kt_ref.shape[2] - width
    rows16 = lax.broadcasted_iota(jnp.int32, (2 * hd, res), 0)
    first = rows16 < hd
    zero16 = jnp.zeros((2 * hd, res), BF16)
    ones = jnp.ones((aug, res), BF16)

    def scores(s, s_ref):
        s = jnp.minimum(s, seqs - 1)
        kt = kt_ref[s]
        for t in range(npairs):
            q16 = q_ref[s, t * 2 * hd:(t + 1) * 2 * hd]
            qa = jnp.where(first, q16, zero16)
            qb = jnp.where(first, zero16, q16)
            left = jnp.concatenate([zero16] * t + [qa] + [zero16] * (npairs - 1 - t) + [ones], axis=0)
            right = jnp.concatenate([zero16] * t + [qb] + [zero16] * (npairs - 1 - t) + [ones], axis=0)
            s_ref[:, t * 2 * res:(t + 1) * 2 * res] = mm(kt, jnp.concatenate([left, right], axis=1))

    def soft(s_ref, p_ref, l_ref):
        for h in range(heads):
            cols = slice(h * res, (h + 1) * res)
            x = s_ref[:, cols] * scale2 + bias_ref[:, cols]
            p = jnp.exp2(x - jnp.max(x, axis=0, keepdims=True))
            l_ref[0:1, cols] = jnp.sum(p, axis=0, keepdims=True)
            p_ref[:, cols] = p.astype(BF16)

    def values(s, p_ref, l_ref):
        s = jnp.maximum(s, 0)
        outs = []
        for t in range(npairs):
            cols = slice(t * 2 * res, (t + 1) * 2 * res)
            o = mm(v_ref[s, t * 2 * hd:(t + 1) * 2 * hd], p_ref[:, cols])
            inv = 1.0 / l_ref[0:1, cols]
            outs += [o[0:hd, 0:res] * inv[:, 0:res], o[hd:2 * hd, res:2 * res] * inv[:, res:2 * res]]
        att = jnp.concatenate(outs, axis=0)
        y_ref[s] = (jax.nn.sigmoid(g_ref[s].astype(F32)) * att).astype(BF16)

    scores(0, s0_ref)

    def body(it, _):
        s = it * 2
        values(s - 1, p1_ref, l1_ref)
        scores(s + 1, s1_ref)
        soft(s0_ref, p0_ref, l0_ref)
        values(s, p0_ref, l0_ref)
        scores(s + 2, s0_ref)
        soft(s1_ref, p1_ref, l1_ref)
        return 0

    lax.fori_loop(0, seqs // 2, body, 0)
    values(seqs - 1, p1_ref, l1_ref)


def row_finish(m_ref, mask_ref, wo_ref, wkvg_ref, y_ref, m1_ref, kv_ref, g_ref, qsum_ref, hd, unroll=8):
    seqs, chans, res = m_ref.shape

    def body(it, _):
        acc = jnp.zeros((chans, res), F32)
        for n in range(unroll // 2):
            s0 = it * unroll + n * 2
            upd = mm(wo_ref[...], jnp.concatenate([y_ref[s0], y_ref[s0 + 1]], axis=1))
            ln1 = []
            for u in range(2):
                m1 = (m_ref[s0 + u].astype(F32) + upd[:, u * res:(u + 1) * res]).astype(BF16)
                m1_ref[s0 + u] = m1
                l1 = ln_rows(m1.astype(F32))
                acc = acc + l1.astype(F32) * mask_ref[pl.ds(s0 + u, 1), :]
                ln1.append(l1)
            kvg = mm(wkvg_ref[...], jnp.concatenate(ln1, axis=1)).astype(BF16)
            for u in range(2):
                kv_ref[pl.ds((s0 + u) * 2 * hd, 2 * hd), :] = kvg[0:2 * hd, u * res:(u + 1) * res].astype(F32)
                g_ref[s0 + u] = kvg[2 * hd:, u * res:(u + 1) * res]
        qsum_ref[...] += acc
        return 0

    lax.fori_loop(0, seqs // unroll, body, 0)


def col_stats(qtot, cnt, mask_ref, wq_ref, planes_ref, stats_ref, heads, hd):
    seqs, res = mask_ref.shape
    qbar = (qtot / (cnt + 1e-10)).astype(BF16)
    q = mm(wq_ref[...], qbar).astype(BF16).astype(F32)
    mb = (mask_ref[...] - 1.0) * (1e4 * LOG2E)
    for h in range(heads):
        acc = q[h * hd:h * hd + 1] * planes_ref[0]
        for d in range(1, hd):
            acc = acc + q[h * hd + d:h * hd + d + 1] * planes_ref[d]
        t = acc * (hd ** -0.5 * LOG2E) + mb
        mx = jnp.max(t, axis=0, keepdims=True)
        p = jnp.exp2(t - mx)
        stats_ref[h:h + 1, :] = mx
        stats_ref[heads + h:heads + h + 1, :] = jnp.sum(p, axis=0, keepdims=True)
        pb = p.astype(BF16).astype(F32)
        for d in range(hd):
            r = 2 * heads + h * hd + d
            stats_ref[r:r + 1, :] = jnp.sum(pb * planes_ref[hd + d], axis=0, keepdims=True)


def combine_stats(stats, heads, hd):
    gm = stats[0][0:heads]
    for st in stats[1:]:
        gm = jnp.maximum(gm, st[0:heads])
    tot = None
    wv = None
    for st in stats:
        f = jnp.exp2(st[0:heads] - gm)
        fx = jnp.concatenate([jnp.broadcast_to(f[h:h + 1], (hd, f.shape[1])) for h in range(heads)], axis=0)
        tot = f * st[heads:2 * heads] if tot is None else tot + f * st[heads:2 * heads]
        wv = fx * st[2 * heads:] if wv is None else wv + fx * st[2 * heads:]
    totx = jnp.concatenate([jnp.broadcast_to(tot[h:h + 1], (hd, tot.shape[1])) for h in range(heads)], axis=0)
    return wv / totx


def col_finish(g_ref, m1_ref, mask_ref, wac_ref, m2_ref, a_ref, c_ref, o_ref, wo_ref, as_ref, cs_ref, at_ref):
    seqs, chans, res = m1_ref.shape
    wide = wac_ref.shape[0] // 2

    def pair(s0):
        ys = [(jax.nn.sigmoid(g_ref[s0 + u].astype(F32)) * o_ref[...]).astype(BF16) for u in range(2)]
        upd = mm(wo_ref[...], jnp.concatenate(ys, axis=1))
        lns = []
        for u in range(2):
            m2 = (m1_ref[s0 + u].astype(F32) + upd[:, u * res:(u + 1) * res]).astype(BF16)
            m2_ref[s0 + u] = m2
            lns.append(ln_rows(m2.astype(F32)))
        ac = mm(wac_ref[...], jnp.concatenate(lns, axis=1)).astype(BF16).astype(F32)
        for u in range(2):
            mrow = mask_ref[pl.ds(s0 + u, 1), :]
            as_ref[pl.ds((s0 + u) * wide, wide), :] = ac[0:wide, u * res:(u + 1) * res] * mrow
            cs_ref[pl.ds((s0 + u) * wide, wide), :] = ac[wide:, u * res:(u + 1) * res] * mrow

    def body(it, _):
        for n in range(4):
            pair(it * 8 + n * 2)
        return 0

    lax.fori_loop(0, seqs // 8, body, 0)

    def planes(it, _):
        for n in range(4):
            e = it * 4 + n
            c_ref[e] = cs_ref[pl.ds(e, seqs, stride=wide), :].astype(BF16)
            at_ref[pl.ds(e, res, stride=wide), :] = as_ref[pl.ds(e, seqs, stride=wide), :].T
        return 0

    lax.fori_loop(0, wide // 4, planes, 0)
    per = a_ref.shape[2]
    for b in range(a_ref.shape[0]):
        for u in range(2):
            r0 = (b * 2 + u) * per
            a_ref[b, u] = at_ref[r0:r0 + per, :].astype(BF16)


def msa_kernel(m_ref, z_ref, fmask_ref, wb_ref, wqkvg_ref, wout_ref, wq_ref, wkv_ref, wg_ref, wcout_ref, wac_ref,
               m2_ref, a_ref, c_ref,
               bsend_ref, ball_ref, qsum_ref, qall_ref, stat_ref, sall_ref, m1_ref, mask_ref, bias_ref, wo_ref, wco_ref, wkvg_ref,
               q_ref, kt_ref, v_ref, g_ref, y_ref, s0_ref, s1_ref, p0_ref, p1_ref, l0_ref, l1_ref, kv_ref, planes_ref, o_ref, as_ref, cs_ref, at_ref,
               send_sem, recv_sem, *, ndap, heads, hd):
    seqs, chans, res = m_ref.shape
    me = lax.axis_index('dap')
    pair_bias(z_ref, wb_ref, bsend_ref)
    group_barrier(me, ndap)
    bias_copies = start_gather(bsend_ref, ball_ref, me, ndap, send_sem.at[0], recv_sem.at[0])
    mask_ref[...] = fmask_ref[pl.ds(me * seqs, seqs), :].astype(F32)
    wo_ref[...] = wout_ref[...].astype(F32).T.astype(BF16)
    wco_ref[...] = wcout_ref[...].astype(F32).T.astype(BF16)
    wkvg_ref[0:2 * hd] = wkv_ref[...]
    wkvg_ref[2 * hd:] = wg_ref[...]
    qsum_ref[...] = jnp.zeros_like(qsum_ref)
    row_project(m_ref, mask_ref, wqkvg_ref, q_ref, kt_ref, v_ref, g_ref, heads, hd)
    finish(bias_copies)
    flat = ball_ref.reshape(ndap * bsend_ref.shape[0], res)
    for h in range(heads):
        bias_ref[:, h * res:(h + 1) * res] = flat[pl.ds(h, res, stride=heads), :].T * LOG2E
    row_attend(bias_ref, q_ref, kt_ref, v_ref, g_ref, y_ref, s0_ref, s1_ref, p0_ref, p1_ref, l0_ref, l1_ref, heads, hd)
    row_finish(m_ref, mask_ref, wo_ref, wkvg_ref, y_ref, m1_ref, kv_ref, g_ref, qsum_ref, hd)

    sum_copies = start_gather(qsum_ref, qall_ref, me, ndap, send_sem.at[1], recv_sem.at[1])
    cnt = jnp.sum(fmask_ref[...], axis=0, keepdims=True).astype(F32)
    for d in range(2 * hd):
        planes_ref[d] = kv_ref[pl.ds(d, seqs, stride=2 * hd), :]
    finish(sum_copies)
    qtot = qall_ref[0]
    for d in range(1, ndap):
        qtot = qtot + qall_ref[d]
    col_stats(qtot, cnt, mask_ref, wq_ref, planes_ref, stat_ref, heads, hd)

    stat_copies = start_gather(stat_ref, sall_ref, me, ndap, send_sem.at[2], recv_sem.at[2])
    finish(stat_copies)
    o_ref[...] = combine_stats([sall_ref[d] for d in range(ndap)], heads, hd)
    col_finish(g_ref, m1_ref, mask_ref, wac_ref, m2_ref, a_ref, c_ref, o_ref, wco_ref, as_ref, cs_ref, at_ref)
    drain(bias_copies + sum_copies + stat_copies)


def dap_index(chip, core, chips):
    return lax.rem(chip + 2 * chips, chips) * 2 + core


def outer_mean(me, a_ref, c_ref, z_ref, mask_ref, w_ref, zs_ref, ap_ref, cp_ref, part_ref, xhi_ref, xlo_ref, wt_ref, w32_ref, cnt_ref, pos_ref, neg_ref, ex_send, ex_recv, send_sem, recv_sem, chips):
    chip, core = me // 2, lax.rem(me, 2)
    wide, seqs, res = c_ref.shape
    rows = z_ref.shape[0]
    brow = rows * wide
    outc = w_ref.shape[1]
    partner = chip * 2 + 1 - core
    peer = {1: dap_index(chip + 1, core, chips), -1: dap_index(chip - 1, core, chips)}
    half_chips = chips // 2

    swaps = []
    for n, (src, dst) in enumerate(((a_ref.at[:, 1 - core], ap_ref), (c_ref, cp_ref))):
        cp = pltpu.make_async_remote_copy(src, dst, ex_send.at[n], ex_recv.at[n], device_id={'dap': partner}, device_id_type=MESH)
        cp.start()
        swaps.append(cp)

    w32_ref[...] = w_ref[...].astype(F32)
    per = 128 // wide
    for b in range(wide // per):
        cols = [w32_ref[pl.ds(b * per + f, wide, stride=wide), :] for f in range(per)]
        wt_ref[:, b * 128:(b + 1) * 128] = jnp.concatenate(cols, axis=0).T.astype(BF16)

    def count_step(n, acc):
        blk = mask_ref[pl.ds(n * 128, 128), :].astype(F32)
        return acc + mm(blk.T.astype(BF16), blk.astype(BF16))

    cnt_ref[...] = lax.fori_loop(0, mask_ref.shape[0] // 128, count_step, jnp.zeros((res, res), F32))

    for cp in swaps:
        cp.wait()

    def block(dest, slot):
        lhs = jnp.concatenate([a_ref[dest, core], ap_ref[dest]], axis=1)

        def outer(fp, _):
            f0 = fp * 2
            rhs = jnp.concatenate([
                jnp.concatenate([c_ref[f0], c_ref[f0 + 1]], axis=1),
                jnp.concatenate([cp_ref[f0], cp_ref[f0 + 1]], axis=1)], axis=0)
            o = mm(lhs, rhs)
            hi = o.astype(BF16)
            lo = (o - hi.astype(F32)).astype(BF16)
            for i in range(rows):
                for u in range(2):
                    r0 = pl.multiple_of((f0 + u) * wide, wide)
                    src = (slice(i * wide, (i + 1) * wide), slice(u * res, (u + 1) * res))
                    xhi_ref[i // 2, pl.ds(r0, wide), (i % 2) * res:(i % 2 + 1) * res] = hi[src]
                    xlo_ref[i // 2, pl.ds(r0, wide), (i % 2) * res:(i % 2 + 1) * res] = lo[src]
            return 0

        lax.fori_loop(0, wide // 2, outer, 0)

        def inner(n, _):
            part_ref[slot, n] = mm(wt_ref[...], xhi_ref[n]) + mm(wt_ref[...], xlo_ref[n])
            return 0

        lax.fori_loop(0, rows // 2, inner, 0)

    sends = []
    arrivals = {}
    bufs = {1: pos_ref, -1: neg_ref}
    hq = rows // 4

    def hops(d, half):
        return half_chips if (half == 1) == (d == 1) else half_chips - 1

    slot_of = {}
    nbuf = 2 * half_chips - 1

    def buf_index(d, half, k):
        return (k - 1) + (0 if (half == 1) == (d == 1) else half_chips)

    def message(d, half, k, slot):
        idx = buf_index(d, half, k)
        src = part_ref.at[slot, pl.ds(half * hq, hq)]
        cp = pltpu.make_async_remote_copy(src, bufs[d].at[idx], send_sem.at[(d + 1) // 2, idx], recv_sem.at[(d + 1) // 2, idx], device_id={'dap': peer[d]}, device_id_type=MESH)
        arrivals[(d, half, k)] = cp
        sends.append(cp)
        cp.start()

    def take(d, half, k, slot):
        arrivals[(d, half, k)].wait_recv()
        part_ref[slot, half * hq:(half + 1) * hq] += bufs[d][buf_index(d, half, k)]

    def relay(d, k, slot):
        for half in ((0, 1) if d == 1 else (1, 0)):
            if k < hops(d, half):
                take(d, half, k + 1, slot)
            if k <= hops(d, half):
                message(d, half, k, slot)

    def dest_of(d, k):
        return lax.rem(chip + d * k + 2 * chips, chips)

    far = half_chips
    block(dest_of(1, far), 0)
    message(1, 1, far, 0)
    message(-1, 0, far, 0)
    slot = 1
    pending = []
    for k in range(far - 1, 0, -1):
        for d in (1, -1):
            block(dest_of(d, k), slot)
            if k == far - 1:
                message(d, 0 if d == 1 else 1, k, slot)
                pending.append((d, slot))
            else:
                relay(d, k, slot)
            slot += 1
        if k == far - 1:
            for d, sl in pending:
                half = 1 if d == 1 else 0
                take(d, half, far, sl)
                message(d, half, k, sl)
    block(chip, slot)
    for half in (0, 1):
        for d in (1, -1):
            take(d, half, 1, slot)
    for n in range(rows // 2):
        pair = part_ref[slot, n]
        for u in range(2):
            i = n * 2 + u
            cnt = cnt_ref[pl.ds(me * rows + i, 1), :] + 1e-3
            upd = (pair[:, u * res:(u + 1) * res] / cnt).T
            zs_ref[i * res:(i + 1) * res, :] = (z_ref[i].astype(F32) + upd).astype(BF16).astype(F32)
    return sends


def tri_bias(zs_ref, ln_ref, w_ref, out_ref, rows, res):
    heads = w_ref.shape[0]
    for r in range(0, rows, 2):
        b = []
        for u in range(2):
            ln = ln_lanes(zs_ref[(r + u) * res:(r + u + 1) * res, :])
            if ln_ref is not None:
                ln_ref[(r + u) * res:(r + u + 1) * res, :] = ln
            b.append(mm_nt(w_ref[...], ln)[0:heads].astype(BF16).astype(F32))
        out_ref[r * heads:(r + 2) * heads, :] = jnp.concatenate(b, axis=0)


def tri_project(ln_ref, w_ref, proj_ref):
    step = 256
    for r in range(0, ln_ref.shape[0], step):
        proj_ref[r:r + step, :] = mm_nt(ln_ref[r:r + step, :], w_ref[...]).astype(BF16)


def tri_attend(zs_ref, proj_ref, bias_ref, wout_ref, heads, rows, res):
    width = proj_ref.shape[1] // 4
    hd = width // heads
    scale2 = hd ** -0.5 * LOG2E
    lane = lax.broadcasted_iota(jnp.int32, (res, width), 1)
    mine = [(lane >= h * hd) & (lane < (h + 1) * hd) for h in range(heads)]
    zero = jnp.zeros((res, width), BF16)

    def one(r0):
        part = lambda n: proj_ref[pl.ds(r0, res), n * width:(n + 1) * width]
        q, k, v, g = part(0), part(1), part(2), part(3)
        s = mm_nt(q, jnp.concatenate([jnp.where(mine[h], k, zero) for h in range(heads)], axis=0))
        ps = []
        for h in range(heads):
            cols = slice(h * res, (h + 1) * res)
            x = s[:, cols] * scale2 + bias_ref[:, cols]
            p = jnp.exp2(x - jnp.max(x, axis=1, keepdims=True))
            ps.append((p * (1.0 / jnp.sum(p, axis=1, keepdims=True))).astype(BF16))
        o = mm(jnp.concatenate(ps, axis=1), jnp.concatenate([jnp.where(mine[h], v, zero) for h in range(heads)], axis=0))
        y = (jax.nn.sigmoid(g.astype(F32)) * o).astype(BF16)
        upd = mm(y, wout_ref[...])
        zs_ref[pl.ds(r0, res), :] = (zs_ref[pl.ds(r0, res), :] + upd).astype(BF16).astype(F32)

    def body(it, _):
        for n in range(4):
            one(pl.multiple_of((it * 4 + n) * res, res))
        return 0

    lax.fori_loop(0, rows // 4, body, 0)


def pack_blocks(zs_ref, send_ref, rows, res, ndap):
    def one(q, _):
        parts = [zs_ref[pl.ds(q * rows + u, rows, stride=res), :] for u in range(rows)]
        send_ref[q] = jnp.concatenate(parts, axis=0).astype(BF16)
        return 0

    lax.fori_loop(0, ndap, one, 0)


def unpack_blocks(recv_ref, put, rows, ndap):
    for p in range(ndap):
        blk = recv_ref[p].astype(F32)
        for u in range(rows):
            put(u, p, blk[u * rows:(u + 1) * rows, :])


def pair_kernel(a_ref, c_ref, z_ref, mask_ref, rmask_ref, w_ref, wsb_ref, wsp_ref, wso_ref, web_ref, wep_ref, weo_ref,
                out_ref,
                ap_ref, cp_ref, part_ref, xhi_ref, xlo_ref, wt_ref, w32_ref, cnt_ref, pos_ref, neg_ref,
                zs_ref, zc_ref, ln_ref, proj_ref, bias_ref, sb_ref, sball_ref, eb_ref, eball_ref, xs_ref, xr_ref, ys_ref, yr_ref,
                ex_send, ex_recv, ring_send, ring_recv, send_sem, recv_sem, *, chips):
    ndap = 2 * chips
    me = lax.axis_index('dap')
    rows, res, _ = z_ref.shape
    heads = wsb_ref.shape[0]
    group_barrier(me, ndap)
    sends = outer_mean(me, a_ref, c_ref, z_ref, mask_ref, w_ref, zs_ref, ap_ref, cp_ref, part_ref, xhi_ref, xlo_ref, wt_ref, w32_ref, cnt_ref, pos_ref, neg_ref, ex_send, ex_recv, ring_send, ring_recv, chips)
    kmask = (rmask_ref[...].astype(F32) - 1.0) * 1e4

    tri_bias(zs_ref, ln_ref, wsb_ref, sb_ref, rows, res)
    c1 = start_gather(sb_ref, sball_ref, me, ndap, send_sem.at[0], recv_sem.at[0])
    tri_project(ln_ref, wsp_ref, proj_ref)
    finish(c1)
    flat = sball_ref.reshape(res * heads, res)
    for h in range(heads):
        bias_ref[:, h * res:(h + 1) * res] = (flat[pl.ds(h, res, stride=heads), :] + kmask) * LOG2E
    tri_attend(zs_ref, proj_ref, bias_ref, wso_ref, heads, rows, res)

    pack_blocks(zs_ref, xs_ref, rows, res, ndap)
    c2 = start_swap(xs_ref, xr_ref, me, ndap, send_sem.at[1], recv_sem.at[1])
    tri_bias(zs_ref, None, web_ref, eb_ref, rows, res)
    c3 = start_gather(eb_ref, eball_ref, me, ndap, send_sem.at[2], recv_sem.at[2])
    finish(c2)

    def put_col(u, p, val):
        zc_ref[u * res + p * rows:u * res + (p + 1) * rows, :] = val

    unpack_blocks(xr_ref, put_col, rows, ndap)
    for r in range(rows):
        ln_ref[r * res:(r + 1) * res, :] = ln_lanes(zc_ref[r * res:(r + 1) * res, :])
    tri_project(ln_ref, wep_ref, proj_ref)
    finish(c3)
    flat = eball_ref.reshape(res * heads, res)
    for h in range(heads):
        bias_ref[:, h * res:(h + 1) * res] = (flat[pl.ds(h, res, stride=heads), :].T + kmask) * LOG2E
    tri_attend(zc_ref, proj_ref, bias_ref, weo_ref, heads, rows, res)

    pack_blocks(zc_ref, ys_ref, rows, res, ndap)
    c4 = start_swap(ys_ref, yr_ref, me, ndap, send_sem.at[3], recv_sem.at[3])
    finish(c4)

    def put_row(u, p, val):
        zs_ref[u * res + p * rows:u * res + (p + 1) * rows, :] = val

    unpack_blocks(yr_ref, put_row, rows, ndap)
    for r in range(rows):
        out_ref[r] = zs_ref[r * res:(r + 1) * res, :].astype(BF16)
    drain(sends + c1 + c2 + c3 + c4)


def vspec():
    return pl.BlockSpec(memory_space=VMEM)


def call(kernel, outs, n_in, scratch, name, cid=None, flops=10 ** 9):
    params = dict(vmem_limit_bytes=60 * 2 ** 20)
    if cid is not None:
        params.update(collective_id=cid, has_side_effects=True)
    return pl.pallas_call(
        kernel,
        out_shape=outs,
        in_specs=[vspec()] * n_in,
        out_specs=jax.tree.map(lambda _: vspec(), outs),
        scratch_shapes=scratch,
        compiler_params=pltpu.CompilerParams(**params),
        cost_estimate=pl.CostEstimate(flops=flops, bytes_accessed=10 ** 6, transcendentals=0),
        name=name,
    )


def sds(shape, dtype):
    return jax.ShapeDtypeStruct(shape, dtype)


def solution(mesh):
    ndap = mesh.shape['dap']
    chips = ndap // 2

    def evoformer_block(msa, pair_act, full_mask, res_mask, row_bias_w, row_qkvg_w, row_out_w, col_query_w, col_kv_w, col_gate_w, col_out_w, opm_proj_w, opm_out_w, start_bias_w, start_qkvg_w, start_out_w, end_bias_w, end_qkvg_w, end_out_w):
        seqs, res, chans = msa.shape
        rows = pair_act.shape[0]
        heads, hd = row_qkvg_w.shape[2], row_qkvg_w.shape[3]
        width = heads * hd
        wide = opm_proj_w.shape[2]
        outc = opm_out_w.shape[2]
        thd = start_qkvg_w.shape[2] * start_qkvg_w.shape[3]
        theads = start_bias_w.shape[1]
        m_t = jnp.swapaxes(msa, 1, 2)
        wt = lambda w: w.reshape(w.shape[0], -1).T
        dma = pltpu.SemaphoreType.DMA

        nstat = 2 * heads + width
        m2, a, c = call(
            functools.partial(msa_kernel, ndap=ndap, heads=heads, hd=hd),
            [sds((seqs, chans, res), BF16), sds((chips, 2, rows * wide, seqs), BF16), sds((wide, seqs, res), BF16)], 11,
            [VMEM((rows * heads, res), F32), VMEM((ndap, rows * heads, res), F32),
             VMEM((chans, res), F32), VMEM((ndap, chans, res), F32),
             VMEM((nstat, res), F32), VMEM((ndap, nstat, res), F32),
             VMEM((seqs, chans, res), BF16), VMEM((seqs, res), F32), VMEM((res, heads * res), F32),
             VMEM((chans, width), BF16), VMEM((chans, width), BF16), VMEM((2 * hd + width, chans), BF16),
             VMEM((seqs, width, res), BF16), VMEM((seqs, res, width + 16), BF16), VMEM((seqs, width, res), BF16), VMEM((seqs, width, res), BF16), VMEM((seqs, width, res), BF16),
             VMEM((res, heads * res), F32), VMEM((res, heads * res), F32), VMEM((res, heads * res), BF16), VMEM((res, heads * res), BF16),
             VMEM((8, heads * res), F32), VMEM((8, heads * res), F32),
             VMEM((seqs * 2 * hd, res), F32), VMEM((2 * hd, seqs, res), F32), VMEM((width, res), F32),
             VMEM((seqs * wide, res), F32), VMEM((seqs * wide, res), F32), VMEM((res * wide, seqs), F32),
             dma((3, ndap)), dma((3, ndap))],
            'msa_stack', cid=0,
        )(m_t, pair_act, full_mask, row_bias_w.T, wt(row_qkvg_w), row_out_w.reshape(width, chans), wt(col_query_w), wt(col_kv_w), wt(col_gate_w), col_out_w.reshape(width, chans), wt(opm_proj_w))
        msa_out = jnp.swapaxes(m2, 1, 2)

        npair = rows // 2
        nbuf = 2 * (chips // 2) - 1
        small = (rows * theads, res)
        block = (ndap, rows * rows, outc)
        pair_out = call(
            functools.partial(pair_kernel, chips=chips),
            sds(pair_act.shape, BF16), 12,
            [VMEM((chips, rows * wide, seqs), BF16), VMEM((wide, seqs, res), BF16),
             VMEM((chips, npair, outc, 2 * res), F32),
             VMEM((npair, wide * wide, 2 * res), BF16), VMEM((npair, wide * wide, 2 * res), BF16),
             VMEM((outc, wide * wide), BF16), VMEM((wide * wide, outc), F32), VMEM((res, res), F32),
             VMEM((nbuf, npair // 2, outc, 2 * res), F32), VMEM((nbuf, npair // 2, outc, 2 * res), F32),
             VMEM((rows * res, outc), F32), VMEM((rows * res, outc), F32), VMEM((rows * res, outc), BF16), VMEM((rows * res, 4 * thd), BF16), VMEM((res, theads * res), F32),
             VMEM(small, F32), VMEM((ndap,) + small, F32), VMEM(small, F32), VMEM((ndap,) + small, F32),
             VMEM(block, BF16), VMEM(block, BF16), VMEM(block, BF16), VMEM(block, BF16),
             dma((2,)), dma((2,)), dma((2, nbuf)), dma((2, nbuf)), dma((4, ndap)), dma((4, ndap))],
            'pair_stack', cid=1,
        )(a, c, pair_act, full_mask, res_mask.reshape(1, res), opm_out_w.reshape(wide * wide, outc),
          start_bias_w.T, wt(start_qkvg_w), start_out_w.reshape(thd, outc), end_bias_w.T, wt(end_qkvg_w), end_out_w.reshape(thd, outc))
        return msa_out, pair_out

    row_spec = P(('data', 'dap'), None, None)
    in_specs = (row_spec, row_spec, P('data', None), P('data')) + (P(),) * 15
    return jax.shard_map(evoformer_block, mesh=mesh, in_specs=in_specs, out_specs=(row_spec, row_spec), check_vma=False)
```

```python
import functools
import math

import jax
import jax.numpy as jnp
from jax import lax
from jax.experimental import pallas as pl
from jax.experimental.pallas import tpu as pltpu
from jax.sharding import PartitionSpec as P

F32 = jnp.float32
BF16 = jnp.bfloat16
MESH = pl.DeviceIdType.MESH
LOG2E = math.log2(math.e)
VMEM = pltpu.VMEM


def mm(left, right):
    return jnp.dot(left, right, preferred_element_type=F32)


def mm_nt(left, right):
    return lax.dot_general(left, right, (((1,), (1,)), ((), ())), preferred_element_type=F32)


def span(n, width):
    return slice(n * width, (n + 1) * width)


def sum0(x):
    return jnp.sum(x, axis=0, keepdims=True)


def max0(x):
    return jnp.max(x, axis=0, keepdims=True)


def ln_rows(x):
    n = x.shape[0]
    xc = x - sum0(x) * (1.0 / n)
    var = sum0(xc * xc) * (1.0 / n)
    return (xc * lax.rsqrt(var + 1e-5)).astype(BF16)


def ln_lanes(x):
    n = x.shape[1]
    xc = x - jnp.sum(x, axis=1, keepdims=True) * (1.0 / n)
    var = jnp.sum(xc * xc, axis=1, keepdims=True) * (1.0 / n)
    return (xc * lax.rsqrt(var + 1e-5)).astype(BF16)


def bf16_split(value, terms):
    import numpy as np
    out = []
    for _ in range(terms):
        t = float(np.asarray(value, dtype=jnp.bfloat16))
        out.append(t)
        value = value - t
    return out


def group_barrier(me, ndap):
    barrier = pltpu.get_barrier_semaphore()
    for k in range(1, ndap):
        pl.semaphore_signal(barrier, inc=1, device_id={'dap': lax.rem(me + k, ndap)}, device_id_type=MESH)
    pl.semaphore_wait(barrier, ndap - 1)


def far_first(count):
    return sorted(range(1, count), key=lambda k: -min(k, count - k))


def remote(src, dst, send_sem, recv_sem, dev):
    cp = pltpu.make_async_remote_copy(src, dst, send_sem, recv_sem, device_id={'dap': dev}, device_id_type=MESH)
    cp.start()
    return cp


def start_gather(src_ref, slab_ref, chip, core, chips, send_sem, recv_sem):
    copies = [remote(src_ref, slab_ref.at[chip], send_sem.at[k], recv_sem.at[k], dap_index(chip + k, core, chips)) for k in far_first(chips)]
    slab_ref[chip] = src_ref[...]
    return copies


def start_swap(send_ref, recv_ref, me, ndap, send_sem, recv_sem):
    copies = []
    for k in far_first(ndap):
        other = lax.rem(me + k, ndap)
        cp = pltpu.make_async_remote_copy(send_ref.at[other], recv_ref.at[me], send_sem.at[k], recv_sem.at[k], device_id={'dap': other}, device_id_type=MESH)
        cp.start()
        copies.append(cp)
    recv_ref[me] = send_ref[me]
    return copies


def finish(copies):
    for cp in copies:
        cp.wait_recv()


def drain(copies):
    for cp in copies:
        cp.wait_send()


def strided(ref, row):
    return ref.reshape(ref.shape[0] * ref.shape[1], ref.shape[2])[pl.ds(row, ref.shape[0], stride=ref.shape[1]), :]


def pair_bias(z_ref, w_ref, out_ref):
    vals = [mm_nt(w_ref[...], ln_lanes(z_ref[r].astype(F32))) for r in range(z_ref.shape[0])]
    out_ref[...] = jnp.concatenate(vals, axis=0).astype(BF16)


def bias_plane(wide_ref, h, heads):
    rows = wide_ref.shape[2] // heads
    return jnp.concatenate([wide_ref[u, c, pl.ds(h, rows, stride=heads), :] for c in range(wide_ref.shape[1]) for u in range(2)], axis=0)


def row_project(m_ref, mask_ref, wqkvg_ref, q_ref, kt_ref, v_ref, g_ref, heads, hd, unroll=8):
    seqs, chans, res = m_ref.shape
    width = heads * hd
    aug = kt_ref.shape[2] - width
    terms = bf16_split(1e4 / hd ** -0.5, 3)
    rowi = lax.broadcasted_iota(jnp.int32, (aug, res), 0)
    mvec = jnp.where(rowi == 0, terms[0], jnp.where(rowi == 1, terms[1], jnp.where(rowi == 2, terms[2], 0.0)))

    def body(it, _):
        for n in range(unroll // 2):
            s0 = it * unroll + n * 2
            lns = [ln_rows(m_ref[s0 + u].astype(F32)) for u in range(2)]
            proj = mm(wqkvg_ref[...], jnp.concatenate(lns, axis=1))
            for u in range(2):
                cols = span(u, res)
                s = s0 + u
                q_ref[s] = proj[0:width, cols].astype(BF16)
                mrow = mask_ref[pl.ds(s, 1), :] - 1.0
                k = proj[width:2 * width, cols].astype(BF16).astype(F32)
                kt_ref[s] = jnp.concatenate([k, mrow * mvec], axis=0).T.astype(BF16)
                v_ref[s] = proj[2 * width:3 * width, cols].astype(BF16)
                g_ref[s] = proj[3 * width:, cols].astype(BF16)
        return 0

    lax.fori_loop(0, seqs // unroll, body, 0)


def row_attend(bias_ref, q_ref, kt_ref, v_ref, g_ref, y_ref, s_refs, p_refs, l_refs, heads, hd):
    seqs, width, res = q_ref.shape
    scale2 = hd ** -0.5 * LOG2E
    npairs = heads // 2
    aug = kt_ref.shape[2] - width
    two, both = 2 * hd, 2 * res
    first = lax.broadcasted_iota(jnp.int32, (two, res), 0) < hd
    zero16 = jnp.zeros((two, res), BF16)
    ones = jnp.ones((aug, res), BF16)

    def scores(s, s_ref, t):
        s = jnp.minimum(s, seqs - 1)
        q16 = q_ref[s, span(t, two)]
        halves = [jnp.concatenate([zero16] * t + [part] + [zero16] * (npairs - 1 - t) + [ones], axis=0)
                  for part in (jnp.where(first, q16, zero16), jnp.where(first, zero16, q16))]
        s_ref[:, span(t, both)] = mm(kt_ref[s], jnp.concatenate(halves, axis=1))

    def soft(s_ref, p_ref, l_ref, t):
        for h in (2 * t, 2 * t + 1):
            cols = span(h, res)
            x = s_ref[:, cols] * scale2 + bias_ref[:, cols]
            p = jnp.exp2(x - max0(x))
            l_ref[:, cols] = sum0(p)
            p_ref[h] = p.astype(BF16)

    def values(s, p_ref, l_ref, t):
        s = jnp.maximum(s, 0)
        o = mm(v_ref[s, span(t, two)], jnp.concatenate([p_ref[2 * t], p_ref[2 * t + 1]], axis=1))
        inv = 1.0 / l_ref[:, span(t, both)]
        att = jnp.concatenate([o[:hd, :res] * inv[:, :res], o[hd:, res:] * inv[:, res:]], axis=0)
        y_ref[s, span(t, two)] = (jax.nn.sigmoid(g_ref[s, span(t, two)].astype(F32)) * att).astype(BF16)

    depth = len(s_refs)
    lead = depth // 2
    for n in range(lead):
        for t in range(npairs):
            scores(n, s_refs[n], t)

    def body(it, _):
        for n in range(depth):
            s = it * depth + n
            far = (n + lead) % depth
            for t in range(npairs):
                values(s - lead, p_refs[far], l_refs[far], t)
                scores(s + lead, s_refs[far], t)
                soft(s_refs[n], p_refs[n], l_refs[n], t)
        return 0

    lax.fori_loop(0, seqs // depth, body, 0)
    for n in range(lead, depth):
        for t in range(npairs):
            values(seqs - depth + n, p_refs[n], l_refs[n], t)


def row_finish(m_ref, mask_ref, wo_ref, wkvg_ref, y_ref, m1_ref, kv_ref, g_ref, qsum_ref, hd, unroll=8):
    seqs, chans, res = m_ref.shape

    def body(it, _):
        acc = jnp.zeros((chans, res), F32)
        for n in range(unroll // 2):
            s0 = it * unroll + n * 2
            upd = mm(wo_ref[...], jnp.concatenate([y_ref[s0], y_ref[s0 + 1]], axis=1))
            ln1 = []
            for u in range(2):
                m1 = (m_ref[s0 + u].astype(F32) + upd[:, span(u, res)]).astype(BF16)
                m1_ref[s0 + u] = m1
                l1 = ln_rows(m1.astype(F32))
                acc = acc + l1.astype(F32) * mask_ref[pl.ds(s0 + u, 1), :]
                ln1.append(l1)
            kvg = mm(wkvg_ref[...], jnp.concatenate(ln1, axis=1)).astype(BF16)
            for u in range(2):
                kv_ref[s0 + u, 0:2 * hd] = kvg[0:2 * hd, span(u, res)].astype(F32)
                g_ref[s0 + u] = kvg[2 * hd:, span(u, res)]
        qsum_ref[...] += acc
        return 0

    lax.fori_loop(0, seqs // unroll, body, 0)


def col_stats(qtot, cnt, mask_ref, wq_ref, planes_ref, stats_ref, heads, hd):
    seqs, res = mask_ref.shape
    qbar = (qtot / (cnt + 1e-10)).astype(BF16)
    q = mm(wq_ref[...], qbar).astype(BF16).astype(F32)
    mb = (mask_ref[...] - 1.0) * (1e4 * LOG2E)
    for h in range(heads):
        acc = q[h * hd:h * hd + 1] * planes_ref[0]
        for d in range(1, hd):
            acc = acc + q[h * hd + d:h * hd + d + 1] * planes_ref[d]
        t = acc * (hd ** -0.5 * LOG2E) + mb
        mx = max0(t)
        p = jnp.exp2(t - mx)
        half, k = h // (heads // 2), h % (heads // 2)
        stats_ref[half, k:k + 1, :] = mx
        stats_ref[half, heads // 2 + k:heads // 2 + k + 1, :] = sum0(p)
        pb = p.astype(BF16).astype(F32)
        for d in range(hd):
            r = heads + k * hd + d
            stats_ref[half, r:r + 1, :] = sum0(pb * planes_ref[hd + d])


def combine_stats(stats, heads, hd):
    gm = functools.reduce(jnp.maximum, [st[0:heads] for st in stats])
    spread = lambda f: jnp.concatenate([jnp.broadcast_to(f[h:h + 1], (hd, f.shape[1])) for h in range(heads)], axis=0)
    tot = wv = 0.0
    for st in stats:
        f = jnp.exp2(st[0:heads] - gm)
        tot = tot + f * st[heads:2 * heads]
        wv = wv + spread(f) * st[2 * heads:]
    return gm, tot, wv, spread


def col_finish(g_ref, m1_ref, mask_ref, wac_ref, m2_ref, a_ref, c_ref, o_ref, wo_ref, as_ref, cs_ref, at_ref):
    seqs, chans, res = m1_ref.shape
    wide = wac_ref.shape[0] // 2

    def pair(s0):
        ys = [(jax.nn.sigmoid(g_ref[s0 + u].astype(F32)) * o_ref[...]).astype(BF16) for u in range(2)]
        upd = mm(wo_ref[...], jnp.concatenate(ys, axis=1))
        lns = []
        for u in range(2):
            m2 = (m1_ref[s0 + u].astype(F32) + upd[:, span(u, res)]).astype(BF16)
            m2_ref[s0 + u] = m2
            lns.append(ln_rows(m2.astype(F32)))
        ac = mm(wac_ref[...], jnp.concatenate(lns, axis=1)).astype(BF16).astype(F32)
        for u in range(2):
            mrow = mask_ref[pl.ds(s0 + u, 1), :]
            as_ref[s0 + u, 0:wide] = ac[0:wide, span(u, res)] * mrow
            cs_ref[s0 + u, 0:wide] = ac[wide:, span(u, res)] * mrow

    def body(it, _):
        for n in range(4):
            pair(it * 8 + n * 2)
        return 0

    lax.fori_loop(0, seqs // 8, body, 0)

    def planes(it, _):
        for n in range(8):
            e = it * 8 + n
            c_ref[e] = strided(cs_ref, e).astype(BF16)
            flat = at_ref.reshape(res * at_ref.shape[1], seqs)
            flat[pl.ds(e, res, stride=at_ref.shape[1]), :] = strided(as_ref, e).T
        return 0

    lax.fori_loop(0, wide // 8, planes, 0)
    rows = a_ref.shape[2] // wide
    for n in range(res):
        b, r = n // rows, n % rows
        a_ref[b // 2, b % 2, span(r, wide)] = at_ref[n, 0:wide].astype(BF16)


def msa_kernel(m_ref, z_ref, fmask_ref, wb_ref, wqkvg_ref, wout_ref, wq_ref, wkv_ref, wg_ref, wcout_ref, wac_ref,
               m2_ref, a_ref, c_ref,
               bsend_ref, ball_ref, bwide_ref, qsum_ref, qpart_ref, qhalf_ref, qall_ref, qfin_ref, stat_ref, spart_ref, smerge_ref, sall_ref, m1_ref, mask_ref, bias_ref, wo_ref, wco_ref, wkvg_ref,
               q_ref, kt_ref, v_ref, g_ref, y_ref, s_refs, p_refs, l_refs, kv_ref, planes_ref, o_ref, as_ref, cs_ref, at_ref,
               send_sem, recv_sem, psend_sem, precv_sem, *, ndap, heads, hd):
    seqs, chans, res = m_ref.shape
    me = lax.axis_index('dap')
    chip, core = me // 2, lax.rem(me, 2)
    chips = ndap // 2
    partner = chip * 2 + 1 - core
    pair_bias(z_ref, wb_ref, bsend_ref)
    group_barrier(me, ndap)
    bias_copies = start_gather(bsend_ref, ball_ref.at[core], chip, core, chips, send_sem.at[0], recv_sem.at[0])
    mask_ref[...] = fmask_ref[pl.ds(me * seqs, seqs), :].astype(F32)
    wo_ref[...] = wout_ref[...].astype(F32).T.astype(BF16)
    wco_ref[...] = wcout_ref[...].astype(F32).T.astype(BF16)
    wkvg_ref[0:2 * hd] = wkv_ref[...]
    wkvg_ref[2 * hd:] = wg_ref[...]
    qsum_ref[...] = jnp.zeros_like(qsum_ref)
    row_project(m_ref, mask_ref, wqkvg_ref, q_ref, kt_ref, v_ref, g_ref, heads, hd)
    finish(bias_copies)
    bias_swap = remote(ball_ref.at[core], ball_ref.at[core], psend_sem.at[0], precv_sem.at[0], partner)
    bias_swap.wait_recv()
    bwide_ref[...] = ball_ref[...].astype(F32)
    for h in range(heads):
        bias_ref[:, span(h, res)] = bias_plane(bwide_ref, h, heads).T * LOG2E
    row_attend(bias_ref, q_ref, kt_ref, v_ref, g_ref, y_ref, s_refs, p_refs, l_refs, heads, hd)
    row_finish(m_ref, mask_ref, wo_ref, wkvg_ref, y_ref, m1_ref, kv_ref, g_ref, qsum_ref, hd)

    half = chans // 2
    mine, other = pl.ds(core * half, half), pl.ds((1 - core) * half, half)
    sum_swap = remote(qsum_ref.at[other], qpart_ref, psend_sem.at[1], precv_sem.at[1], partner)
    cnt = sum0(fmask_ref[...]).astype(F32)
    sum_swap.wait_recv()
    qhalf_ref[...] = qsum_ref[mine, :] + qpart_ref[...]
    sum_copies = start_gather(qhalf_ref, qall_ref, chip, core, chips, send_sem.at[1], recv_sem.at[1])
    for d in range(2 * hd):
        planes_ref[d] = strided(kv_ref, d)
    finish(sum_copies)
    qfin_ref[mine, :] = functools.reduce(lambda x, y: x + y, [qall_ref[d] for d in range(chips)])
    fin_swap = remote(qfin_ref.at[mine], qfin_ref.at[mine], psend_sem.at[2], precv_sem.at[2], partner)
    fin_swap.wait_recv()
    col_stats(qfin_ref[...], cnt, mask_ref, wq_ref, planes_ref, stat_ref, heads, hd)

    stat_swap = remote(stat_ref.at[1 - core], spart_ref, psend_sem.at[3], precv_sem.at[3], partner)
    stat_swap.wait_recv()
    hh = heads // 2
    gm, tot, wv, _ = combine_stats([stat_ref[core], spart_ref[...]], hh, hd)
    smerge_ref[0:hh] = gm
    smerge_ref[hh:2 * hh] = tot
    smerge_ref[2 * hh:] = wv
    stat_copies = start_gather(smerge_ref, sall_ref, chip, core, chips, send_sem.at[2], recv_sem.at[2])
    finish(stat_copies)
    gm, tot, wv, spread = combine_stats([sall_ref[d] for d in range(chips)], hh, hd)
    omine = pl.ds(core * hh * hd, hh * hd)
    o_ref[omine, :] = wv / spread(tot)
    out_swap = remote(o_ref.at[omine], o_ref.at[omine], psend_sem.at[4], precv_sem.at[4], partner)
    out_swap.wait_recv()
    col_finish(g_ref, m1_ref, mask_ref, wac_ref, m2_ref, a_ref, c_ref, o_ref, wco_ref, as_ref, cs_ref, at_ref)
    drain(bias_copies + sum_copies + stat_copies + [bias_swap, sum_swap, fin_swap, stat_swap, out_swap])


def dap_index(chip, core, chips):
    return lax.rem(chip + 2 * chips, chips) * 2 + core


def outer_mean(me, a_ref, c_ref, z_ref, mask_ref, w_ref, zs_ref, ap_ref, cp_ref, part_ref, x_ref, wt_ref, w32_ref, cnt_ref, pos_ref, neg_ref, ex_send, ex_recv, send_sem, recv_sem, chips):
    chip, core = me // 2, lax.rem(me, 2)
    wide, seqs, res = c_ref.shape
    rows = z_ref.shape[0]
    brow = rows * wide
    outc = w_ref.shape[1]
    partner = chip * 2 + 1 - core
    peer = {1: dap_index(chip + 1, core, chips), -1: dap_index(chip - 1, core, chips)}
    half_chips = chips // 2
    depth, unroll = wide * wide, 4

    swaps = []
    for n, (src, dst) in enumerate(((a_ref.at[:, 1 - core], ap_ref), (c_ref, cp_ref))):
        cp = pltpu.make_async_remote_copy(src, dst, ex_send.at[n], ex_recv.at[n], device_id={'dap': partner}, device_id_type=MESH)
        cp.start()
        swaps.append(cp)

    w32_ref[...] = w_ref[...].astype(F32)
    per = 128 // wide
    for b in range(wide // per):
        cols = [w32_ref[pl.ds(b * per + f, wide, stride=wide), :] for f in range(per)]
        wt_ref[:, span(b, 128)] = jnp.concatenate(cols, axis=0).T.astype(BF16)
    wt_ref[:, depth:] = wt_ref[:, :depth]

    def count_step(n, acc):
        blk = mask_ref[pl.ds(n * 128, 128), :].astype(F32)
        return acc + mm(blk.T.astype(BF16), blk.astype(BF16))

    cnt_ref[...] = lax.fori_loop(0, mask_ref.shape[0] // 128, count_step, jnp.zeros((res, res), F32))

    for cp in swaps:
        cp.wait()

    def block(dest, slot):
        lhs = jnp.concatenate([a_ref[dest, core], ap_ref[dest]], axis=1)

        def outer(it, _):
            for n in range(unroll):
                f0 = (it * unroll + n) * 2
                rhs = [jnp.concatenate([c[f0], c[f0 + 1]], axis=1) for c in (c_ref, cp_ref)]
                o = mm(lhs, jnp.concatenate(rhs, axis=0))
                hi = o.astype(BF16)
                lo = (o - hi.astype(F32)).astype(BF16)
                for m, val in enumerate((hi, lo)):
                    for i in range(rows):
                        for u in range(2):
                            r0 = pl.multiple_of((f0 + u) * wide + m * depth, wide)
                            x_ref[i, pl.ds(r0, wide)] = val[span(i, wide), span(u, res)]
            return 0

        lax.fori_loop(0, wide // 2 // unroll, outer, 0)
        for n in range(rows // 2):
            part_ref[slot, n] = mm(wt_ref[...], jnp.concatenate([x_ref[2 * n], x_ref[2 * n + 1]], axis=1))

    sends = []
    arrivals = {}
    bufs = {1: pos_ref, -1: neg_ref}
    hq = rows // 4

    def hops(d, half):
        return half_chips if (half == 1) == (d == 1) else half_chips - 1

    slot_of = {}
    nbuf = 2 * half_chips - 1

    def buf_index(d, half, k):
        return (k - 1) + (0 if (half == 1) == (d == 1) else half_chips)

    def message(d, half, k, slot):
        idx = buf_index(d, half, k)
        src = part_ref.at[slot, pl.ds(half * hq, hq)]
        cp = pltpu.make_async_remote_copy(src, bufs[d].at[idx], send_sem.at[(d + 1) // 2, idx], recv_sem.at[(d + 1) // 2, idx], device_id={'dap': peer[d]}, device_id_type=MESH)
        arrivals[(d, half, k)] = cp
        sends.append(cp)
        cp.start()

    def take(d, half, k, slot):
        arrivals[(d, half, k)].wait_recv()
        part_ref[slot, span(half, hq)] += bufs[d][buf_index(d, half, k)]

    def dest_of(d, k):
        return lax.rem(chip + d * k + 2 * chips, chips)

    far = half_chips
    long_half = {1: 1, -1: 0}
    slots = {}

    def forward(long, k):
        for d in (1, -1):
            half = long_half[d] if long else 1 - long_half[d]
            take(d, half, k + 1, slots[(d, k)])
            message(d, half, k, slots[(d, k)])

    moves = []
    for k in range(far - 1, 0, -1):
        moves.append((True, k))
        if k > 1:
            moves.append((False, k - 1))
    todo = [(1, far)] + [(d, k) for k in range(far - 1, 0, -1) for d in (1, -1)] + [(1, 0)]
    for slot, (d, k) in enumerate(todo):
        slots[(d, k)] = slot
        block(dest_of(d, k), slot)
        if k == far:
            message(1, 1, far, slot)
            message(-1, 0, far, slot)
        elif k == far - 1:
            message(d, 1 - long_half[d], k, slot)
        if slot >= 3 and slot % 2 == 1 and slot < len(todo) - 1:
            forward(*moves.pop(0))
    for move in moves:
        forward(*move)
    for half in (0, 1):
        for d in (1, -1):
            take(d, half, 1, slot)
    for n in range(rows // 2):
        pair = part_ref[slot, n]
        for u in range(2):
            i = n * 2 + u
            cnt = cnt_ref[pl.ds(me * rows + i, 1), :] + 1e-3
            upd = (pair[:, span(u, res)] / cnt).T
            zs_ref[span(i, res), :] = (z_ref[i].astype(F32) + upd).astype(BF16).astype(F32)
    return sends


def tri_bias(zs_ref, ln_ref, w_ref, out_ref, rows, res):
    heads = w_ref.shape[0]
    vals = []
    for r in range(rows):
        ln = ln_lanes(zs_ref[span(r, res), :])
        if ln_ref is not None:
            ln_ref[span(r, res), :] = ln
        vals.append(mm_nt(w_ref[...], ln)[0:heads])
    out_ref[...] = jnp.concatenate(vals, axis=0).astype(BF16)


def tri_project(ln_ref, w_ref, proj_ref):
    step = 256
    for r in range(0, ln_ref.shape[0], step):
        proj_ref[r:r + step, :] = mm_nt(ln_ref[r:r + step, :], w_ref[...]).astype(BF16)


def tri_attend(zs_ref, proj_ref, bias_ref, wout_ref, heads, rows, res):
    width = proj_ref.shape[1] // 4
    hd = width // heads
    scale2 = hd ** -0.5 * LOG2E
    lane = lax.broadcasted_iota(jnp.int32, (res, width), 1)
    mine = [(lane >= h * hd) & (lane < (h + 1) * hd) for h in range(heads)]
    zero = jnp.zeros((res, width), BF16)

    def one(r0):
        part = lambda n: proj_ref[pl.ds(r0, res), span(n, width)]
        q, k, v, g = part(0), part(1), part(2), part(3)
        s = mm_nt(q, jnp.concatenate([jnp.where(mine[h], k, zero) for h in range(heads)], axis=0))
        ps = []
        for h in range(heads):
            cols = span(h, res)
            x = s[:, cols] * scale2 + bias_ref[:, cols]
            p = jnp.exp2(x - jnp.max(x, axis=1, keepdims=True))
            ps.append((p * (1.0 / jnp.sum(p, axis=1, keepdims=True))).astype(BF16))
        o = mm(jnp.concatenate(ps, axis=1), jnp.concatenate([jnp.where(mine[h], v, zero) for h in range(heads)], axis=0))
        y = (jax.nn.sigmoid(g.astype(F32)) * o).astype(BF16)
        upd = mm(y, wout_ref[...])
        zs_ref[pl.ds(r0, res), :] = (zs_ref[pl.ds(r0, res), :] + upd).astype(BF16).astype(F32)

    def body(it, _):
        for n in range(4):
            one(pl.multiple_of((it * 4 + n) * res, res))
        return 0

    lax.fori_loop(0, rows // 4, body, 0)


def pack_blocks(zs_ref, send_ref, rows, res, ndap):
    def one(q, _):
        parts = [zs_ref[pl.ds(q * rows + u, rows, stride=res), :] for u in range(rows)]
        send_ref[q] = jnp.concatenate(parts, axis=0).astype(BF16)
        return 0

    lax.fori_loop(0, ndap, one, 0)


def unpack_blocks(recv_ref, put, rows, ndap):
    for p in range(ndap):
        blk = recv_ref[p].astype(F32)
        for u in range(rows):
            put(u, p, blk[span(u, rows), :])


def pair_kernel(a_ref, c_ref, z_ref, mask_ref, rmask_ref, w_ref, wsb_ref, wsp_ref, wso_ref, web_ref, wep_ref, weo_ref,
                out_ref,
                ap_ref, cp_ref, part_ref, x_ref, wt_ref, w32_ref, cnt_ref, pos_ref, neg_ref,
                zs_ref, zc_ref, ln_ref, proj_ref, bias_ref, bwide_ref, sb_ref, sball_ref, eb_ref, eball_ref, xs_ref, xr_ref, ys_ref, yr_ref,
                ex_send, ex_recv, ring_send, ring_recv, send_sem, recv_sem, gsend, grecv, psend, precv, *, chips):
    ndap = 2 * chips
    me = lax.axis_index('dap')
    rows, res, _ = z_ref.shape
    heads = wsb_ref.shape[0]
    chip, core = me // 2, lax.rem(me, 2)
    partner = chip * 2 + 1 - core
    group_barrier(me, ndap)
    sends = outer_mean(me, a_ref, c_ref, z_ref, mask_ref, w_ref, zs_ref, ap_ref, cp_ref, part_ref, x_ref, wt_ref, w32_ref, cnt_ref, pos_ref, neg_ref, ex_send, ex_recv, ring_send, ring_recv, chips)
    kmask = (rmask_ref[...].astype(F32) - 1.0) * 1e4

    tri_bias(zs_ref, ln_ref, wsb_ref, sb_ref, rows, res)
    c1 = start_gather(sb_ref, sball_ref.at[core], chip, core, chips, gsend.at[0], grecv.at[0])
    tri_project(ln_ref, wsp_ref, proj_ref)
    finish(c1)
    p1 = remote(sball_ref.at[core], sball_ref.at[core], psend.at[0], precv.at[0], partner)
    p1.wait_recv()
    bwide_ref[...] = sball_ref[...].astype(F32)
    for h in range(heads):
        bias_ref[:, span(h, res)] = (bias_plane(bwide_ref, h, heads) + kmask) * LOG2E
    tri_attend(zs_ref, proj_ref, bias_ref, wso_ref, heads, rows, res)

    pack_blocks(zs_ref, xs_ref, rows, res, ndap)
    c2 = start_swap(xs_ref, xr_ref, me, ndap, send_sem.at[0], recv_sem.at[0])
    tri_bias(zs_ref, None, web_ref, eb_ref, rows, res)
    c3 = start_gather(eb_ref, eball_ref.at[core], chip, core, chips, gsend.at[1], grecv.at[1])
    finish(c2)
    finish(c3)
    p3 = remote(eball_ref.at[core], eball_ref.at[core], psend.at[1], precv.at[1], partner)

    def put_col(u, p, val):
        zc_ref[u * res + p * rows:u * res + (p + 1) * rows, :] = val

    unpack_blocks(xr_ref, put_col, rows, ndap)
    for r in range(rows):
        ln_ref[span(r, res), :] = ln_lanes(zc_ref[span(r, res), :])
    tri_project(ln_ref, wep_ref, proj_ref)
    p3.wait_recv()
    bwide_ref[...] = eball_ref[...].astype(F32)
    for h in range(heads):
        bias_ref[:, span(h, res)] = (bias_plane(bwide_ref, h, heads).T + kmask) * LOG2E
    tri_attend(zc_ref, proj_ref, bias_ref, weo_ref, heads, rows, res)

    pack_blocks(zc_ref, ys_ref, rows, res, ndap)
    c4 = start_swap(ys_ref, yr_ref, me, ndap, send_sem.at[1], recv_sem.at[1])
    finish(c4)

    def put_row(u, p, val):
        zs_ref[u * res + p * rows:u * res + (p + 1) * rows, :] = val

    unpack_blocks(yr_ref, put_row, rows, ndap)
    for r in range(rows):
        out_ref[r] = zs_ref[span(r, res), :].astype(BF16)
    drain(sends + c1 + c2 + c3 + c4 + [p1, p3])


def vspec():
    return pl.BlockSpec(memory_space=VMEM)


def call(kernel, outs, n_in, scratch, name, cid=None, flops=10 ** 9):
    params = dict(vmem_limit_bytes=60 * 2 ** 20)
    if cid is not None:
        params.update(collective_id=cid, has_side_effects=True)
    return pl.pallas_call(
        kernel,
        out_shape=outs,
        in_specs=[vspec()] * n_in,
        out_specs=jax.tree.map(lambda _: vspec(), outs),
        scratch_shapes=scratch,
        compiler_params=pltpu.CompilerParams(**params),
        cost_estimate=pl.CostEstimate(flops=flops, bytes_accessed=10 ** 6, transcendentals=0),
        name=name,
    )


def sds(shape, dtype):
    return jax.ShapeDtypeStruct(shape, dtype)


def solution(mesh):
    ndap = mesh.shape['dap']
    chips = ndap // 2

    def evoformer_block(msa, pair_act, full_mask, res_mask, row_bias_w, row_qkvg_w, row_out_w, col_query_w, col_kv_w, col_gate_w, col_out_w, opm_proj_w, opm_out_w, start_bias_w, start_qkvg_w, start_out_w, end_bias_w, end_qkvg_w, end_out_w):
        seqs, res, chans = msa.shape
        rows = pair_act.shape[0]
        heads, hd = row_qkvg_w.shape[2], row_qkvg_w.shape[3]
        width = heads * hd
        wide = opm_proj_w.shape[2]
        outc = opm_out_w.shape[2]
        thd = start_qkvg_w.shape[2] * start_qkvg_w.shape[3]
        theads = start_bias_w.shape[1]
        m_t = jnp.swapaxes(msa, 1, 2)
        wt = lambda w: w.reshape(w.shape[0], -1).T
        dma = pltpu.SemaphoreType.DMA

        nstat = heads + width // 2
        depth = 2
        m2, a, c = call(
            functools.partial(msa_kernel, ndap=ndap, heads=heads, hd=hd),
            [sds((seqs, chans, res), BF16), sds((chips, 2, rows * wide, seqs), BF16), sds((wide, seqs, res), BF16)], 11,
            [VMEM((rows * heads, res), BF16), VMEM((2, chips, rows * heads, res), BF16), VMEM((2, chips, rows * heads, res), F32),
             VMEM((chans, res), F32), VMEM((chans // 2, res), F32), VMEM((chans // 2, res), F32), VMEM((chips, chans // 2, res), F32), VMEM((chans, res), F32),
             VMEM((2, nstat, res), F32), VMEM((nstat, res), F32), VMEM((nstat, res), F32), VMEM((chips, nstat, res), F32),
             VMEM((seqs, chans, res), BF16), VMEM((seqs, res), F32), VMEM((res, heads * res), F32),
             VMEM((chans, width), BF16), VMEM((chans, width), BF16), VMEM((2 * hd + width, chans), BF16),
             VMEM((seqs, width, res), BF16), VMEM((seqs, res, width + 16), BF16), VMEM((seqs, width, res), BF16), VMEM((seqs, width, res), BF16), VMEM((seqs, width, res), BF16),
             [VMEM((res, heads * res), F32)] * depth, [VMEM((heads, res, res), BF16)] * depth, [VMEM((1, heads * res), F32)] * depth,
             VMEM((seqs, 3 * hd, res), F32), VMEM((2 * hd, seqs, res), F32), VMEM((width, res), F32),
             VMEM((seqs, wide + 8, res), F32), VMEM((seqs, wide + 8, res), F32), VMEM((res, wide + 8, seqs), F32),
             dma((3, chips)), dma((3, chips)), dma((5,)), dma((5,))],
            'msa_stack', cid=0,
        )(m_t, pair_act, full_mask, row_bias_w.T, wt(row_qkvg_w), row_out_w.reshape(width, chans), wt(col_query_w), wt(col_kv_w), wt(col_gate_w), col_out_w.reshape(width, chans), wt(opm_proj_w))
        msa_out = jnp.swapaxes(m2, 1, 2)

        npair = rows // 2
        nbuf = 2 * (chips // 2) - 1
        small = (rows * theads, res)
        block = (ndap, rows * rows, outc)
        pair_out = call(
            functools.partial(pair_kernel, chips=chips),
            sds(pair_act.shape, BF16), 12,
            [VMEM((chips, rows * wide, seqs), BF16), VMEM((wide, seqs, res), BF16),
             VMEM((chips, npair, outc, 2 * res), F32),
             VMEM((rows, 2 * wide * wide, res), BF16),
             VMEM((outc, 2 * wide * wide), BF16), VMEM((wide * wide, outc), F32), VMEM((res, res), F32),
             VMEM((nbuf, npair // 2, outc, 2 * res), F32), VMEM((nbuf, npair // 2, outc, 2 * res), F32),
             VMEM((rows * res, outc), F32), VMEM((rows * res, outc), F32), VMEM((rows * res, outc), BF16), VMEM((rows * res, 4 * thd), BF16), VMEM((res, theads * res), F32),
             VMEM((2, chips) + small, F32), VMEM(small, BF16), VMEM((2, chips) + small, BF16), VMEM(small, BF16), VMEM((2, chips) + small, BF16),
             VMEM(block, BF16), VMEM(block, BF16), VMEM(block, BF16), VMEM(block, BF16),
             dma((2,)), dma((2,)), dma((2, nbuf)), dma((2, nbuf)), dma((2, ndap)), dma((2, ndap)), dma((2, chips)), dma((2, chips)), dma((2,)), dma((2,))],
            'pair_stack', cid=1,
        )(a, c, pair_act, full_mask, res_mask.reshape(1, res), opm_out_w.reshape(wide * wide, outc),
          start_bias_w.T, wt(start_qkvg_w), start_out_w.reshape(thd, outc), end_bias_w.T, wt(end_qkvg_w), end_out_w.reshape(thd, outc))
        return msa_out, pair_out

    row_spec = P(('data', 'dap'), None, None)
    in_specs = (row_spec, row_spec, P('data', None), P('data')) + (P(),) * 15
    return jax.shard_map(evoformer_block, mesh=mesh, in_specs=in_specs, out_specs=(row_spec, row_spec), check_vma=False)
```

```python
import functools
import math

import jax
import jax.numpy as jnp
from jax import lax
from jax.experimental import pallas as pl
from jax.experimental.pallas import tpu as pltpu
from jax.sharding import PartitionSpec as P

F32 = jnp.float32
BF16 = jnp.bfloat16
MESH = pl.DeviceIdType.MESH
LOG2E = math.log2(math.e)
VMEM = pltpu.VMEM


def mm(left, right):
    return jnp.dot(left, right, preferred_element_type=F32)


def mm_nt(left, right):
    return lax.dot_general(left, right, (((1,), (1,)), ((), ())), preferred_element_type=F32)


def span(n, width):
    return slice(n * width, (n + 1) * width)


def sum0(x):
    return jnp.sum(x, axis=0, keepdims=True)


def max0(x):
    return jnp.max(x, axis=0, keepdims=True)


def ln_rows(x):
    n = x.shape[0]
    xc = x - sum0(x) * (1.0 / n)
    var = sum0(xc * xc) * (1.0 / n)
    return (xc * lax.rsqrt(var + 1e-5)).astype(BF16)


def ln_lanes(x):
    n = x.shape[1]
    xc = x - jnp.sum(x, axis=1, keepdims=True) * (1.0 / n)
    var = jnp.sum(xc * xc, axis=1, keepdims=True) * (1.0 / n)
    return (xc * lax.rsqrt(var + 1e-5)).astype(BF16)


def bf16_split(value, terms):
    import numpy as np
    out = []
    for _ in range(terms):
        t = float(np.asarray(value, dtype=jnp.bfloat16))
        out.append(t)
        value = value - t
    return out


def group_barrier(me, ndap):
    barrier = pltpu.get_barrier_semaphore()
    for k in range(1, ndap):
        pl.semaphore_signal(barrier, inc=1, device_id={'dap': lax.rem(me + k, ndap)}, device_id_type=MESH)
    pl.semaphore_wait(barrier, ndap - 1)


def far_first(count):
    return sorted(range(1, count), key=lambda k: -min(k, count - k))


def remote(src, dst, send_sem, recv_sem, dev):
    cp = pltpu.make_async_remote_copy(src, dst, send_sem, recv_sem, device_id={'dap': dev}, device_id_type=MESH)
    cp.start()
    return cp


def start_gather(src_ref, slab_ref, chip, core, chips, send_sem, recv_sem):
    copies = [remote(src_ref, slab_ref.at[chip], send_sem.at[k], recv_sem.at[k], dap_index(chip + k, core, chips)) for k in far_first(chips)]
    slab_ref[chip] = src_ref[...]
    return copies


def start_swap(send_ref, recv_ref, me, ndap, send_sem, recv_sem):
    copies = []
    for k in far_first(ndap):
        other = lax.rem(me + k, ndap)
        cp = pltpu.make_async_remote_copy(send_ref.at[other], recv_ref.at[me], send_sem.at[k], recv_sem.at[k], device_id={'dap': other}, device_id_type=MESH)
        cp.start()
        copies.append(cp)
    recv_ref[me] = send_ref[me]
    return copies


def finish(copies):
    for cp in copies:
        cp.wait_recv()


def drain(copies):
    for cp in copies:
        cp.wait_send()


def strided(ref, row):
    return ref.reshape(ref.shape[0] * ref.shape[1], ref.shape[2])[pl.ds(row, ref.shape[0], stride=ref.shape[1]), :]


def pair_bias(z_ref, w_ref, out_ref):
    vals = [mm_nt(w_ref[...], ln_lanes(z_ref[r].astype(F32))) for r in range(z_ref.shape[0])]
    out_ref[...] = jnp.concatenate(vals, axis=0).astype(BF16)


def bias_plane(wide_ref, h, heads):
    rows = wide_ref.shape[2] // heads
    return jnp.concatenate([wide_ref[u, c, pl.ds(h, rows, stride=heads), :] for c in range(wide_ref.shape[1]) for u in range(2)], axis=0)


def row_project(m_ref, mask_ref, wqkvg_ref, q_ref, kt_ref, v_ref, g_ref, heads, hd, unroll=8):
    seqs, chans, res = m_ref.shape
    width = heads * hd
    aug = kt_ref.shape[2] - width
    terms = bf16_split(1e4 / hd ** -0.5, 3)
    rowi = lax.broadcasted_iota(jnp.int32, (aug, res), 0)
    mvec = jnp.where(rowi == 0, terms[0], jnp.where(rowi == 1, terms[1], jnp.where(rowi == 2, terms[2], 0.0)))

    def body(it, _):
        for n in range(unroll // 2):
            s0 = it * unroll + n * 2
            lns = [ln_rows(m_ref[s0 + u].astype(F32)) for u in range(2)]
            proj = mm(wqkvg_ref[...], jnp.concatenate(lns, axis=1))
            for u in range(2):
                cols = span(u, res)
                s = s0 + u
                q_ref[s] = proj[0:width, cols].astype(BF16)
                mrow = mask_ref[pl.ds(s, 1), :] - 1.0
                k = proj[width:2 * width, cols].astype(BF16).astype(F32)
                kt_ref[s] = jnp.concatenate([k, mrow * mvec], axis=0).T.astype(BF16)
                v_ref[s] = proj[2 * width:3 * width, cols].astype(BF16)
                g_ref[s] = proj[3 * width:, cols].astype(BF16)
        return 0

    lax.fori_loop(0, seqs // unroll, body, 0)


def row_attend(bias_ref, q_ref, kt_ref, v_ref, g_ref, y_ref, s_refs, p_refs, l_refs, heads, hd):
    seqs, width, res = q_ref.shape
    scale2 = hd ** -0.5 * LOG2E
    npairs = heads // 2
    aug = kt_ref.shape[2] - width
    two, both = 2 * hd, 2 * res
    first = lax.broadcasted_iota(jnp.int32, (two, res), 0) < hd
    zero16 = jnp.zeros((two, res), BF16)
    ones = jnp.ones((aug, res), BF16)

    def scores(s, s_ref, t):
        s = jnp.minimum(s, seqs - 1)
        q16 = q_ref[s, span(t, two)]
        halves = [jnp.concatenate([zero16] * t + [part] + [zero16] * (npairs - 1 - t) + [ones], axis=0)
                  for part in (jnp.where(first, q16, zero16), jnp.where(first, zero16, q16))]
        s_ref[:, span(t, both)] = mm(kt_ref[s], jnp.concatenate(halves, axis=1))

    def soft(s_ref, p_ref, l_ref, t):
        for h in (2 * t, 2 * t + 1):
            cols = span(h, res)
            x = s_ref[:, cols] * scale2 + bias_ref[:, cols]
            p = jnp.exp2(x - max0(x))
            l_ref[:, cols] = sum0(p)
            p_ref[h] = p.astype(BF16)

    def values(s, p_ref, l_ref, t):
        s = jnp.maximum(s, 0)
        o = mm(v_ref[s, span(t, two)], jnp.concatenate([p_ref[2 * t], p_ref[2 * t + 1]], axis=1))
        inv = 1.0 / l_ref[:, span(t, both)]
        att = jnp.concatenate([o[:hd, :res] * inv[:, :res], o[hd:, res:] * inv[:, res:]], axis=0)
        y_ref[s, span(t, two)] = (jax.nn.sigmoid(g_ref[s, span(t, two)].astype(F32)) * att).astype(BF16)

    depth = len(s_refs)
    lead = depth // 2
    for n in range(lead):
        for t in range(npairs):
            scores(n, s_refs[n], t)

    def body(it, _):
        for n in range(depth):
            s = it * depth + n
            far = (n + lead) % depth
            for t in range(npairs):
                values(s - lead, p_refs[far], l_refs[far], t)
                scores(s + lead, s_refs[far], t)
                soft(s_refs[n], p_refs[n], l_refs[n], t)
        return 0

    lax.fori_loop(0, seqs // depth, body, 0)
    for n in range(lead, depth):
        for t in range(npairs):
            values(seqs - depth + n, p_refs[n], l_refs[n], t)


def row_finish(m_ref, mask_ref, wo_ref, wkvg_ref, y_ref, m1_ref, kv_ref, g_ref, qsum_ref, hd, unroll=8):
    seqs, chans, res = m_ref.shape

    def body(it, _):
        acc = jnp.zeros((chans, res), F32)
        for n in range(unroll // 2):
            s0 = it * unroll + n * 2
            upd = mm(wo_ref[...], jnp.concatenate([y_ref[s0], y_ref[s0 + 1]], axis=1))
            ln1 = []
            for u in range(2):
                m1 = (m_ref[s0 + u].astype(F32) + upd[:, span(u, res)]).astype(BF16)
                m1_ref[s0 + u] = m1
                l1 = ln_rows(m1.astype(F32))
                acc = acc + l1.astype(F32) * mask_ref[pl.ds(s0 + u, 1), :]
                ln1.append(l1)
            kvg = mm(wkvg_ref[...], jnp.concatenate(ln1, axis=1)).astype(BF16)
            for u in range(2):
                kv_ref[s0 + u, 0:2 * hd] = kvg[0:2 * hd, span(u, res)].astype(F32)
                g_ref[s0 + u] = kvg[2 * hd:, span(u, res)]
        qsum_ref[...] += acc
        return 0

    lax.fori_loop(0, seqs // unroll, body, 0)


def col_stats(qtot, cnt, mask_ref, wq_ref, planes_ref, stats_ref, heads, hd):
    seqs, res = mask_ref.shape
    qbar = (qtot / (cnt + 1e-10)).astype(BF16)
    q = mm(wq_ref[...], qbar).astype(BF16).astype(F32)
    mb = (mask_ref[...] - 1.0) * (1e4 * LOG2E)
    for h in range(heads):
        acc = q[h * hd:h * hd + 1] * planes_ref[0]
        for d in range(1, hd):
            acc = acc + q[h * hd + d:h * hd + d + 1] * planes_ref[d]
        t = acc * (hd ** -0.5 * LOG2E) + mb
        mx = max0(t)
        p = jnp.exp2(t - mx)
        half, k = h // (heads // 2), h % (heads // 2)
        stats_ref[half, k:k + 1, :] = mx
        stats_ref[half, heads // 2 + k:heads // 2 + k + 1, :] = sum0(p)
        pb = p.astype(BF16).astype(F32)
        for d in range(hd):
            r = heads + k * hd + d
            stats_ref[half, r:r + 1, :] = sum0(pb * planes_ref[hd + d])


def combine_stats(stats, heads, hd):
    gm = functools.reduce(jnp.maximum, [st[0:heads] for st in stats])
    spread = lambda f: jnp.concatenate([jnp.broadcast_to(f[h:h + 1], (hd, f.shape[1])) for h in range(heads)], axis=0)
    tot = wv = 0.0
    for st in stats:
        f = jnp.exp2(st[0:heads] - gm)
        tot = tot + f * st[heads:2 * heads]
        wv = wv + spread(f) * st[2 * heads:]
    return gm, tot, wv, spread


def col_finish(g_ref, m1_ref, mask_ref, wac_ref, m2_ref, a_ref, c_ref, o_ref, wo_ref, as_ref, cs_ref, at_ref, write_out, send_c, send_a):
    seqs, chans, res = m1_ref.shape
    wide = wac_ref.shape[0] // 2

    def pair(s0):
        ys = [(jax.nn.sigmoid(g_ref[s0 + u].astype(F32)) * o_ref[...]).astype(BF16) for u in range(2)]
        upd = mm(wo_ref[...], jnp.concatenate(ys, axis=1))
        lns = []
        for u in range(2):
            m2 = (m1_ref[s0 + u].astype(F32) + upd[:, span(u, res)]).astype(BF16)
            m2_ref[s0 + u] = m2
            lns.append(ln_rows(m2.astype(F32)))
        ac = mm(wac_ref[...], jnp.concatenate(lns, axis=1)).astype(BF16).astype(F32)
        for u in range(2):
            mrow = mask_ref[pl.ds(s0 + u, 1), :]
            as_ref[s0 + u, 0:wide] = ac[0:wide, span(u, res)] * mrow
            cs_ref[s0 + u, 0:wide] = ac[wide:, span(u, res)] * mrow

    def body(it, _):
        for n in range(4):
            pair(it * 8 + n * 2)
        return 0

    lax.fori_loop(0, seqs // 8, body, 0)

    write_out()
    unroll = 8

    def planes_c(it, _):
        for n in range(unroll):
            e = it * unroll + n
            c_ref[e] = strided(cs_ref, e).astype(BF16)
        return 0

    def planes_a(it, _):
        flat = at_ref.reshape(res * at_ref.shape[1], seqs)
        for n in range(unroll):
            e = it * unroll + n
            flat[pl.ds(e, res, stride=at_ref.shape[1]), :] = strided(as_ref, e).T
        return 0

    lax.fori_loop(0, wide // unroll, planes_c, 0)
    send_c()
    lax.fori_loop(0, wide // unroll, planes_a, 0)
    rows = a_ref.shape[2] // wide
    for n in range(res):
        b, r = n // rows, n % rows
        a_ref[b // 2, b % 2, span(r, wide)] = at_ref[n, 0:wide].astype(BF16)
    send_a()


def msa_part(m_ref, z_ref, fmask_ref, wb_ref, wqkvg_ref, wout_ref, wq_ref, wkv_ref, wg_ref, wcout_ref, wac_ref, m2_ref, a_ref, c_ref, idle, hooks,
               bsend_ref, ball_ref, bwide_ref, qsum_ref, qpart_ref, qhalf_ref, qall_ref, qfin_ref, stat_ref, spart_ref, smerge_ref, sall_ref, m1_ref, mask_ref, bias_ref, wo_ref, wco_ref, wkvg_ref,
               q_ref, kt_ref, v_ref, g_ref, y_ref, s_refs, p_refs, l_refs, kv_ref, planes_ref, o_ref, as_ref, cs_ref, at_ref,
               send_sem, recv_sem, psend_sem, precv_sem, ndap, heads, hd):
    seqs, chans, res = m_ref.shape
    me = lax.axis_index('dap')
    chip, core = me // 2, lax.rem(me, 2)
    chips = ndap // 2
    partner = chip * 2 + 1 - core
    pair_bias(z_ref, wb_ref, bsend_ref)
    group_barrier(me, ndap)
    bias_copies = start_gather(bsend_ref, ball_ref.at[core], chip, core, chips, send_sem.at[0], recv_sem.at[0])
    mask_ref[...] = fmask_ref[pl.ds(me * seqs, seqs), :].astype(F32)
    wo_ref[...] = wout_ref[...].astype(F32).T.astype(BF16)
    wco_ref[...] = wcout_ref[...].astype(F32).T.astype(BF16)
    wkvg_ref[0:2 * hd] = wkv_ref[...]
    wkvg_ref[2 * hd:] = wg_ref[...]
    qsum_ref[...] = jnp.zeros_like(qsum_ref)
    row_project(m_ref, mask_ref, wqkvg_ref, q_ref, kt_ref, v_ref, g_ref, heads, hd)
    finish(bias_copies)
    bias_swap = remote(ball_ref.at[core], ball_ref.at[core], psend_sem.at[0], precv_sem.at[0], partner)
    bias_swap.wait_recv()
    bwide_ref[...] = ball_ref[...].astype(F32)
    for h in range(heads):
        bias_ref[:, span(h, res)] = bias_plane(bwide_ref, h, heads).T * LOG2E
    row_attend(bias_ref, q_ref, kt_ref, v_ref, g_ref, y_ref, s_refs, p_refs, l_refs, heads, hd)
    row_finish(m_ref, mask_ref, wo_ref, wkvg_ref, y_ref, m1_ref, kv_ref, g_ref, qsum_ref, hd)

    half = chans // 2
    mine, other = pl.ds(core * half, half), pl.ds((1 - core) * half, half)
    sum_swap = remote(qsum_ref.at[other], qpart_ref, psend_sem.at[1], precv_sem.at[1], partner)
    cnt = sum0(fmask_ref[...]).astype(F32)
    sum_swap.wait_recv()
    qhalf_ref[...] = qsum_ref[mine, :] + qpart_ref[...]
    sum_copies = start_gather(qhalf_ref, qall_ref, chip, core, chips, send_sem.at[1], recv_sem.at[1])
    for d in range(2 * hd):
        planes_ref[d] = strided(kv_ref, d)
    finish(sum_copies)
    qfin_ref[mine, :] = functools.reduce(lambda x, y: x + y, [qall_ref[d] for d in range(chips)])
    fin_swap = remote(qfin_ref.at[mine], qfin_ref.at[mine], psend_sem.at[2], precv_sem.at[2], partner)
    fin_swap.wait_recv()
    col_stats(qfin_ref[...], cnt, mask_ref, wq_ref, planes_ref, stat_ref, heads, hd)

    stat_swap = remote(stat_ref.at[1 - core], spart_ref, psend_sem.at[3], precv_sem.at[3], partner)
    stat_swap.wait_recv()
    hh = heads // 2
    gm, tot, wv, _ = combine_stats([stat_ref[core], spart_ref[...]], hh, hd)
    smerge_ref[0:hh] = gm
    smerge_ref[hh:2 * hh] = tot
    smerge_ref[2 * hh:] = wv
    stat_copies = start_gather(smerge_ref, sall_ref, chip, core, chips, send_sem.at[2], recv_sem.at[2])
    idle()
    finish(stat_copies)
    gm, tot, wv, spread = combine_stats([sall_ref[d] for d in range(chips)], hh, hd)
    omine = pl.ds(core * hh * hd, hh * hd)
    o_ref[omine, :] = wv / spread(tot)
    out_swap = remote(o_ref.at[omine], o_ref.at[omine], psend_sem.at[4], precv_sem.at[4], partner)
    out_swap.wait_recv()
    col_finish(g_ref, m1_ref, mask_ref, wac_ref, m2_ref, a_ref, c_ref, o_ref, wco_ref, as_ref, cs_ref, at_ref, *hooks)
    return bias_copies + sum_copies + stat_copies + [bias_swap, sum_swap, fin_swap, stat_swap, out_swap]


def dap_index(chip, core, chips):
    return lax.rem(chip + 2 * chips, chips) * 2 + core


def outer_prepare(mask_ref, w_ref, wt_ref, w32_ref, cnt_ref, wide):
    depth, lanes = w_ref.shape
    w32_ref[...] = w_ref[...].astype(F32)
    per = lanes // wide
    for b in range(wide // per):
        cols = [w32_ref[pl.ds(b * per + f, wide, stride=wide), :] for f in range(per)]
        wt_ref[:, span(b, lanes)] = jnp.concatenate(cols, axis=0).T.astype(BF16)
    wt_ref[:, depth:] = wt_ref[:, :depth]
    res = mask_ref.shape[1]

    def count_step(n, acc):
        blk = mask_ref[pl.ds(n * res, res), :].astype(F32)
        return acc + mm(blk.T.astype(BF16), blk.astype(BF16))

    cnt_ref[...] = lax.fori_loop(0, mask_ref.shape[0] // res, count_step, jnp.zeros((res, res), F32))


def outer_mean(me, a_ref, c_ref, z_ref, zs_ref, ap_ref, cp_ref, part_ref, x_ref, wt_ref, cnt_ref, pos_ref, neg_ref, send_sem, recv_sem, chips):
    chip, core = me // 2, lax.rem(me, 2)
    wide, seqs, res = c_ref.shape
    rows = z_ref.shape[0]
    peer = {1: dap_index(chip + 1, core, chips), -1: dap_index(chip - 1, core, chips)}
    half_chips = chips // 2
    depth, unroll = wide * wide, 4

    def block(dest, slot):
        lhs = jnp.concatenate([a_ref[dest, core], ap_ref[dest]], axis=1)

        def outer(it, _):
            for n in range(unroll):
                f0 = (it * unroll + n) * 2
                rhs = [jnp.concatenate([c[f0], c[f0 + 1]], axis=1) for c in (c_ref, cp_ref)]
                o = mm(lhs, jnp.concatenate(rhs, axis=0))
                hi = o.astype(BF16)
                lo = (o - hi.astype(F32)).astype(BF16)
                for m, val in enumerate((hi, lo)):
                    for i in range(rows):
                        for u in range(2):
                            r0 = pl.multiple_of((f0 + u) * wide + m * depth, wide)
                            x_ref[i, pl.ds(r0, wide)] = val[span(i, wide), span(u, res)]
            return 0

        lax.fori_loop(0, wide // 2 // unroll, outer, 0)
        for n in range(rows // 2):
            part_ref[slot, n] = mm(wt_ref[...], jnp.concatenate([x_ref[2 * n], x_ref[2 * n + 1]], axis=1))

    sends = []
    arrivals = {}
    bufs = {1: pos_ref, -1: neg_ref}
    hq = rows // 4

    def hops(d, half):
        return half_chips if (half == 1) == (d == 1) else half_chips - 1

    slot_of = {}
    nbuf = 2 * half_chips - 1

    def buf_index(d, half, k):
        return (k - 1) + (0 if (half == 1) == (d == 1) else half_chips)

    def message(d, half, k, slot):
        idx = buf_index(d, half, k)
        src = part_ref.at[slot, pl.ds(half * hq, hq)]
        cp = pltpu.make_async_remote_copy(src, bufs[d].at[idx], send_sem.at[(d + 1) // 2, idx], recv_sem.at[(d + 1) // 2, idx], device_id={'dap': peer[d]}, device_id_type=MESH)
        arrivals[(d, half, k)] = cp
        sends.append(cp)
        cp.start()

    def take(d, half, k, slot):
        arrivals[(d, half, k)].wait_recv()
        part_ref[slot, span(half, hq)] += bufs[d][buf_index(d, half, k)]

    def dest_of(d, k):
        return lax.rem(chip + d * k + 2 * chips, chips)

    far = half_chips
    long_half = {1: 1, -1: 0}
    slots = {}

    def forward(long, k):
        for d in (1, -1):
            half = long_half[d] if long else 1 - long_half[d]
            take(d, half, k + 1, slots[(d, k)])
            message(d, half, k, slots[(d, k)])

    moves = []
    for k in range(far - 1, 0, -1):
        moves.append((True, k))
        if k > 1:
            moves.append((False, k - 1))
    todo = [(1, far)] + [(d, k) for k in range(far - 1, 0, -1) for d in (1, -1)] + [(1, 0)]
    for slot, (d, k) in enumerate(todo):
        slots[(d, k)] = slot
        block(dest_of(d, k), slot)
        if k == far:
            message(1, 1, far, slot)
            message(-1, 0, far, slot)
        elif k == far - 1:
            message(d, 1 - long_half[d], k, slot)
        if slot >= 3 and slot % 2 == 1 and slot < len(todo) - 1:
            forward(*moves.pop(0))
    for move in moves:
        forward(*move)
    for half in (0, 1):
        for d in (1, -1):
            take(d, half, 1, slot)
    for n in range(rows // 2):
        pair = part_ref[slot, n]
        for u in range(2):
            i = n * 2 + u
            cnt = cnt_ref[pl.ds(me * rows + i, 1), :] + 1e-3
            upd = (pair[:, span(u, res)] / cnt).T
            zs_ref[span(i, res), :] = (z_ref[i].astype(F32) + upd).astype(BF16).astype(F32)
    return sends


def tri_bias(zs_ref, ln_ref, w_ref, out_ref, rows, res):
    heads = w_ref.shape[0]
    vals = []
    for r in range(rows):
        ln = ln_lanes(zs_ref[span(r, res), :])
        if ln_ref is not None:
            ln_ref[span(r, res), :] = ln
        vals.append(mm_nt(w_ref[...], ln)[0:heads])
    out_ref[...] = jnp.concatenate(vals, axis=0).astype(BF16)


def tri_project(ln_ref, w_ref, proj_ref):
    step = 256
    for r in range(0, ln_ref.shape[0], step):
        proj_ref[r:r + step, :] = mm_nt(ln_ref[r:r + step, :], w_ref[...]).astype(BF16)


def tri_attend(zs_ref, proj_ref, bias_ref, wout_ref, heads, rows, res, after):
    width = proj_ref.shape[1] // 4
    hd = width // heads
    scale2 = hd ** -0.5 * LOG2E
    lane = lax.broadcasted_iota(jnp.int32, (res, width), 1)
    mine = [(lane >= h * hd) & (lane < (h + 1) * hd) for h in range(heads)]
    zero = jnp.zeros((res, width), BF16)

    def one(r0):
        part = lambda n: proj_ref[pl.ds(r0, res), span(n, width)]
        q, k, v, g = part(0), part(1), part(2), part(3)
        s = mm_nt(q, jnp.concatenate([jnp.where(mine[h], k, zero) for h in range(heads)], axis=0))
        ps = []
        for h in range(heads):
            cols = span(h, res)
            x = s[:, cols] * scale2 + bias_ref[:, cols]
            p = jnp.exp2(x - jnp.max(x, axis=1, keepdims=True))
            ps.append((p * (1.0 / jnp.sum(p, axis=1, keepdims=True))).astype(BF16))
        o = mm(jnp.concatenate(ps, axis=1), jnp.concatenate([jnp.where(mine[h], v, zero) for h in range(heads)], axis=0))
        y = (jax.nn.sigmoid(g.astype(F32)) * o).astype(BF16)
        upd = mm(y, wout_ref[...])
        zs_ref[pl.ds(r0, res), :] = (zs_ref[pl.ds(r0, res), :] + upd).astype(BF16).astype(F32)

    part_rows = rows // 2
    for half in range(2):
        for n in range(part_rows):
            one((half * part_rows + n) * res)
        after(half)


def pack_blocks(zs_ref, send_ref, half, rows, res, ndap):
    few = rows // 2

    def one(q, _):
        parts = [zs_ref[pl.ds(half * few * res + q * rows + u, few, stride=res), :] for u in range(rows)]
        send_ref[half, q] = jnp.concatenate(parts, axis=0).astype(BF16)
        return 0

    lax.fori_loop(0, ndap, one, 0)


def unpack_blocks(recv_ref, dst_ref, rows, res, ndap):
    few = rows // 2
    for half in range(2):
        for p in range(ndap):
            blk = recv_ref[half, p].astype(F32)
            for u in range(rows):
                r0 = u * res + p * rows + half * few
                dst_ref[r0:r0 + few, :] = blk[span(u, few), :]


def block_kernel(m_ref, z_ref, fmask_ref, wb_ref, wqkvg_ref, wout_ref, wq_ref, wkv_ref, wg_ref, wcout_ref, wac_ref,
                 rmask_ref, w_ref, wsb_ref, wsp_ref, wso_ref, web_ref, wep_ref, weo_ref,
                 m2_ref, out_ref, msa_refs, pair_refs, *, ndap, heads, hd):
    (a_ref, c_ref, m2v_ref, out_sem, ap_ref, cp_ref, part_ref, x_ref, wt_ref, w32_ref, cnt_ref, pos_ref, neg_ref,
     zs_ref, zc_ref, ln_ref, proj_ref, bias_ref, bwide_ref, sb_ref, sball_ref, eb_ref, eball_ref, xs_ref, xr_ref, ys_ref, yr_ref,
     ex_send, ex_recv, ring_send, ring_recv, send_sem, recv_sem, gsend, grecv, psend, precv) = pair_refs
    chips = ndap // 2
    me = lax.axis_index('dap')
    rows, res, _ = z_ref.shape
    chip, core = me // 2, lax.rem(me, 2)
    partner = chip * 2 + 1 - core
    swaps = []
    out_copy = pltpu.make_async_copy(m2v_ref, m2_ref, out_sem)

    def send_c():
        swaps.append(remote(c_ref, cp_ref, ex_send.at[0], ex_recv.at[0], partner))

    def send_a():
        swaps.append(remote(a_ref.at[:, 1 - core], ap_ref, ex_send.at[1], ex_recv.at[1], partner))

    idle = lambda: outer_prepare(fmask_ref, w_ref, wt_ref, w32_ref, cnt_ref, c_ref.shape[0])
    early = msa_part(m_ref, z_ref, fmask_ref, wb_ref, wqkvg_ref, wout_ref, wq_ref, wkv_ref, wg_ref, wcout_ref, wac_ref, m2v_ref, a_ref, c_ref,
                     idle, (out_copy.start, send_c, send_a), *msa_refs, ndap, heads, hd)
    finish(swaps)
    sends = outer_mean(me, a_ref, c_ref, z_ref, zs_ref, ap_ref, cp_ref, part_ref, x_ref, wt_ref, cnt_ref, pos_ref, neg_ref, ring_send, ring_recv, chips)
    heads = wsb_ref.shape[0]
    kmask = (rmask_ref[...].astype(F32) - 1.0) * 1e4

    tri_bias(zs_ref, ln_ref, wsb_ref, sb_ref, rows, res)
    c1 = start_gather(sb_ref, sball_ref.at[core], chip, core, chips, gsend.at[0], grecv.at[0])
    tri_project(ln_ref, wsp_ref, proj_ref)
    finish(c1)
    p1 = remote(sball_ref.at[core], sball_ref.at[core], psend.at[0], precv.at[0], partner)
    p1.wait_recv()
    bwide_ref[...] = sball_ref[...].astype(F32)
    for h in range(heads):
        bias_ref[:, span(h, res)] = (bias_plane(bwide_ref, h, heads) + kmask) * LOG2E
    moved = []

    def swap_after(src_ref, send_ref, recv_ref, stage):
        def after(half):
            pack_blocks(src_ref, send_ref, half, rows, res, ndap)
            moved.append(start_swap(send_ref.at[half], recv_ref.at[half], me, ndap, send_sem.at[stage, half], recv_sem.at[stage, half]))
        return after

    tri_attend(zs_ref, proj_ref, bias_ref, wso_ref, heads, rows, res, swap_after(zs_ref, xs_ref, xr_ref, 0))
    tri_bias(zs_ref, None, web_ref, eb_ref, rows, res)
    c3 = start_gather(eb_ref, eball_ref.at[core], chip, core, chips, gsend.at[1], grecv.at[1])
    finish(moved[0] + moved[1])
    finish(c3)
    p3 = remote(eball_ref.at[core], eball_ref.at[core], psend.at[1], precv.at[1], partner)
    unpack_blocks(xr_ref, zc_ref, rows, res, ndap)
    for r in range(rows):
        ln_ref[span(r, res), :] = ln_lanes(zc_ref[span(r, res), :])
    tri_project(ln_ref, wep_ref, proj_ref)
    p3.wait_recv()
    bwide_ref[...] = eball_ref[...].astype(F32)
    for h in range(heads):
        bias_ref[:, span(h, res)] = (bias_plane(bwide_ref, h, heads).T + kmask) * LOG2E
    tri_attend(zc_ref, proj_ref, bias_ref, weo_ref, heads, rows, res, swap_after(zc_ref, ys_ref, yr_ref, 1))
    finish(moved[2] + moved[3])
    unpack_blocks(yr_ref, zs_ref, rows, res, ndap)
    for r in range(rows):
        out_ref[r] = zs_ref[span(r, res), :].astype(BF16)
    drain(early + swaps + sends + c1 + c3 + sum(moved, []) + [p1, p3])
    out_copy.wait()


def sds(shape, dtype):
    return jax.ShapeDtypeStruct(shape, dtype)


def solution(mesh):
    ndap = mesh.shape['dap']
    chips = ndap // 2

    def evoformer_block(msa, pair_act, full_mask, res_mask, row_bias_w, row_qkvg_w, row_out_w, col_query_w, col_kv_w, col_gate_w, col_out_w, opm_proj_w, opm_out_w, start_bias_w, start_qkvg_w, start_out_w, end_bias_w, end_qkvg_w, end_out_w):
        seqs, res, chans = msa.shape
        rows = pair_act.shape[0]
        heads, hd = row_qkvg_w.shape[2], row_qkvg_w.shape[3]
        width = heads * hd
        wide = opm_proj_w.shape[2]
        outc = opm_out_w.shape[2]
        thd = start_qkvg_w.shape[2] * start_qkvg_w.shape[3]
        theads = start_bias_w.shape[1]
        m_t = jnp.swapaxes(msa, 1, 2)
        wt = lambda w: w.reshape(w.shape[0], -1).T
        dma = pltpu.SemaphoreType.DMA

        nstat = heads + width // 2
        depth = 2
        npair = rows // 2
        nbuf = 2 * (chips // 2) - 1
        small = (rows * theads, res)
        block = (2, ndap, rows * rows // 2, outc)
        msa_scratch = (
            [VMEM((rows * heads, res), BF16), VMEM((2, chips, rows * heads, res), BF16), VMEM((2, chips, rows * heads, res), F32),
             VMEM((chans, res), F32), VMEM((chans // 2, res), F32), VMEM((chans // 2, res), F32), VMEM((chips, chans // 2, res), F32), VMEM((chans, res), F32),
             VMEM((2, nstat, res), F32), VMEM((nstat, res), F32), VMEM((nstat, res), F32), VMEM((chips, nstat, res), F32),
             VMEM((seqs, chans, res), BF16), VMEM((seqs, res), F32), VMEM((res, heads * res), F32),
             VMEM((chans, width), BF16), VMEM((chans, width), BF16), VMEM((2 * hd + width, chans), BF16),
             VMEM((seqs, width, res), BF16), VMEM((seqs, res, width + 16), BF16), VMEM((seqs, width, res), BF16), VMEM((seqs, width, res), BF16), VMEM((seqs, width, res), BF16),
             [VMEM((res, heads * res), F32)] * depth, [VMEM((heads, res, res), BF16)] * depth, [VMEM((1, heads * res), F32)] * depth,
             VMEM((seqs, 3 * hd, res), F32), VMEM((2 * hd, seqs, res), F32), VMEM((width, res), F32),
             VMEM((seqs, wide + 8, res), F32), VMEM((seqs, wide + 8, res), F32), VMEM((res, wide + 8, seqs), F32),
             dma((3, chips)), dma((3, chips)), dma((5,)), dma((5,))])
        pair_scratch = (
            [VMEM((chips, 2, rows * wide, seqs), BF16), VMEM((wide, seqs, res), BF16), VMEM((seqs, chans, res), BF16), dma(()),
             VMEM((chips, rows * wide, seqs), BF16), VMEM((wide, seqs, res), BF16),
             VMEM((chips, npair, outc, 2 * res), F32),
             VMEM((rows, 2 * wide * wide, res), BF16),
             VMEM((outc, 2 * wide * wide), BF16), VMEM((wide * wide, outc), F32), VMEM((res, res), F32),
             VMEM((nbuf, npair // 2, outc, 2 * res), F32), VMEM((nbuf, npair // 2, outc, 2 * res), F32),
             VMEM((rows * res, outc), F32), VMEM((rows * res, outc), F32), VMEM((rows * res, outc), BF16), VMEM((rows * res, 4 * thd), BF16), VMEM((res, theads * res), F32),
             VMEM((2, chips) + small, F32), VMEM(small, BF16), VMEM((2, chips) + small, BF16), VMEM(small, BF16), VMEM((2, chips) + small, BF16),
             VMEM(block, BF16), VMEM(block, BF16), VMEM(block, BF16), VMEM(block, BF16),
             dma((2,)), dma((2,)), dma((2, nbuf)), dma((2, nbuf)), dma((2, 2, ndap)), dma((2, 2, ndap)), dma((2, chips)), dma((2, chips)), dma((2,)), dma((2,))])
        vspec = pl.BlockSpec(memory_space=VMEM)
        m2, pair_out = pl.pallas_call(
            functools.partial(block_kernel, ndap=ndap, heads=heads, hd=hd),
            out_shape=[sds((seqs, chans, res), BF16), sds(pair_act.shape, BF16)],
            in_specs=[vspec] * 19,
            out_specs=[pl.BlockSpec(memory_space=pl.ANY), vspec],
            scratch_shapes=[msa_scratch, pair_scratch],
            compiler_params=pltpu.CompilerParams(vmem_limit_bytes=63 * 2 ** 20, collective_id=0, has_side_effects=True),
            name='evoformer_block',
        )(m_t, pair_act, full_mask, row_bias_w.T, wt(row_qkvg_w), row_out_w.reshape(width, chans), wt(col_query_w), wt(col_kv_w), wt(col_gate_w), col_out_w.reshape(width, chans), wt(opm_proj_w),
          res_mask.reshape(1, res), opm_out_w.reshape(wide * wide, outc),
          start_bias_w.T, wt(start_qkvg_w), start_out_w.reshape(thd, outc), end_bias_w.T, wt(end_qkvg_w), end_out_w.reshape(thd, outc))
        return jnp.swapaxes(m2, 1, 2), pair_out

    row_spec = P(('data', 'dap'), None, None)
    in_specs = (row_spec, row_spec, P('data', None), P('data')) + (P(),) * 15
    return jax.shard_map(evoformer_block, mesh=mesh, in_specs=in_specs, out_specs=(row_spec, row_spec), check_vma=False)
```

```python
import functools
import math

import jax
import jax.numpy as jnp
from jax import lax
from jax.experimental import pallas as pl
from jax.experimental.pallas import tpu as pltpu
from jax.sharding import PartitionSpec as P

F32 = jnp.float32
BF16 = jnp.bfloat16
MESH = pl.DeviceIdType.MESH
LOG2E = math.log2(math.e)
VMEM = pltpu.VMEM


def mm(left, right):
    return jnp.dot(left, right, preferred_element_type=F32)


def paired(w_ref, arrs):
    outs = []
    for n in range(0, len(arrs), 2):
        both = mm(w_ref[...], jnp.concatenate(arrs[n:n + 2], axis=1))
        width = arrs[n].shape[1]
        outs += [both[:, :width], both[:, width:]]
    return outs


def mm_nt(left, right):
    return lax.dot_general(left, right, (((1,), (1,)), ((), ())), preferred_element_type=F32)


def span(n, width):
    return slice(n * width, (n + 1) * width)


def sum0(x):
    return jnp.sum(x, axis=0, keepdims=True)


def max0(x):
    return jnp.max(x, axis=0, keepdims=True)


def ln_rows(x):
    n = x.shape[0]
    xc = x - sum0(x) * (1.0 / n)
    var = sum0(xc * xc) * (1.0 / n)
    return (xc * lax.rsqrt(var + 1e-5)).astype(BF16)


def ln_lanes(x):
    n = x.shape[1]
    xc = x - jnp.sum(x, axis=1, keepdims=True) * (1.0 / n)
    var = jnp.sum(xc * xc, axis=1, keepdims=True) * (1.0 / n)
    return (xc * lax.rsqrt(var + 1e-5)).astype(BF16)


def bf16_split(value, terms):
    import numpy as np
    out = []
    for _ in range(terms):
        t = float(np.asarray(value, dtype=jnp.bfloat16))
        out.append(t)
        value = value - t
    return out


def greet(me, ndap):
    for k in range(1, ndap):
        pl.semaphore_signal(pltpu.get_barrier_semaphore(), inc=1, device_id={'dap': lax.rem(me + k, ndap)}, device_id_type=MESH)


def await_group(ndap):
    pl.semaphore_wait(pltpu.get_barrier_semaphore(), ndap - 1)


def far_first(count):
    return sorted(range(1, count), key=lambda k: -min(k, count - k))


def remote(src, dst, send_sem, recv_sem, dev):
    cp = pltpu.make_async_remote_copy(src, dst, send_sem, recv_sem, device_id={'dap': dev}, device_id_type=MESH)
    cp.start()
    return cp


def start_gather(src_ref, slab_ref, chip, core, chips, send_sem, recv_sem):
    copies = [remote(src_ref, slab_ref.at[chip], send_sem.at[k], recv_sem.at[k], dap_index(chip + k, core, chips)) for k in far_first(chips)]
    slab_ref[chip] = src_ref[...]
    return copies


def start_swap(send_ref, recv_ref, me, ndap, send_sem, recv_sem):
    copies = []
    for k in far_first(ndap):
        other = lax.rem(me + k, ndap)
        cp = pltpu.make_async_remote_copy(send_ref.at[other], recv_ref.at[me], send_sem.at[k], recv_sem.at[k], device_id={'dap': other}, device_id_type=MESH)
        cp.start()
        copies.append(cp)
    recv_ref[me] = send_ref[me]
    return copies


def finish(copies):
    for cp in copies:
        cp.wait_recv()


def drain(copies):
    for cp in copies:
        cp.wait_send()


def strided(ref, row):
    return ref.reshape(ref.shape[0] * ref.shape[1], ref.shape[2])[pl.ds(row, ref.shape[0], stride=ref.shape[1]), :]


def pair_bias(z_ref, w_ref, out_ref):
    vals = [mm_nt(w_ref[...], ln_lanes(z_ref[r].astype(F32))) for r in range(z_ref.shape[0])]
    out_ref[...] = jnp.concatenate(vals, axis=0).astype(BF16)


def bias_plane(wide_ref, h, heads):
    rows = wide_ref.shape[2] // heads
    return jnp.concatenate([wide_ref[u, c, pl.ds(h, rows, stride=heads), :] for c in range(wide_ref.shape[1]) for u in range(2)], axis=0)


def row_project(m_ref, mask_ref, wqkvg_ref, q_ref, kt_ref, v_ref, g_ref, heads, hd, unroll=32):
    seqs, chans, res = m_ref.shape
    width = heads * hd
    aug = kt_ref.shape[2] - width
    terms = bf16_split(1e4 / hd ** -0.5, 3)
    rowi = lax.broadcasted_iota(jnp.int32, (aug, res), 0)
    mvec = jnp.where(rowi == 0, terms[0], jnp.where(rowi == 1, terms[1], jnp.where(rowi == 2, terms[2], 0.0)))

    def body(it, _):
        ids = [it * unroll + n for n in range(unroll)]
        for s, proj in zip(ids, paired(wqkvg_ref, [ln_rows(m_ref[s].astype(F32)) for s in ids])):
            q, k, v, g = [proj[span(n, width)].astype(BF16) for n in range(4)]
            q_ref[s], v_ref[s], g_ref[s] = q, v, g
            kt_ref[s] = jnp.concatenate([k.astype(F32), (mask_ref[pl.ds(s, 1), :] - 1.0) * mvec], axis=0).T.astype(BF16)
        return 0

    lax.fori_loop(0, seqs // unroll, body, 0)


def row_attend(bias_ref, q_ref, kt_ref, v_ref, g_ref, y_ref, s_refs, p_refs, l_refs, heads, hd, reps=4):
    seqs, width, res = q_ref.shape
    scale2 = hd ** -0.5 * LOG2E
    npairs = heads // 2
    aug = kt_ref.shape[2] - width
    two, both = 2 * hd, 2 * res
    first = lax.broadcasted_iota(jnp.int32, (two, res), 0) < hd
    zero16 = jnp.zeros((two, res), BF16)
    ones = jnp.ones((aug, res), BF16)

    def scores(s, s_ref, t):
        s = jnp.minimum(s, seqs - 1)
        q16 = q_ref[s, span(t, two)]
        halves = [jnp.concatenate([zero16] * t + [part] + [zero16] * (npairs - 1 - t) + [ones], axis=0)
                  for part in (jnp.where(first, q16, zero16), jnp.where(first, zero16, q16))]
        s_ref[:, span(t, both)] = mm(kt_ref[s], jnp.concatenate(halves, axis=1))

    def soft(s_ref, p_ref, l_ref, t):
        for h in (2 * t, 2 * t + 1):
            cols = span(h, res)
            x = s_ref[:, cols] * scale2 + bias_ref[:, cols]
            p = jnp.exp2(x - max0(x))
            l_ref[:, cols] = sum0(p)
            p_ref[h] = p.astype(BF16)

    def values(s, p_ref, l_ref, t):
        s = jnp.maximum(s, 0)
        o = mm(v_ref[s, span(t, two)], jnp.concatenate([p_ref[2 * t], p_ref[2 * t + 1]], axis=1))
        inv = 1.0 / l_ref[:, span(t, both)]
        att = jnp.concatenate([o[:hd, :res] * inv[:, :res], o[hd:, res:] * inv[:, res:]], axis=0)
        y_ref[s, span(t, two)] = (jax.nn.sigmoid(g_ref[s, span(t, two)].astype(F32)) * att).astype(BF16)

    depth = len(s_refs)
    lead = depth // 2
    for n in range(lead):
        for t in range(npairs):
            scores(n, s_refs[n], t)

    def body(it, _):
        for m in range(depth * reps):
            s = it * depth * reps + m
            n = m % depth
            far = (n + lead) % depth
            for t in range(npairs):
                values(s - lead, p_refs[far], l_refs[far], t)
                scores(s + lead, s_refs[far], t)
                soft(s_refs[n], p_refs[n], l_refs[n], t)
        return 0

    lax.fori_loop(0, seqs // (depth * reps), body, 0)
    for n in range(lead, depth):
        for t in range(npairs):
            values(seqs - depth + n, p_refs[n], l_refs[n], t)


def row_finish(m_ref, mask_ref, wo_ref, wkvg_ref, y_ref, m1_ref, kv_ref, g_ref, qsum_ref, hd, unroll=32):
    seqs, chans, res = m_ref.shape

    def body(it, _):
        ids = [it * unroll + n for n in range(unroll)]
        upds = paired(wo_ref, [y_ref[s] for s in ids])
        lns = []
        acc = jnp.zeros((chans, res), F32)
        for s, upd in zip(ids, upds):
            m1 = (m_ref[s].astype(F32) + upd).astype(BF16)
            m1_ref[s] = m1
            lns.append(ln_rows(m1.astype(F32)))
            acc = acc + lns[-1].astype(F32) * mask_ref[pl.ds(s, 1), :]
        qsum_ref[...] += acc
        for s, kvg in zip(ids, paired(wkvg_ref, lns)):
            kvg = kvg.astype(BF16)
            kv_ref[s, 0:2 * hd] = kvg[0:2 * hd].astype(F32)
            g_ref[s] = kvg[2 * hd:]
        return 0

    lax.fori_loop(0, seqs // unroll, body, 0)


def col_stats(qtot, cnt, mask_ref, wq_ref, planes_ref, stats_ref, heads, hd):
    seqs, res = mask_ref.shape
    qbar = (qtot / (cnt + 1e-10)).astype(BF16)
    q = mm(wq_ref[...], qbar).astype(BF16).astype(F32)
    mb = (mask_ref[...] - 1.0) * (1e4 * LOG2E)
    for h in range(heads):
        acc = q[h * hd:h * hd + 1] * planes_ref[0]
        for d in range(1, hd):
            acc = acc + q[h * hd + d:h * hd + d + 1] * planes_ref[d]
        t = acc * (hd ** -0.5 * LOG2E) + mb
        mx = max0(t)
        p = jnp.exp2(t - mx)
        half, k = h // (heads // 2), h % (heads // 2)
        stats_ref[half, k:k + 1, :] = mx
        stats_ref[half, heads // 2 + k:heads // 2 + k + 1, :] = sum0(p)
        pb = p.astype(BF16).astype(F32)
        for d in range(hd):
            r = heads + k * hd + d
            stats_ref[half, r:r + 1, :] = sum0(pb * planes_ref[hd + d])


def combine_stats(stats, heads, hd):
    gm = functools.reduce(jnp.maximum, [st[0:heads] for st in stats])
    spread = lambda f: jnp.concatenate([jnp.broadcast_to(f[h:h + 1], (hd, f.shape[1])) for h in range(heads)], axis=0)
    tot = wv = 0.0
    for st in stats:
        f = jnp.exp2(st[0:heads] - gm)
        tot = tot + f * st[heads:2 * heads]
        wv = wv + spread(f) * st[2 * heads:]
    return gm, tot, wv, spread


def col_finish(g_ref, m1_ref, mask_ref, wac_ref, m2_ref, a_ref, c_ref, o_ref, wo_ref, as_ref, cs_ref, at_ref, write_out, send_c, send_a):
    seqs, chans, res = m1_ref.shape
    wide = wac_ref.shape[0] // 2

    unroll = 32

    def body(it, _):
        ids = [it * unroll + n for n in range(unroll)]
        upds = paired(wo_ref, [(jax.nn.sigmoid(g_ref[s].astype(F32)) * o_ref[...]).astype(BF16) for s in ids])
        lns = []
        for s, upd in zip(ids, upds):
            m2 = (m1_ref[s].astype(F32) + upd).astype(BF16)
            m2_ref[s] = m2
            lns.append(ln_rows(m2.astype(F32)))
        for s, ac in zip(ids, paired(wac_ref, lns)):
            ac = ac.astype(BF16).astype(F32) * mask_ref[pl.ds(s, 1), :]
            as_ref[s, 0:wide] = ac[0:wide]
            cs_ref[s, 0:wide] = ac[wide:]
        return 0

    lax.fori_loop(0, seqs // unroll, body, 0)
    write_out()
    unroll = 8

    def planes_c(it, _):
        for n in range(unroll):
            e = it * unroll + n
            c_ref[e] = strided(cs_ref, e).astype(BF16)
        return 0

    def planes_a(it, _):
        flat = at_ref.reshape(res * at_ref.shape[1], seqs)
        for n in range(unroll):
            e = it * unroll + n
            flat[pl.ds(e, res, stride=at_ref.shape[1]), :] = strided(as_ref, e).T
        return 0

    lax.fori_loop(0, wide // unroll, planes_c, 0)
    send_c()
    lax.fori_loop(0, wide // unroll, planes_a, 0)
    rows = a_ref.shape[2] // wide
    for n in range(res):
        b, r = n // rows, n % rows
        a_ref[b // 2, b % 2, span(r, wide)] = at_ref[n, 0:wide].astype(BF16)
    send_a()


def msa_part(m_ref, z_ref, fmask_ref, wb_ref, wqkvg_ref, wout_ref, wq_ref, wkv_ref, wg_ref, wcout_ref, wac_ref, m2_ref, a_ref, c_ref, idle, hooks,
               bsend_ref, ball_ref, bwide_ref, qsum_ref, qpart_ref, qhalf_ref, qall_ref, qfin_ref, stat_ref, spart_ref, smerge_ref, sall_ref, m1_ref, mask_ref, bias_ref, wo_ref, wco_ref, wkvg_ref,
               q_ref, kt_ref, v_ref, g_ref, y_ref, s_refs, p_refs, l_refs, kv_ref, planes_ref, o_ref, as_ref, cs_ref, at_ref,
               send_sem, recv_sem, psend_sem, precv_sem, ndap, heads, hd):
    seqs, chans, res = m_ref.shape
    me = lax.axis_index('dap')
    chip, core = me // 2, lax.rem(me, 2)
    chips = ndap // 2
    partner = chip * 2 + 1 - core
    greet(me, ndap)
    pair_bias(z_ref, wb_ref, bsend_ref)
    await_group(ndap)
    bias_copies = start_gather(bsend_ref, ball_ref.at[core], chip, core, chips, send_sem.at[0], recv_sem.at[0])
    mask_ref[...] = fmask_ref[pl.ds(me * seqs, seqs), :].astype(F32)
    wo_ref[...] = wout_ref[...].astype(F32).T.astype(BF16)
    wco_ref[...] = wcout_ref[...].astype(F32).T.astype(BF16)
    wkvg_ref[0:2 * hd] = wkv_ref[...]
    wkvg_ref[2 * hd:] = wg_ref[...]
    qsum_ref[...] = jnp.zeros_like(qsum_ref)
    row_project(m_ref, mask_ref, wqkvg_ref, q_ref, kt_ref, v_ref, g_ref, heads, hd)
    finish(bias_copies)
    bias_swap = remote(ball_ref.at[core], ball_ref.at[core], psend_sem.at[0], precv_sem.at[0], partner)
    bias_swap.wait_recv()
    bwide_ref[...] = ball_ref[...].astype(F32)
    for h in range(heads):
        bias_ref[:, span(h, res)] = bias_plane(bwide_ref, h, heads).T * LOG2E
    row_attend(bias_ref, q_ref, kt_ref, v_ref, g_ref, y_ref, s_refs, p_refs, l_refs, heads, hd)
    row_finish(m_ref, mask_ref, wo_ref, wkvg_ref, y_ref, m1_ref, kv_ref, g_ref, qsum_ref, hd)

    half = chans // 2
    mine, other = pl.ds(core * half, half), pl.ds((1 - core) * half, half)
    sum_swap = remote(qsum_ref.at[other], qpart_ref, psend_sem.at[1], precv_sem.at[1], partner)
    cnt = sum0(fmask_ref[...]).astype(F32)
    sum_swap.wait_recv()
    qhalf_ref[...] = qsum_ref[mine, :] + qpart_ref[...]
    sum_copies = start_gather(qhalf_ref, qall_ref, chip, core, chips, send_sem.at[1], recv_sem.at[1])
    for d in range(2 * hd):
        planes_ref[d] = strided(kv_ref, d)
    finish(sum_copies)
    qfin_ref[mine, :] = functools.reduce(lambda x, y: x + y, [qall_ref[d] for d in range(chips)])
    fin_swap = remote(qfin_ref.at[mine], qfin_ref.at[mine], psend_sem.at[2], precv_sem.at[2], partner)
    fin_swap.wait_recv()
    col_stats(qfin_ref[...], cnt, mask_ref, wq_ref, planes_ref, stat_ref, heads, hd)

    stat_swap = remote(stat_ref.at[1 - core], spart_ref, psend_sem.at[3], precv_sem.at[3], partner)
    stat_swap.wait_recv()
    hh = heads // 2
    gm, tot, wv, _ = combine_stats([stat_ref[core], spart_ref[...]], hh, hd)
    smerge_ref[0:hh] = gm
    smerge_ref[hh:2 * hh] = tot
    smerge_ref[2 * hh:] = wv
    stat_copies = start_gather(smerge_ref, sall_ref, chip, core, chips, send_sem.at[2], recv_sem.at[2])
    idle()
    finish(stat_copies)
    gm, tot, wv, spread = combine_stats([sall_ref[d] for d in range(chips)], hh, hd)
    omine = pl.ds(core * hh * hd, hh * hd)
    o_ref[omine, :] = wv / spread(tot)
    out_swap = remote(o_ref.at[omine], o_ref.at[omine], psend_sem.at[4], precv_sem.at[4], partner)
    out_swap.wait_recv()
    col_finish(g_ref, m1_ref, mask_ref, wac_ref, m2_ref, a_ref, c_ref, o_ref, wco_ref, as_ref, cs_ref, at_ref, *hooks)
    return bias_copies + sum_copies + stat_copies + [bias_swap, sum_swap, fin_swap, stat_swap, out_swap]


def dap_index(chip, core, chips):
    return lax.rem(chip + 2 * chips, chips) * 2 + core


def outer_prepare(mask_ref, w_ref, wt_ref, w32_ref, cnt_ref, wide):
    depth, lanes = w_ref.shape
    w32_ref[...] = w_ref[...].astype(F32)
    per = lanes // wide
    for b in range(wide // per):
        cols = [w32_ref[pl.ds(b * per + f, wide, stride=wide), :] for f in range(per)]
        wt_ref[:, span(b, lanes)] = jnp.concatenate(cols, axis=0).T.astype(BF16)
    wt_ref[:, depth:] = wt_ref[:, :depth]
    res = mask_ref.shape[1]

    def count_step(n, acc):
        blk = mask_ref[pl.ds(n * res, res), :].astype(F32)
        return acc + mm(blk.T.astype(BF16), blk.astype(BF16))

    cnt_ref[...] = lax.fori_loop(0, mask_ref.shape[0] // res, count_step, jnp.zeros((res, res), F32))


def outer_mean(me, a_ref, c_ref, z_ref, zs_ref, ap_ref, cp_ref, part_ref, x_ref, wt_ref, cnt_ref, pos_ref, neg_ref, send_sem, recv_sem, chips):
    chip, core = me // 2, lax.rem(me, 2)
    wide, seqs, res = c_ref.shape
    rows = z_ref.shape[0]
    peer = {1: dap_index(chip + 1, core, chips), -1: dap_index(chip - 1, core, chips)}
    half_chips = chips // 2
    depth, unroll = wide * wide, 4

    def block(dest, slot):
        lhs = jnp.concatenate([a_ref[dest, core], ap_ref[dest]], axis=1)

        def outer(it, _):
            for n in range(unroll):
                f0 = (it * unroll + n) * 2
                rhs = [jnp.concatenate([c[f0], c[f0 + 1]], axis=1) for c in (c_ref, cp_ref)]
                o = mm(lhs, jnp.concatenate(rhs, axis=0))
                hi = o.astype(BF16)
                lo = (o - hi.astype(F32)).astype(BF16)
                for m, val in enumerate((hi, lo)):
                    for i in range(rows):
                        for u in range(2):
                            r0 = pl.multiple_of((f0 + u) * wide + m * depth, wide)
                            x_ref[i, pl.ds(r0, wide)] = val[span(i, wide), span(u, res)]
            return 0

        lax.fori_loop(0, wide // 2 // unroll, outer, 0)
        for n in range(rows // 2):
            part_ref[slot, n] = mm(wt_ref[...], jnp.concatenate([x_ref[2 * n], x_ref[2 * n + 1]], axis=1))

    sends = []
    arrivals = {}
    bufs = {1: pos_ref, -1: neg_ref}
    hq = rows // 4

    def hops(d, half):
        return half_chips if (half == 1) == (d == 1) else half_chips - 1

    slot_of = {}
    nbuf = 2 * half_chips - 1

    def buf_index(d, half, k):
        return (k - 1) + (0 if (half == 1) == (d == 1) else half_chips)

    def message(d, half, k, slot):
        idx = buf_index(d, half, k)
        src = part_ref.at[slot, pl.ds(half * hq, hq)]
        cp = pltpu.make_async_remote_copy(src, bufs[d].at[idx], send_sem.at[(d + 1) // 2, idx], recv_sem.at[(d + 1) // 2, idx], device_id={'dap': peer[d]}, device_id_type=MESH)
        arrivals[(d, half, k)] = cp
        sends.append(cp)
        cp.start()

    def take(d, half, k, slot):
        arrivals[(d, half, k)].wait_recv()
        part_ref[slot, span(half, hq)] += bufs[d][buf_index(d, half, k)]

    def dest_of(d, k):
        return lax.rem(chip + d * k + 2 * chips, chips)

    far = half_chips
    long_half = {1: 1, -1: 0}
    slots = {}

    def forward(long, k):
        for d in (1, -1):
            half = long_half[d] if long else 1 - long_half[d]
            take(d, half, k + 1, slots[(d, k)])
            message(d, half, k, slots[(d, k)])

    moves = []
    for k in range(far - 1, 0, -1):
        moves.append((True, k))
        if k > 1:
            moves.append((False, k - 1))
    todo = [(1, far)] + [(d, k) for k in range(far - 1, 0, -1) for d in (1, -1)] + [(1, 0)]
    for slot, (d, k) in enumerate(todo):
        slots[(d, k)] = slot
        block(dest_of(d, k), slot)
        if k == far:
            message(1, 1, far, slot)
            message(-1, 0, far, slot)
        elif k == far - 1:
            message(d, 1 - long_half[d], k, slot)
        if slot >= 3 and slot % 2 == 1 and slot < len(todo) - 1:
            forward(*moves.pop(0))
    for move in moves:
        forward(*move)
    for half in (0, 1):
        for d in (1, -1):
            take(d, half, 1, slot)
    for n in range(rows // 2):
        pair = part_ref[slot, n]
        for u in range(2):
            i = n * 2 + u
            cnt = cnt_ref[pl.ds(me * rows + i, 1), :] + 1e-3
            upd = (pair[:, span(u, res)] / cnt).T
            zs_ref[span(i, res), :] = (z_ref[i].astype(F32) + upd).astype(BF16).astype(F32)
    return sends


def tri_bias(zs_ref, ln_ref, w_ref, out_ref, rows, res):
    heads = w_ref.shape[0]
    vals = []
    for r in range(rows):
        ln = ln_lanes(zs_ref[span(r, res), :])
        if ln_ref is not None:
            ln_ref[span(r, res), :] = ln
        vals.append(mm_nt(w_ref[...], ln)[0:heads])
    out_ref[...] = jnp.concatenate(vals, axis=0).astype(BF16)


def tri_project(ln_ref, w_ref, proj_ref):
    step = 256
    for r in range(0, ln_ref.shape[0], step):
        proj_ref[r:r + step, :] = mm(ln_ref[r:r + step, :], w_ref[...]).astype(BF16)


def tri_attend(zs_ref, proj_ref, bias_ref, wout_ref, heads, rows, res, after):
    width = proj_ref.shape[1] // 4
    hd = width // heads
    scale2 = hd ** -0.5 * LOG2E
    lane = lax.broadcasted_iota(jnp.int32, (res, width), 1)
    mine = [(lane >= h * hd) & (lane < (h + 1) * hd) for h in range(heads)]
    deep = lax.broadcasted_iota(jnp.int32, (width, res), 0)
    under = [(deep >= h * hd) & (deep < (h + 1) * hd) for h in range(heads)]
    zero = jnp.zeros((res, width), BF16)

    def one(r0):
        part = lambda n: proj_ref[pl.ds(r0, res), span(n, width)]
        q, k, v, g = part(0), part(1), part(2), part(3)
        kt = k.T
        s = mm(q, jnp.concatenate([jnp.where(under[h], kt, zero) for h in range(heads)], axis=1))
        ps = []
        for h in range(heads):
            cols = span(h, res)
            x = s[:, cols] * scale2 + bias_ref[:, cols]
            p = jnp.exp2(x - jnp.max(x, axis=1, keepdims=True))
            ps.append((p * (1.0 / jnp.sum(p, axis=1, keepdims=True))).astype(BF16))
        o = mm(jnp.concatenate(ps, axis=1), jnp.concatenate([jnp.where(mine[h], v, zero) for h in range(heads)], axis=0))
        y = (jax.nn.sigmoid(g.astype(F32)) * o).astype(BF16)
        upd = mm(y, wout_ref[...])
        zs_ref[pl.ds(r0, res), :] = (zs_ref[pl.ds(r0, res), :] + upd).astype(BF16).astype(F32)

    part_rows = rows // 2
    for half in range(2):
        for n in range(part_rows):
            one((half * part_rows + n) * res)
        after(half)


def pack_blocks(zs_ref, send_ref, half, rows, res, ndap):
    few = rows // 2

    def one(q, _):
        parts = [zs_ref[pl.ds(half * few * res + q * rows + u, few, stride=res), :] for u in range(rows)]
        send_ref[half, q] = jnp.concatenate(parts, axis=0).astype(BF16)
        return 0

    lax.fori_loop(0, ndap, one, 0)


def unpack_blocks(recv_ref, dst_ref, rows, res, ndap):
    few = rows // 2
    for half in range(2):
        for p in range(ndap):
            blk = recv_ref[half, p].astype(F32)
            for u in range(rows):
                r0 = u * res + p * rows + half * few
                dst_ref[r0:r0 + few, :] = blk[span(u, few), :]


def block_kernel(m_ref, z_ref, fmask_ref, wb_ref, wqkvg_ref, wout_ref, wq_ref, wkv_ref, wg_ref, wcout_ref, wac_ref,
                 rmask_ref, w_ref, wsb_ref, wsp_ref, wso_ref, web_ref, wep_ref, weo_ref,
                 m2_ref, out_ref, msa_refs, pair_refs, *, ndap, heads, hd):
    (a_ref, c_ref, m2v_ref, out_sem, ap_ref, cp_ref, part_ref, x_ref, wt_ref, w32_ref, cnt_ref, pos_ref, neg_ref,
     zs_ref, zc_ref, ln_ref, proj_ref, bias_ref, bwide_ref, sb_ref, sball_ref, eb_ref, eball_ref, xs_ref, xr_ref, ys_ref, yr_ref, wsn_ref, wen_ref,
     ex_send, ex_recv, ring_send, ring_recv, send_sem, recv_sem, gsend, grecv, psend, precv) = pair_refs
    chips = ndap // 2
    me = lax.axis_index('dap')
    rows, res, _ = z_ref.shape
    chip, core = me // 2, lax.rem(me, 2)
    partner = chip * 2 + 1 - core
    swaps = []
    out_copy = pltpu.make_async_copy(m2v_ref, m2_ref, out_sem)

    def send_c():
        swaps.append(remote(c_ref, cp_ref, ex_send.at[0], ex_recv.at[0], partner))

    def send_a():
        swaps.append(remote(a_ref.at[:, 1 - core], ap_ref, ex_send.at[1], ex_recv.at[1], partner))

    def idle():
        outer_prepare(fmask_ref, w_ref, wt_ref, w32_ref, cnt_ref, c_ref.shape[0])
        wsn_ref[...] = wsp_ref[...].T
        wen_ref[...] = wep_ref[...].T

    early = msa_part(m_ref, z_ref, fmask_ref, wb_ref, wqkvg_ref, wout_ref, wq_ref, wkv_ref, wg_ref, wcout_ref, wac_ref, m2v_ref, a_ref, c_ref,
                     idle, (out_copy.start, send_c, send_a), *msa_refs, ndap, heads, hd)
    finish(swaps)
    sends = outer_mean(me, a_ref, c_ref, z_ref, zs_ref, ap_ref, cp_ref, part_ref, x_ref, wt_ref, cnt_ref, pos_ref, neg_ref, ring_send, ring_recv, chips)
    heads = wsb_ref.shape[0]
    kmask = (rmask_ref[...].astype(F32) - 1.0) * 1e4

    tri_bias(zs_ref, ln_ref, wsb_ref, sb_ref, rows, res)
    c1 = start_gather(sb_ref, sball_ref.at[core], chip, core, chips, gsend.at[0], grecv.at[0])
    tri_project(ln_ref, wsn_ref, proj_ref)
    finish(c1)
    p1 = remote(sball_ref.at[core], sball_ref.at[core], psend.at[0], precv.at[0], partner)
    p1.wait_recv()
    bwide_ref[...] = sball_ref[...].astype(F32)
    for h in range(heads):
        bias_ref[:, span(h, res)] = (bias_plane(bwide_ref, h, heads) + kmask) * LOG2E
    moved = []

    def swap_after(src_ref, send_ref, recv_ref, stage):
        def after(half):
            pack_blocks(src_ref, send_ref, half, rows, res, ndap)
            moved.append(start_swap(send_ref.at[half], recv_ref.at[half], me, ndap, send_sem.at[stage, half], recv_sem.at[stage, half]))
        return after

    tri_attend(zs_ref, proj_ref, bias_ref, wso_ref, heads, rows, res, swap_after(zs_ref, xs_ref, xr_ref, 0))
    tri_bias(zs_ref, None, web_ref, eb_ref, rows, res)
    c3 = start_gather(eb_ref, eball_ref.at[core], chip, core, chips, gsend.at[1], grecv.at[1])
    drain(early + swaps)
    finish(moved[0] + moved[1])
    finish(c3)
    p3 = remote(eball_ref.at[core], eball_ref.at[core], psend.at[1], precv.at[1], partner)
    unpack_blocks(xr_ref, zc_ref, rows, res, ndap)
    for r in range(rows):
        ln_ref[span(r, res), :] = ln_lanes(zc_ref[span(r, res), :])
    tri_project(ln_ref, wen_ref, proj_ref)
    p3.wait_recv()
    bwide_ref[...] = eball_ref[...].astype(F32)
    for h in range(heads):
        bias_ref[:, span(h, res)] = (bias_plane(bwide_ref, h, heads).T + kmask) * LOG2E
    tri_attend(zc_ref, proj_ref, bias_ref, weo_ref, heads, rows, res, swap_after(zc_ref, ys_ref, yr_ref, 1))
    drain(sends + c1 + c3 + moved[0] + moved[1] + [p1, p3])
    finish(moved[2] + moved[3])
    unpack_blocks(yr_ref, zs_ref, rows, res, ndap)
    for r in range(rows):
        out_ref[r] = zs_ref[span(r, res), :].astype(BF16)
    drain(moved[2] + moved[3])
    out_copy.wait()


def sds(shape, dtype):
    return jax.ShapeDtypeStruct(shape, dtype)


def solution(mesh):
    ndap = mesh.shape['dap']
    chips = ndap // 2

    def evoformer_block(msa, pair_act, full_mask, res_mask, row_bias_w, row_qkvg_w, row_out_w, col_query_w, col_kv_w, col_gate_w, col_out_w, opm_proj_w, opm_out_w, start_bias_w, start_qkvg_w, start_out_w, end_bias_w, end_qkvg_w, end_out_w):
        seqs, res, chans = msa.shape
        rows = pair_act.shape[0]
        heads, hd = row_qkvg_w.shape[2], row_qkvg_w.shape[3]
        width = heads * hd
        wide = opm_proj_w.shape[2]
        outc = opm_out_w.shape[2]
        thd = start_qkvg_w.shape[2] * start_qkvg_w.shape[3]
        theads = start_bias_w.shape[1]
        m_t = jnp.swapaxes(msa, 1, 2)
        wt = lambda w: w.reshape(w.shape[0], -1).T
        dma = pltpu.SemaphoreType.DMA

        nstat = heads + width // 2
        depth = 2
        npair = rows // 2
        nbuf = 2 * (chips // 2) - 1
        small = (rows * theads, res)
        block = (2, ndap, rows * rows // 2, outc)
        msa_scratch = (
            [VMEM((rows * heads, res), BF16), VMEM((2, chips, rows * heads, res), BF16), VMEM((2, chips, rows * heads, res), F32),
             VMEM((chans, res), F32), VMEM((chans // 2, res), F32), VMEM((chans // 2, res), F32), VMEM((chips, chans // 2, res), F32), VMEM((chans, res), F32),
             VMEM((2, nstat, res), F32), VMEM((nstat, res), F32), VMEM((nstat, res), F32), VMEM((chips, nstat, res), F32),
             VMEM((seqs, chans, res), BF16), VMEM((seqs, res), F32), VMEM((res, heads * res), F32),
             VMEM((chans, width), BF16), VMEM((chans, width), BF16), VMEM((2 * hd + width, chans), BF16),
             VMEM((seqs, width, res), BF16), VMEM((seqs, res, width + 16), BF16), VMEM((seqs, width, res), BF16), VMEM((seqs, width, res), BF16), VMEM((seqs, width, res), BF16),
             [VMEM((res, heads * res), F32)] * depth, [VMEM((heads, res, res), BF16)] * depth, [VMEM((1, heads * res), F32)] * depth,
             VMEM((seqs, 3 * hd, res), F32), VMEM((2 * hd, seqs, res), F32), VMEM((width, res), F32),
             VMEM((seqs, wide + 8, res), F32), VMEM((seqs, wide + 8, res), F32), VMEM((res, wide + 8, seqs), F32),
             dma((3, chips)), dma((3, chips)), dma((5,)), dma((5,))])
        pair_scratch = (
            [VMEM((chips, 2, rows * wide, seqs), BF16), VMEM((wide, seqs, res), BF16), VMEM((seqs, chans, res), BF16), dma(()),
             VMEM((chips, rows * wide, seqs), BF16), VMEM((wide, seqs, res), BF16),
             VMEM((chips, npair, outc, 2 * res), F32),
             VMEM((rows, 2 * wide * wide, res), BF16),
             VMEM((outc, 2 * wide * wide), BF16), VMEM((wide * wide, outc), F32), VMEM((res, res), F32),
             VMEM((nbuf, npair // 2, outc, 2 * res), F32), VMEM((nbuf, npair // 2, outc, 2 * res), F32),
             VMEM((rows * res, outc), F32), VMEM((rows * res, outc), F32), VMEM((rows * res, outc), BF16), VMEM((rows * res, 4 * thd), BF16), VMEM((res, theads * res), F32),
             VMEM((2, chips) + small, F32), VMEM(small, BF16), VMEM((2, chips) + small, BF16), VMEM(small, BF16), VMEM((2, chips) + small, BF16),
             VMEM(block, BF16), VMEM(block, BF16), VMEM(block, BF16), VMEM(block, BF16), VMEM((outc, 4 * thd), BF16), VMEM((outc, 4 * thd), BF16),
             dma((2,)), dma((2,)), dma((2, nbuf)), dma((2, nbuf)), dma((2, 2, ndap)), dma((2, 2, ndap)), dma((2, chips)), dma((2, chips)), dma((2,)), dma((2,))])
        vspec = pl.BlockSpec(memory_space=VMEM)
        m2, pair_out = pl.pallas_call(
            functools.partial(block_kernel, ndap=ndap, heads=heads, hd=hd),
            out_shape=[sds((seqs, chans, res), BF16), sds(pair_act.shape, BF16)],
            in_specs=[vspec] * 19,
            out_specs=[pl.BlockSpec(memory_space=pl.ANY), vspec],
            scratch_shapes=[msa_scratch, pair_scratch],
            compiler_params=pltpu.CompilerParams(vmem_limit_bytes=63 * 2 ** 20, collective_id=0, has_side_effects=True),
            name='evoformer_block',
        )(m_t, pair_act, full_mask, row_bias_w.T, wt(row_qkvg_w), row_out_w.reshape(width, chans), wt(col_query_w), wt(col_kv_w), wt(col_gate_w), col_out_w.reshape(width, chans), wt(opm_proj_w),
          res_mask.reshape(1, res), opm_out_w.reshape(wide * wide, outc),
          start_bias_w.T, wt(start_qkvg_w), start_out_w.reshape(thd, outc), end_bias_w.T, wt(end_qkvg_w), end_out_w.reshape(thd, outc))
        return jnp.swapaxes(m2, 1, 2), pair_out

    row_spec = P(('data', 'dap'), None, None)
    in_specs = (row_spec, row_spec, P('data', None), P('data')) + (P(),) * 15
    return jax.shard_map(evoformer_block, mesh=mesh, in_specs=in_specs, out_specs=(row_spec, row_spec), check_vma=False)
```

```python
import functools
import math

import jax
import jax.numpy as jnp
from jax import lax
from jax.experimental import pallas as pl
from jax.experimental.pallas import tpu as pltpu
from jax.sharding import PartitionSpec as P

F32 = jnp.float32
BF16 = jnp.bfloat16
MESH = pl.DeviceIdType.MESH
LOG2E = math.log2(math.e)
VMEM = pltpu.VMEM


def mm(left, right):
    return jnp.dot(left, right, preferred_element_type=F32)


def paired(w_ref, arrs):
    outs = []
    for n in range(0, len(arrs), 2):
        both = mm(w_ref[...], jnp.concatenate(arrs[n:n + 2], axis=1))
        width = arrs[n].shape[1]
        outs += [both[:, :width], both[:, width:]]
    return outs


def mm_nt(left, right):
    return lax.dot_general(left, right, (((1,), (1,)), ((), ())), preferred_element_type=F32)


def span(n, width):
    return slice(n * width, (n + 1) * width)


def sum0(x):
    return jnp.sum(x, axis=0, keepdims=True)


def max0(x):
    return jnp.max(x, axis=0, keepdims=True)


def ln_rows(x):
    n = x.shape[0]
    xc = x - sum0(x) * (1.0 / n)
    var = sum0(xc * xc) * (1.0 / n)
    return (xc * lax.rsqrt(var + 1e-5)).astype(BF16)


def ln_lanes(x):
    n = x.shape[1]
    xc = x - jnp.sum(x, axis=1, keepdims=True) * (1.0 / n)
    var = jnp.sum(xc * xc, axis=1, keepdims=True) * (1.0 / n)
    return (xc * lax.rsqrt(var + 1e-5)).astype(BF16)


def bf16_split(value, terms):
    import numpy as np
    out = []
    for _ in range(terms):
        t = float(np.asarray(value, dtype=jnp.bfloat16))
        out.append(t)
        value = value - t
    return out


def greet(me, ndap):
    for k in range(1, ndap):
        pl.semaphore_signal(pltpu.get_barrier_semaphore(), inc=1, device_id={'dap': lax.rem(me + k, ndap)}, device_id_type=MESH)


def await_group(ndap):
    pl.semaphore_wait(pltpu.get_barrier_semaphore(), ndap - 1)


def far_first(count):
    return sorted(range(1, count), key=lambda k: -min(k, count - k))


def remote(src, dst, send_sem, recv_sem, dev):
    cp = pltpu.make_async_remote_copy(src, dst, send_sem, recv_sem, device_id={'dap': dev}, device_id_type=MESH)
    cp.start()
    return cp


def start_gather(src_ref, slab_ref, chip, core, chips, send_sem, recv_sem):
    copies = [remote(src_ref, slab_ref.at[chip], send_sem.at[k], recv_sem.at[k], dap_index(chip + k, core, chips)) for k in far_first(chips)]
    slab_ref[chip] = src_ref[...]
    return copies


def start_swap(send_ref, recv_ref, me, ndap, send_sem, recv_sem):
    copies = []
    for k in far_first(ndap):
        other = lax.rem(me + k, ndap)
        cp = pltpu.make_async_remote_copy(send_ref.at[other], recv_ref.at[me], send_sem.at[k], recv_sem.at[k], device_id={'dap': other}, device_id_type=MESH)
        cp.start()
        copies.append(cp)
    recv_ref[me] = send_ref[me]
    return copies


def finish(copies):
    for cp in copies:
        cp.wait_recv()


def drain(copies):
    for cp in copies:
        cp.wait_send()


def strided(ref, row):
    return ref.reshape(ref.shape[0] * ref.shape[1], ref.shape[2])[pl.ds(row, ref.shape[0], stride=ref.shape[1]), :]


def pair_bias(z_ref, w_ref, out_ref):
    vals = [mm_nt(w_ref[...], ln_lanes(z_ref[r].astype(F32))) for r in range(z_ref.shape[0])]
    out_ref[...] = jnp.concatenate(vals, axis=0).astype(BF16)


def bias_plane(wide_ref, h, heads):
    rows = wide_ref.shape[2] // heads
    return jnp.concatenate([wide_ref[u, c, pl.ds(h, rows, stride=heads), :] for c in range(wide_ref.shape[1]) for u in range(2)], axis=0)


def row_project(m_ref, mask_ref, wqkvg_ref, q_ref, kt_ref, v_ref, g_ref, heads, hd, unroll=32):
    seqs, chans, res = m_ref.shape
    width = heads * hd
    aug = kt_ref.shape[2] - width
    terms = bf16_split(1e4 / hd ** -0.5, 3)
    rowi = lax.broadcasted_iota(jnp.int32, (aug, res), 0)
    mvec = jnp.where(rowi == 0, terms[0], jnp.where(rowi == 1, terms[1], jnp.where(rowi == 2, terms[2], 0.0)))

    def body(it, _):
        ids = [it * unroll + n for n in range(unroll)]
        for s, proj in zip(ids, paired(wqkvg_ref, [ln_rows(m_ref[s].astype(F32)) for s in ids])):
            q, k, v, g = [proj[span(n, width)].astype(BF16) for n in range(4)]
            q_ref[s], v_ref[s], g_ref[s] = q, v, g
            kt_ref[s] = jnp.concatenate([k.astype(F32), (mask_ref[pl.ds(s, 1), :] - 1.0) * mvec], axis=0).T.astype(BF16)
        return 0

    lax.fori_loop(0, seqs // unroll, body, 0)


def row_attend(bias_ref, q_ref, kt_ref, v_ref, g_ref, y_ref, s_refs, p_refs, l_refs, heads, hd, reps=8):
    seqs, width, res = q_ref.shape
    scale2 = hd ** -0.5 * LOG2E
    npairs = heads // 2
    aug = kt_ref.shape[2] - width
    two, both = 2 * hd, 2 * res
    first = lax.broadcasted_iota(jnp.int32, (two, res), 0) < hd
    zero16 = jnp.zeros((two, res), BF16)
    ones = jnp.ones((aug, res), BF16)

    def scores(s, s_ref, t):
        s = jnp.minimum(s, seqs - 1)
        q16 = q_ref[s, span(t, two)]
        halves = [jnp.concatenate([zero16] * t + [part] + [zero16] * (npairs - 1 - t) + [ones], axis=0)
                  for part in (jnp.where(first, q16, zero16), jnp.where(first, zero16, q16))]
        s_ref[:, span(t, both)] = mm(kt_ref[s], jnp.concatenate(halves, axis=1))

    def soft(s_ref, p_ref, l_ref, t):
        for h in (2 * t, 2 * t + 1):
            cols = span(h, res)
            x = s_ref[:, cols] * scale2 + bias_ref[:, cols]
            p = jnp.exp2(x - max0(x))
            l_ref[:, cols] = sum0(p)
            p_ref[h] = p.astype(BF16)

    def values(s, p_ref, l_ref, t):
        s = jnp.maximum(s, 0)
        o = mm(v_ref[s, span(t, two)], jnp.concatenate([p_ref[2 * t], p_ref[2 * t + 1]], axis=1))
        inv = 1.0 / l_ref[:, span(t, both)]
        att = jnp.concatenate([o[:hd, :res] * inv[:, :res], o[hd:, res:] * inv[:, res:]], axis=0)
        y_ref[s, span(t, two)] = (jax.nn.sigmoid(g_ref[s, span(t, two)].astype(F32)) * att).astype(BF16)

    depth = len(s_refs)
    lead = depth // 2
    for n in range(lead):
        for t in range(npairs):
            scores(n, s_refs[n], t)

    def body(it, _):
        for m in range(depth * reps):
            s = it * depth * reps + m
            n = m % depth
            far = (n + lead) % depth
            for t in range(npairs):
                values(s - lead, p_refs[far], l_refs[far], t)
                scores(s + lead, s_refs[far], t)
                soft(s_refs[n], p_refs[n], l_refs[n], t)
        return 0

    lax.fori_loop(0, seqs // (depth * reps), body, 0)
    for n in range(lead, depth):
        for t in range(npairs):
            values(seqs - depth + n, p_refs[n], l_refs[n], t)


def row_finish(m_ref, mask_ref, wo_ref, wkvg_ref, y_ref, m1_ref, kv_ref, g_ref, qsum_ref, hd, unroll=32):
    seqs, chans, res = m_ref.shape

    def body(it, _):
        ids = [it * unroll + n for n in range(unroll)]
        upds = paired(wo_ref, [y_ref[s] for s in ids])
        lns = []
        acc = jnp.zeros((chans, res), F32)
        for s, upd in zip(ids, upds):
            m1 = (m_ref[s].astype(F32) + upd).astype(BF16)
            m1_ref[s] = m1
            lns.append(ln_rows(m1.astype(F32)))
            acc = acc + lns[-1].astype(F32) * mask_ref[pl.ds(s, 1), :]
        qsum_ref[...] += acc
        for s, kvg in zip(ids, paired(wkvg_ref, lns)):
            kvg = kvg.astype(BF16)
            kv_ref[s, 0:2 * hd] = kvg[0:2 * hd].astype(F32)
            g_ref[s] = kvg[2 * hd:]
        return 0

    lax.fori_loop(0, seqs // unroll, body, 0)


def col_stats(qtot, cnt, mask_ref, wq_ref, planes_ref, stats_ref, heads, hd):
    seqs, res = mask_ref.shape
    qbar = (qtot / (cnt + 1e-10)).astype(BF16)
    q = mm(wq_ref[...], qbar).astype(BF16).astype(F32)
    mb = (mask_ref[...] - 1.0) * (1e4 * LOG2E)
    for h in range(heads):
        acc = q[h * hd:h * hd + 1] * planes_ref[0]
        for d in range(1, hd):
            acc = acc + q[h * hd + d:h * hd + d + 1] * planes_ref[d]
        t = acc * (hd ** -0.5 * LOG2E) + mb
        mx = max0(t)
        p = jnp.exp2(t - mx)
        half, k = h // (heads // 2), h % (heads // 2)
        stats_ref[half, k:k + 1, :] = mx
        stats_ref[half, heads // 2 + k:heads // 2 + k + 1, :] = sum0(p)
        pb = p.astype(BF16).astype(F32)
        for d in range(hd):
            r = heads + k * hd + d
            stats_ref[half, r:r + 1, :] = sum0(pb * planes_ref[hd + d])


def combine_stats(stats, heads, hd):
    gm = functools.reduce(jnp.maximum, [st[0:heads] for st in stats])
    spread = lambda f: jnp.concatenate([jnp.broadcast_to(f[h:h + 1], (hd, f.shape[1])) for h in range(heads)], axis=0)
    tot = wv = 0.0
    for st in stats:
        f = jnp.exp2(st[0:heads] - gm)
        tot = tot + f * st[heads:2 * heads]
        wv = wv + spread(f) * st[2 * heads:]
    return gm, tot, wv, spread


def col_finish(g_ref, m1_ref, mask_ref, wac_ref, m2_ref, a_ref, c_ref, o_ref, wo_ref, as_ref, cs_ref, at_ref, write_out, send_c, send_a):
    seqs, chans, res = m1_ref.shape
    wide = wac_ref.shape[0] // 2

    unroll = 32

    def body(it, _):
        ids = [it * unroll + n for n in range(unroll)]
        upds = paired(wo_ref, [(jax.nn.sigmoid(g_ref[s].astype(F32)) * o_ref[...]).astype(BF16) for s in ids])
        lns = []
        for s, upd in zip(ids, upds):
            m2 = (m1_ref[s].astype(F32) + upd).astype(BF16)
            m2_ref[s] = m2
            lns.append(ln_rows(m2.astype(F32)))
        for s, ac in zip(ids, paired(wac_ref, lns)):
            ac = ac.astype(BF16).astype(F32) * mask_ref[pl.ds(s, 1), :]
            as_ref[s, 0:wide] = ac[0:wide]
            cs_ref[s, 0:wide] = ac[wide:]
        return 0

    lax.fori_loop(0, seqs // unroll, body, 0)
    write_out()
    unroll = 16

    def planes_c(it, _):
        for n in range(unroll):
            e = it * unroll + n
            c_ref[e] = strided(cs_ref, e).astype(BF16)
        return 0

    def planes_a(it, _):
        flat = at_ref.reshape(res * at_ref.shape[1], seqs)
        for n in range(unroll):
            e = it * unroll + n
            flat[pl.ds(e, res, stride=at_ref.shape[1]), :] = strided(as_ref, e).T
        return 0

    lax.fori_loop(0, wide // unroll, planes_c, 0)
    send_c()
    lax.fori_loop(0, wide // unroll, planes_a, 0)
    rows = a_ref.shape[2] // wide
    for n in range(res):
        b, r = n // rows, n % rows
        a_ref[b // 2, b % 2, span(r, wide)] = at_ref[n, 0:wide].astype(BF16)
    send_a()


def msa_part(m_ref, z_ref, fmask_ref, wb_ref, wqkvg_ref, wout_ref, wq_ref, wkv_ref, wg_ref, wcout_ref, wac_ref, m2_ref, a_ref, c_ref, idle, hooks,
               bsend_ref, ball_ref, bwide_ref, qsum_ref, qpart_ref, qhalf_ref, qall_ref, qfin_ref, stat_ref, spart_ref, smerge_ref, sall_ref, m1_ref, mask_ref, bias_ref, wo_ref, wco_ref, wkvg_ref,
               q_ref, kt_ref, v_ref, g_ref, y_ref, s_refs, p_refs, l_refs, kv_ref, planes_ref, o_ref, as_ref, cs_ref, at_ref,
               send_sem, recv_sem, psend_sem, precv_sem, ndap, heads, hd):
    seqs, chans, res = m_ref.shape
    me = lax.axis_index('dap')
    chip, core = me // 2, lax.rem(me, 2)
    chips = ndap // 2
    partner = chip * 2 + 1 - core
    greet(me, ndap)
    pair_bias(z_ref, wb_ref, bsend_ref)
    await_group(ndap)
    bias_copies = start_gather(bsend_ref, ball_ref.at[core], chip, core, chips, send_sem.at[0], recv_sem.at[0])
    mask_ref[...] = fmask_ref[pl.ds(me * seqs, seqs), :].astype(F32)
    wo_ref[...] = wout_ref[...].astype(F32).T.astype(BF16)
    wco_ref[...] = wcout_ref[...].astype(F32).T.astype(BF16)
    wkvg_ref[0:2 * hd] = wkv_ref[...]
    wkvg_ref[2 * hd:] = wg_ref[...]
    qsum_ref[...] = jnp.zeros_like(qsum_ref)
    row_project(m_ref, mask_ref, wqkvg_ref, q_ref, kt_ref, v_ref, g_ref, heads, hd)
    finish(bias_copies)
    bias_swap = remote(ball_ref.at[core], ball_ref.at[core], psend_sem.at[0], precv_sem.at[0], partner)
    bias_swap.wait_recv()
    bwide_ref[...] = ball_ref[...].astype(F32)
    for h in range(heads):
        bias_ref[:, span(h, res)] = bias_plane(bwide_ref, h, heads).T * LOG2E
    row_attend(bias_ref, q_ref, kt_ref, v_ref, g_ref, y_ref, s_refs, p_refs, l_refs, heads, hd)
    row_finish(m_ref, mask_ref, wo_ref, wkvg_ref, y_ref, m1_ref, kv_ref, g_ref, qsum_ref, hd)

    half = chans // 2
    mine, other = pl.ds(core * half, half), pl.ds((1 - core) * half, half)
    sum_swap = remote(qsum_ref.at[other], qpart_ref, psend_sem.at[1], precv_sem.at[1], partner)
    cnt = sum0(fmask_ref[...]).astype(F32)
    sum_swap.wait_recv()
    qhalf_ref[...] = qsum_ref[mine, :] + qpart_ref[...]
    sum_copies = start_gather(qhalf_ref, qall_ref, chip, core, chips, send_sem.at[1], recv_sem.at[1])
    for d in range(2 * hd):
        planes_ref[d] = strided(kv_ref, d)
    finish(sum_copies)
    qfin_ref[mine, :] = functools.reduce(lambda x, y: x + y, [qall_ref[d] for d in range(chips)])
    fin_swap = remote(qfin_ref.at[mine], qfin_ref.at[mine], psend_sem.at[2], precv_sem.at[2], partner)
    fin_swap.wait_recv()
    col_stats(qfin_ref[...], cnt, mask_ref, wq_ref, planes_ref, stat_ref, heads, hd)

    stat_swap = remote(stat_ref.at[1 - core], spart_ref, psend_sem.at[3], precv_sem.at[3], partner)
    stat_swap.wait_recv()
    hh = heads // 2
    gm, tot, wv, _ = combine_stats([stat_ref[core], spart_ref[...]], hh, hd)
    smerge_ref[0:hh] = gm
    smerge_ref[hh:2 * hh] = tot
    smerge_ref[2 * hh:] = wv
    stat_copies = start_gather(smerge_ref, sall_ref, chip, core, chips, send_sem.at[2], recv_sem.at[2])
    idle()
    finish(stat_copies)
    gm, tot, wv, spread = combine_stats([sall_ref[d] for d in range(chips)], hh, hd)
    omine = pl.ds(core * hh * hd, hh * hd)
    o_ref[omine, :] = wv / spread(tot)
    out_swap = remote(o_ref.at[omine], o_ref.at[omine], psend_sem.at[4], precv_sem.at[4], partner)
    out_swap.wait_recv()
    col_finish(g_ref, m1_ref, mask_ref, wac_ref, m2_ref, a_ref, c_ref, o_ref, wco_ref, as_ref, cs_ref, at_ref, *hooks)
    return bias_copies + sum_copies + stat_copies + [bias_swap, sum_swap, fin_swap, stat_swap, out_swap]


def dap_index(chip, core, chips):
    return lax.rem(chip + 2 * chips, chips) * 2 + core


def outer_prepare(mask_ref, w_ref, wt_ref, w32_ref, cnt_ref, wide):
    depth, lanes = w_ref.shape
    w32_ref[...] = w_ref[...].astype(F32)
    per = lanes // wide
    for b in range(wide // per):
        cols = [w32_ref[pl.ds(b * per + f, wide, stride=wide), :] for f in range(per)]
        wt_ref[:, span(b, lanes)] = jnp.concatenate(cols, axis=0).T.astype(BF16)
    wt_ref[:, depth:] = wt_ref[:, :depth]
    res = mask_ref.shape[1]

    def count_step(n, acc):
        blk = mask_ref[pl.ds(n * res, res), :].astype(F32)
        return acc + mm(blk.T.astype(BF16), blk.astype(BF16))

    cnt_ref[...] = lax.fori_loop(0, mask_ref.shape[0] // res, count_step, jnp.zeros((res, res), F32))


def outer_mean(me, a_ref, c_ref, z_ref, zs_ref, ap_ref, cp_ref, part_ref, x_ref, wt_ref, cnt_ref, pos_ref, neg_ref, send_sem, recv_sem, chips):
    chip, core = me // 2, lax.rem(me, 2)
    wide, seqs, res = c_ref.shape
    rows = z_ref.shape[0]
    peer = {1: dap_index(chip + 1, core, chips), -1: dap_index(chip - 1, core, chips)}
    half_chips = chips // 2
    depth, unroll = wide * wide, 4

    def block(dest, slot):
        lhs = jnp.concatenate([a_ref[dest, core], ap_ref[dest]], axis=1)

        def outer(it, _):
            for n in range(unroll):
                f0 = (it * unroll + n) * 2
                rhs = [jnp.concatenate([c[f0], c[f0 + 1]], axis=1) for c in (c_ref, cp_ref)]
                o = mm(lhs, jnp.concatenate(rhs, axis=0))
                hi = o.astype(BF16)
                lo = (o - hi.astype(F32)).astype(BF16)
                for m, val in enumerate((hi, lo)):
                    for i in range(rows):
                        for u in range(2):
                            r0 = pl.multiple_of((f0 + u) * wide + m * depth, wide)
                            x_ref[i, pl.ds(r0, wide)] = val[span(i, wide), span(u, res)]
            return 0

        lax.fori_loop(0, wide // 2 // unroll, outer, 0)
        for n in range(rows // 2):
            part_ref[slot, n] = mm(wt_ref[...], jnp.concatenate([x_ref[2 * n], x_ref[2 * n + 1]], axis=1))

    sends = []
    arrivals = {}
    bufs = {1: pos_ref, -1: neg_ref}
    hq = rows // 4

    def hops(d, half):
        return half_chips if (half == 1) == (d == 1) else half_chips - 1

    slot_of = {}
    nbuf = 2 * half_chips - 1

    def buf_index(d, half, k):
        return (k - 1) + (0 if (half == 1) == (d == 1) else half_chips)

    def message(d, half, k, slot):
        idx = buf_index(d, half, k)
        src = part_ref.at[slot, pl.ds(half * hq, hq)]
        cp = pltpu.make_async_remote_copy(src, bufs[d].at[idx], send_sem.at[(d + 1) // 2, idx], recv_sem.at[(d + 1) // 2, idx], device_id={'dap': peer[d]}, device_id_type=MESH)
        arrivals[(d, half, k)] = cp
        sends.append(cp)
        cp.start()

    def take(d, half, k, slot):
        arrivals[(d, half, k)].wait_recv()
        part_ref[slot, span(half, hq)] += bufs[d][buf_index(d, half, k)]

    def dest_of(d, k):
        return lax.rem(chip + d * k + 2 * chips, chips)

    far = half_chips
    long_half = {1: 1, -1: 0}
    slots = {}

    def forward(long, k):
        for d in (1, -1):
            half = long_half[d] if long else 1 - long_half[d]
            take(d, half, k + 1, slots[(d, k)])
            message(d, half, k, slots[(d, k)])

    moves = []
    for k in range(far - 1, 0, -1):
        moves.append((True, k))
        if k > 1:
            moves.append((False, k - 1))
    todo = [(1, far)] + [(d, k) for k in range(far - 1, 0, -1) for d in (1, -1)] + [(1, 0)]
    for slot, (d, k) in enumerate(todo):
        slots[(d, k)] = slot
        block(dest_of(d, k), slot)
        if k == far:
            message(1, 1, far, slot)
            message(-1, 0, far, slot)
        elif k == far - 1:
            message(d, 1 - long_half[d], k, slot)
        if slot >= 3 and slot % 2 == 1 and slot < len(todo) - 1:
            forward(*moves.pop(0))
    for move in moves:
        forward(*move)
    for half in (0, 1):
        for d in (1, -1):
            take(d, half, 1, slot)
    for n in range(rows // 2):
        pair = part_ref[slot, n]
        for u in range(2):
            i = n * 2 + u
            cnt = cnt_ref[pl.ds(me * rows + i, 1), :] + 1e-3
            upd = (pair[:, span(u, res)] / cnt).T
            zs_ref[span(i, res), :] = (z_ref[i].astype(F32) + upd).astype(BF16).astype(F32)
    return sends


def tri_bias(zs_ref, ln_ref, w_ref, out_ref, rows, res):
    heads = w_ref.shape[0]
    vals = []
    for r in range(rows):
        ln = ln_lanes(zs_ref[span(r, res), :])
        if ln_ref is not None:
            ln_ref[span(r, res), :] = ln
        vals.append(mm_nt(w_ref[...], ln)[0:heads])
    out_ref[...] = jnp.concatenate(vals, axis=0).astype(BF16)


def tri_project(ln_ref, w_ref, proj_ref):
    step = 256
    for r in range(0, ln_ref.shape[0], step):
        proj_ref[r:r + step, :] = mm(ln_ref[r:r + step, :], w_ref[...]).astype(BF16)


def tri_attend(zs_ref, proj_ref, bias_ref, wout_ref, heads, rows, res, after):
    width = proj_ref.shape[1] // 4
    hd = width // heads
    scale2 = hd ** -0.5 * LOG2E
    lane = lax.broadcasted_iota(jnp.int32, (res, width), 1)
    mine = [(lane >= h * hd) & (lane < (h + 1) * hd) for h in range(heads)]
    zero = jnp.zeros((res, width), BF16)

    def part(r, n):
        return proj_ref[r * res:(r + 1) * res, span(n, width)]

    def weights(s):
        ps = []
        for h in range(heads):
            x = s[:, span(h, res)] * scale2 + bias_ref[:, span(h, res)]
            p = jnp.exp2(x - jnp.max(x, axis=1, keepdims=True))
            ps.append((p * (1.0 / jnp.sum(p, axis=1, keepdims=True))).astype(BF16))
        return jnp.concatenate(ps, axis=1)

    def by_head(val):
        return jnp.concatenate([jnp.where(mine[h], val, zero) for h in range(heads)], axis=0)

    few = rows // 2
    for half in range(2):
        ids = range(half * few, (half + 1) * few)
        logits = [mm_nt(part(r, 0), by_head(part(r, 1))) for r in ids]
        probs = [weights(s) for s in logits]
        outs = [mm(p, by_head(part(r, 2))) for r, p in zip(ids, probs)]
        gated = [(jax.nn.sigmoid(part(r, 3).astype(F32)) * o).astype(BF16) for r, o in zip(ids, outs)]
        upds = [mm(y, wout_ref[...]) for y in gated]
        for r, upd in zip(ids, upds):
            zs_ref[span(r, res), :] = (zs_ref[span(r, res), :] + upd).astype(BF16).astype(F32)
        after(half)


def pack_blocks(zs_ref, send_ref, half, rows, res, ndap):
    few = rows // 2

    def one(q, _):
        parts = [zs_ref[pl.ds(half * few * res + q * rows + u, few, stride=res), :] for u in range(rows)]
        send_ref[half, q] = jnp.concatenate(parts, axis=0).astype(BF16)
        return 0

    lax.fori_loop(0, ndap, one, 0)


def unpack_blocks(recv_ref, dst_ref, rows, res, ndap):
    few = rows // 2
    for half in range(2):
        for p in range(ndap):
            blk = recv_ref[half, p].astype(F32)
            for u in range(rows):
                r0 = u * res + p * rows + half * few
                dst_ref[r0:r0 + few, :] = blk[span(u, few), :]


def block_kernel(m_ref, z_ref, fmask_ref, wb_ref, wqkvg_ref, wout_ref, wq_ref, wkv_ref, wg_ref, wcout_ref, wac_ref,
                 rmask_ref, w_ref, wsb_ref, wsp_ref, wso_ref, web_ref, wep_ref, weo_ref,
                 m2_ref, out_ref, msa_refs, pair_refs, *, ndap, heads, hd):
    (a_ref, c_ref, m2v_ref, out_sem, ap_ref, cp_ref, part_ref, x_ref, wt_ref, w32_ref, cnt_ref, pos_ref, neg_ref,
     zs_ref, zc_ref, ln_ref, proj_ref, bias_ref, bwide_ref, sb_ref, sball_ref, eb_ref, eball_ref, xs_ref, xr_ref, ys_ref, yr_ref, wsn_ref, wen_ref,
     ex_send, ex_recv, ring_send, ring_recv, send_sem, recv_sem, gsend, grecv, psend, precv) = pair_refs
    chips = ndap // 2
    me = lax.axis_index('dap')
    rows, res, _ = z_ref.shape
    chip, core = me // 2, lax.rem(me, 2)
    partner = chip * 2 + 1 - core
    swaps = []
    out_copy = pltpu.make_async_copy(m2v_ref, m2_ref, out_sem)

    def send_c():
        swaps.append(remote(c_ref, cp_ref, ex_send.at[0], ex_recv.at[0], partner))

    def send_a():
        swaps.append(remote(a_ref.at[:, 1 - core], ap_ref, ex_send.at[1], ex_recv.at[1], partner))

    def idle():
        outer_prepare(fmask_ref, w_ref, wt_ref, w32_ref, cnt_ref, c_ref.shape[0])
        wsn_ref[...] = wsp_ref[...].T
        wen_ref[...] = wep_ref[...].T

    early = msa_part(m_ref, z_ref, fmask_ref, wb_ref, wqkvg_ref, wout_ref, wq_ref, wkv_ref, wg_ref, wcout_ref, wac_ref, m2v_ref, a_ref, c_ref,
                     idle, (out_copy.start, send_c, send_a), *msa_refs, ndap, heads, hd)
    finish(swaps)
    sends = outer_mean(me, a_ref, c_ref, z_ref, zs_ref, ap_ref, cp_ref, part_ref, x_ref, wt_ref, cnt_ref, pos_ref, neg_ref, ring_send, ring_recv, chips)
    heads = wsb_ref.shape[0]
    kmask = (rmask_ref[...].astype(F32) - 1.0) * 1e4

    tri_bias(zs_ref, ln_ref, wsb_ref, sb_ref, rows, res)
    c1 = start_gather(sb_ref, sball_ref.at[core], chip, core, chips, gsend.at[0], grecv.at[0])
    tri_project(ln_ref, wsn_ref, proj_ref)
    finish(c1)
    p1 = remote(sball_ref.at[core], sball_ref.at[core], psend.at[0], precv.at[0], partner)
    p1.wait_recv()
    bwide_ref[...] = sball_ref[...].astype(F32)
    for h in range(heads):
        bias_ref[:, span(h, res)] = (bias_plane(bwide_ref, h, heads) + kmask) * LOG2E
    moved = []

    def swap_after(src_ref, send_ref, recv_ref, stage):
        def after(half):
            pack_blocks(src_ref, send_ref, half, rows, res, ndap)
            moved.append(start_swap(send_ref.at[half], recv_ref.at[half], me, ndap, send_sem.at[stage, half], recv_sem.at[stage, half]))
        return after

    tri_attend(zs_ref, proj_ref, bias_ref, wso_ref, heads, rows, res, swap_after(zs_ref, xs_ref, xr_ref, 0))
    tri_bias(zs_ref, None, web_ref, eb_ref, rows, res)
    c3 = start_gather(eb_ref, eball_ref.at[core], chip, core, chips, gsend.at[1], grecv.at[1])
    drain(early + swaps)
    finish(moved[0] + moved[1])
    finish(c3)
    p3 = remote(eball_ref.at[core], eball_ref.at[core], psend.at[1], precv.at[1], partner)
    unpack_blocks(xr_ref, zc_ref, rows, res, ndap)
    for r in range(rows):
        ln_ref[span(r, res), :] = ln_lanes(zc_ref[span(r, res), :])
    tri_project(ln_ref, wen_ref, proj_ref)
    p3.wait_recv()
    bwide_ref[...] = eball_ref[...].astype(F32)
    for h in range(heads):
        bias_ref[:, span(h, res)] = (bias_plane(bwide_ref, h, heads).T + kmask) * LOG2E
    tri_attend(zc_ref, proj_ref, bias_ref, weo_ref, heads, rows, res, swap_after(zc_ref, ys_ref, yr_ref, 1))
    drain(sends + c1 + c3 + moved[0] + moved[1] + [p1, p3])
    finish(moved[2] + moved[3])
    unpack_blocks(yr_ref, zs_ref, rows, res, ndap)
    for r in range(rows):
        out_ref[r] = zs_ref[span(r, res), :].astype(BF16)
    drain(moved[2] + moved[3])
    out_copy.wait()


def sds(shape, dtype):
    return jax.ShapeDtypeStruct(shape, dtype)


def solution(mesh):
    ndap = mesh.shape['dap']
    chips = ndap // 2

    def evoformer_block(msa, pair_act, full_mask, res_mask, row_bias_w, row_qkvg_w, row_out_w, col_query_w, col_kv_w, col_gate_w, col_out_w, opm_proj_w, opm_out_w, start_bias_w, start_qkvg_w, start_out_w, end_bias_w, end_qkvg_w, end_out_w):
        seqs, res, chans = msa.shape
        rows = pair_act.shape[0]
        heads, hd = row_qkvg_w.shape[2], row_qkvg_w.shape[3]
        width = heads * hd
        wide = opm_proj_w.shape[2]
        outc = opm_out_w.shape[2]
        thd = start_qkvg_w.shape[2] * start_qkvg_w.shape[3]
        theads = start_bias_w.shape[1]
        m_t = jnp.swapaxes(msa, 1, 2)
        wt = lambda w: w.reshape(w.shape[0], -1).T
        dma = pltpu.SemaphoreType.DMA

        nstat = heads + width // 2
        depth = 2
        npair = rows // 2
        nbuf = 2 * (chips // 2) - 1
        small = (rows * theads, res)
        block = (2, ndap, rows * rows // 2, outc)
        msa_scratch = (
            [VMEM((rows * heads, res), BF16), VMEM((2, chips, rows * heads, res), BF16), VMEM((2, chips, rows * heads, res), F32),
             VMEM((chans, res), F32), VMEM((chans // 2, res), F32), VMEM((chans // 2, res), F32), VMEM((chips, chans // 2, res), F32), VMEM((chans, res), F32),
             VMEM((2, nstat, res), F32), VMEM((nstat, res), F32), VMEM((nstat, res), F32), VMEM((chips, nstat, res), F32),
             VMEM((seqs, chans, res), BF16), VMEM((seqs, res), F32), VMEM((res, heads * res), F32),
             VMEM((chans, width), BF16), VMEM((chans, width), BF16), VMEM((2 * hd + width, chans), BF16),
             VMEM((seqs, width, res), BF16), VMEM((seqs, res, width + 16), BF16), VMEM((seqs, width, res), BF16), VMEM((seqs, width, res), BF16), VMEM((seqs, width, res), BF16),
             [VMEM((res, heads * res), F32)] * depth, [VMEM((heads, res, res), BF16)] * depth, [VMEM((1, heads * res), F32)] * depth,
             VMEM((seqs, 3 * hd, res), F32), VMEM((2 * hd, seqs, res), F32), VMEM((width, res), F32),
             VMEM((seqs, wide + 8, res), F32), VMEM((seqs, wide + 8, res), F32), VMEM((res, wide + 8, seqs), F32),
             dma((3, chips)), dma((3, chips)), dma((5,)), dma((5,))])
        pair_scratch = (
            [VMEM((chips, 2, rows * wide, seqs), BF16), VMEM((wide, seqs, res), BF16), VMEM((seqs, chans, res), BF16), dma(()),
             VMEM((chips, rows * wide, seqs), BF16), VMEM((wide, seqs, res), BF16),
             VMEM((chips, npair, outc, 2 * res), F32),
             VMEM((rows, 2 * wide * wide, res), BF16),
             VMEM((outc, 2 * wide * wide), BF16), VMEM((wide * wide, outc), F32), VMEM((res, res), F32),
             VMEM((nbuf, npair // 2, outc, 2 * res), F32), VMEM((nbuf, npair // 2, outc, 2 * res), F32),
             VMEM((rows * res, outc), F32), VMEM((rows * res, outc), F32), VMEM((rows * res, outc), BF16), VMEM((rows * res, 4 * thd), BF16), VMEM((res, theads * res), F32),
             VMEM((2, chips) + small, F32), VMEM(small, BF16), VMEM((2, chips) + small, BF16), VMEM(small, BF16), VMEM((2, chips) + small, BF16),
             VMEM(block, BF16), VMEM(block, BF16), VMEM(block, BF16), VMEM(block, BF16), VMEM((outc, 4 * thd), BF16), VMEM((outc, 4 * thd), BF16),
             dma((2,)), dma((2,)), dma((2, nbuf)), dma((2, nbuf)), dma((2, 2, ndap)), dma((2, 2, ndap)), dma((2, chips)), dma((2, chips)), dma((2,)), dma((2,))])
        vspec = pl.BlockSpec(memory_space=VMEM)
        m2, pair_out = pl.pallas_call(
            functools.partial(block_kernel, ndap=ndap, heads=heads, hd=hd),
            out_shape=[sds((seqs, chans, res), BF16), sds(pair_act.shape, BF16)],
            in_specs=[vspec] * 19,
            out_specs=[pl.BlockSpec(memory_space=pl.ANY), vspec],
            scratch_shapes=[msa_scratch, pair_scratch],
            compiler_params=pltpu.CompilerParams(vmem_limit_bytes=63 * 2 ** 20, collective_id=0, has_side_effects=True),
            name='evoformer_block',
        )(m_t, pair_act, full_mask, row_bias_w.T, wt(row_qkvg_w), row_out_w.reshape(width, chans), wt(col_query_w), wt(col_kv_w), wt(col_gate_w), col_out_w.reshape(width, chans), wt(opm_proj_w),
          res_mask.reshape(1, res), opm_out_w.reshape(wide * wide, outc),
          start_bias_w.T, wt(start_qkvg_w), start_out_w.reshape(thd, outc), end_bias_w.T, wt(end_qkvg_w), end_out_w.reshape(thd, outc))
        return jnp.swapaxes(m2, 1, 2), pair_out

    row_spec = P(('data', 'dap'), None, None)
    in_specs = (row_spec, row_spec, P('data', None), P('data')) + (P(),) * 15
    return jax.shard_map(evoformer_block, mesh=mesh, in_specs=in_specs, out_specs=(row_spec, row_spec), check_vma=False)
```
